1024 devices in a mesh: gx: 16 (over z), gy: 8 (over x, core), gz: 8 (over y).
Axes of the slice: x: 4, y: 8, z: 16, core: 2. Of those that a mesh axis runs over, the one named last changes fastest.
Arguments:
- dist: float32 [19, 32, 64, 2048], P(None, 'gx', 'gy', 'gz'), may hold values from 0.01 to 0.1
- site_kinds: int32 [32, 64, 2048], P('gx', 'gy', 'gz'), may hold values from 0 to 3
- relax: float32 [32, 64, 2048], P('gx', 'gy', 'gz'), may hold values from 0.5 to 1.9
- inflow: float32 [3, 32, 64, 2048], P(None, 'gx', 'gy', 'gz'), may hold values from -0.3 to 0.3
Outputs:
- density: float32 [32, 64, 2048], P('gx', 'gy', 'gz')
- momentum: float32 [3, 32, 64, 2048], P(None, 'gx', 'gy', 'gz')
The draws below stay inside these ranges and needn't reach their ends.
All inputs are finite; a program needn't handle non-finite values.
Results may differ from the reference program's by a relative error of at most 0.0001.
Values sent between devices are 32-bit elements; how exact they have to be, the bound alone decides.
A program may use at most 32 MiB of HBM per device.

```python
import math
import jax
import jax.numpy as jnp
import numpy as np

STEPS = 2
NX = 32
NY = 64
NZ = 2048


def with_ends(values, own_key, low, high):
    dims = values.shape
    place = [jax.random.randint(jax.random.fold_in(own_key, axis), (), 0, dims[axis]) for axis in range(len(dims))]
    values = values.at[tuple(place)].set(low)
    longest = dims.index(max(dims))
    place[longest] = (place[longest] + 1) % dims[longest]
    return values.at[tuple(place)].set(high)


def steps_of(rng, shape, split, smallest, top_value):
    level, own = 1.0, jax.random.fold_in(rng, 6)
    for position, blocks in split:
        draws = jnp.exp(jax.random.uniform(jax.random.fold_in(own, position), (blocks,), jnp.float32, smallest / len(split), top_value / len(split)))
        level = level * jnp.repeat(draws, shape[position] // blocks).reshape([-1 if axis == position else 1 for axis in range(len(shape))])
    return level


def setup_inputs(seed: int = 0) -> dict:
    arg_keys = jax.random.split(jax.random.key(seed), 5)
    return {
        "dist": jnp.clip(0.01 + 0.09 * jax.random.uniform(arg_keys[0], (19, NX, NY, NZ), jnp.float32) ** steps_of(arg_keys[0], (19, NX, NY, NZ), ((1, 16), (2, 8), (3, 8)), -0.2, 0.2), 0.01, 0.1),
        "site_kinds": with_ends(jax.random.randint(arg_keys[1], (NX, NY, NZ), 0, 4), jax.random.fold_in(arg_keys[1], 1), 0, 3).astype(jnp.int32),
        "relax": jnp.clip(jnp.exp(math.log(1.9) - 1.3350011 * jax.random.uniform(arg_keys[2], (NX, NY, NZ), jnp.float32) ** steps_of(arg_keys[2], (NX, NY, NZ), ((0, 16), (1, 8), (2, 8)), -0.2, 0.2)), 0.5, 1.9),
        "inflow": jnp.clip(jax.random.uniform(arg_keys[3], (3, NX, NY, NZ), jnp.float32, -0.3, 0.3) * steps_of(arg_keys[3], (3, NX, NY, NZ), ((1, 16), (2, 8), (3, 8)), -0.4, 0.0), -0.3, 0.3),
    }


VELOCITIES = [(0, 0, 0), (1, 0, 0), (-1, 0, 0), (0, 1, 0), (0, -1, 0), (0, 0, 1), (0, 0, -1),
              (1, 1, 0), (-1, -1, 0), (1, -1, 0), (-1, 1, 0), (1, 0, 1), (-1, 0, -1),
              (1, 0, -1), (-1, 0, 1), (0, 1, 1), (0, -1, -1), (0, 1, -1), (0, -1, 1)]
WEIGHTS = [1.0 / 3.0] + [1.0 / 18.0] * 6 + [1.0 / 36.0] * 12
OPPOSITE = [0, 2, 1, 4, 3, 6, 5, 8, 7, 10, 9, 12, 11, 14, 13, 16, 15, 18, 17]


def moments(dist):
    table = np.array(VELOCITIES, dtype=np.float32)
    density = jnp.sum(dist, axis=0)
    parts = []
    for axis_id in range(3):
        column = jnp.asarray(table[:, axis_id]).astype(dist.dtype)
        parts.append(jnp.sum(column[:, None, None, None] * dist, axis=0))
    return density, jnp.stack(parts)


def equilibrium(density, speed):
    usq = speed[0] * speed[0] + speed[1] * speed[1] + speed[2] * speed[2]
    result = []
    for index in range(19):
        vel = VELOCITIES[index]
        along = vel[0] * speed[0] + vel[1] * speed[1] + vel[2] * speed[2]
        result.append(WEIGHTS[index] * (density + 3.0 * along + 4.5 * along * along - 1.5 * usq))
    return jnp.stack(result)


def collide(dist, site_kinds, relax, inflow):
    density, speed = moments(dist)
    fluid = dist - relax[None] * (dist - equilibrium(density, speed))
    wall = dist[np.array(OPPOSITE)]
    inlet = equilibrium(density, inflow)
    outlet = equilibrium(jnp.ones_like(density), speed)
    kinds = site_kinds[None]
    return jnp.where(kinds == 0, wall, jnp.where(kinds == 1, fluid, jnp.where(kinds == 2, inlet, outlet)))


def reference(dist, site_kinds, relax, inflow):
    field = dist
    for step in range(STEPS):
        post = collide(field, site_kinds, relax, inflow)
        padded = jnp.pad(post, ((0, 0), (1, 1), (1, 1), (1, 1)))
        moved = []
        for index in range(19):
            vel = VELOCITIES[index]
            moved.append(padded[index, 1 - vel[0]:1 - vel[0] + NX, 1 - vel[1]:1 - vel[1] + NY, 1 - vel[2]:1 - vel[2] + NZ])
        field = jnp.stack(moved)
    return moments(field)
```

```python
import functools

import jax
import jax.numpy as jnp
from jax import lax
from jax.experimental import pallas as pl
from jax.experimental.pallas import tpu as pltpu
from jax.sharding import PartitionSpec as P

VELOCITIES = [
    (0, 0, 0),
    (1, 0, 0),
    (-1, 0, 0),
    (0, 1, 0),
    (0, -1, 0),
    (0, 0, 1),
    (0, 0, -1),
    (1, 1, 0),
    (-1, -1, 0),
    (1, -1, 0),
    (-1, 1, 0),
    (1, 0, 1),
    (-1, 0, -1),
    (1, 0, -1),
    (-1, 0, 1),
    (0, 1, 1),
    (0, -1, -1),
    (0, 1, -1),
    (0, -1, 1),
]
WEIGHTS = [1.0 / 3.0] + [1.0 / 18.0] * 6 + [1.0 / 36.0] * 12
AXES = ("gx", "gy", "gz")
MESH = pl.DeviceIdType.MESH

FACES = [v for v in VELOCITIES if sum(map(abs, v)) == 1]
EDGES = [v for v in VELOCITIES if sum(map(abs, v)) == 2]
DIRECTIONS = FACES + EDGES
X_POPS = {s: [i for i, v in enumerate(VELOCITIES) if v[0] == s] for s in (1, -1)}


def side(sign):
    return 0 if sign == 1 else 1


def crossing(axis, sign):
    inside, corner = [], []
    for i, v in enumerate(VELOCITIES):
        if v[axis] != sign:
            continue
        for plane in (0, 1):
            (inside if 0 <= plane + v[0] <= 1 else corner).append((i, plane))
    return inside + sorted(corner, key=lambda pair: -VELOCITIES[pair[0]][0])


Y_SLOTS = {s: crossing(1, s) for s in (1, -1)}
Z_SLOTS = {s: crossing(2, s) for s in (1, -1)}


def slot_of(slots, sign, i, plane):
    return slots[sign].index((i, plane))


def kernel(
    sizes, dist_hbm, kinds_hbm, relax_hbm, inflow_hbm, rho_ref, mom_ref,
    field, kinds, relax, inflow, post, xs1, xs2, xr1, xr2, ys, yr, xyr, zs, zr, xzr, yzr,
    load_sem, send_sem, recv_sem,
):
    me = tuple(lax.axis_index(a) for a in AXES)
    exists = {}
    for axis in range(3):
        exists[axis, 1] = me[axis] < sizes[axis] - 1
        exists[axis, -1] = me[axis] > 0

    def has(direction):
        parts = [exists[a, s] for a, s in enumerate(direction) if s != 0]
        return parts[0] if len(parts) == 1 else jnp.logical_and(parts[0], parts[1])

    def target(direction):
        return tuple(m + s for m, s in zip(me, direction))

    def opposite(direction):
        return tuple(-s for s in direction)

    loads = []
    for plane in (1, 0):
        group = [
            pltpu.make_async_copy(dist_hbm.at[:, plane], field.at[:, plane], load_sem.at[plane, 0]),
            pltpu.make_async_copy(kinds_hbm.at[plane], kinds.at[plane], load_sem.at[plane, 1]),
            pltpu.make_async_copy(relax_hbm.at[plane], relax.at[plane], load_sem.at[plane, 2]),
            pltpu.make_async_copy(inflow_hbm.at[:, plane], inflow.at[:, plane], load_sem.at[plane, 3]),
        ]
        for copy in group:
            copy.start()
        loads.append(group)

    barrier = pltpu.get_barrier_semaphore()
    neighbours = 0
    for d in DIRECTIONS:
        present = has(d)
        neighbours = neighbours + present.astype(jnp.int32)

        @pl.when(present)
        def _():
            pl.semaphore_signal(barrier, inc=1, device_id=target(d), device_id_type=MESH)

    def message(step, d):
        dx, dy, dz = d
        if dy == 0 and dz == 0:
            return ((xs1, xr1), (xs2, xr2))[step][0].at[side(dx)], ((xs1, xr1), (xs2, xr2))[step][1].at[side(dx)]
        if dz == 0 and dx == 0:
            return ys.at[step, side(dy), 0:8], yr.at[step, side(dy)]
        if dx == 0 and dy == 0:
            return zs.at[step, side(dz)], zr.at[step, side(dz)]
        if dz == 0:
            row = 8 + side(dx)
            return ys.at[step, side(dy), row : row + 1], xyr.at[step, side(dx), side(dy), 0:1]
        if dy == 0:
            return zs.at[step, side(dz)], xzr.at[step, side(dx), side(dz)]
        row = 7 if dy == 1 else 0
        return zs.at[step, side(dz), row : row + 1], yzr.at[step, side(dy), side(dz), 0:1]

    def copy_of(step, d):
        src, dst = message(step, d)
        k = DIRECTIONS.index(d)
        return pltpu.make_async_remote_copy(
            src_ref=src, dst_ref=dst, send_sem=send_sem.at[step, k], recv_sem=recv_sem.at[step, k],
            device_id=target(d), device_id_type=MESH,
        )

    def send(step, d):
        @pl.when(has(d))
        def _():
            copy_of(step, d).start()

    def received(step, d):
        @pl.when(has(opposite(d)))
        def _():
            copy_of(step, d).wait_recv()

    for d in DIRECTIONS:
        @pl.when(jnp.logical_not(has(opposite(d))))
        def _():
            for step in (0, 1):
                dst = message(step, d)[1]
                dst[...] = jnp.zeros(dst.shape, jnp.float32)

    row_id = lax.broadcasted_iota(jnp.int32, (8, 128), 0)
    lane_id = lax.broadcasted_iota(jnp.int32, (8, 128), 1)

    def halves(ref, *index):
        return [ref[index + (slice(None), slice(h * 128, h * 128 + 128))] for h in (0, 1)]

    def collide(plane):
        for h in (0, 1):
            z = slice(h * 128, h * 128 + 128)
            f = [field[i, plane, :, z] for i in range(19)]
            rho = f[0]
            for i in range(1, 19):
                rho = rho + f[i]
            u = []
            for axis in range(3):
                plus = [f[i] for i in range(19) if VELOCITIES[i][axis] == 1]
                minus = [f[i] for i in range(19) if VELOCITIES[i][axis] == -1]
                u.append(functools.reduce(jnp.add, plus) - functools.reduce(jnp.add, minus))
            kind = kinds[plane, :, z]
            wall, fluid, inlet, outlet = kind == 0, kind == 1, kind == 2, kind == 3
            one = jnp.ones((8, 128), jnp.float32)
            r = jnp.where(jnp.logical_or(wall, jnp.logical_or(fluid, inlet)), rho, one)
            v = [jnp.where(inlet, inflow[a, plane, :, z], u[a]) for a in range(3)]
            take = jnp.where(wall, jnp.zeros_like(one), jnp.where(fluid, relax[plane, :, z], one))
            keep = one - take
            usq = v[0] * v[0] + v[1] * v[1] + v[2] * v[2]
            common = r - 1.5 * usq
            post[0, plane, :, z] = keep * f[0] + take * (WEIGHTS[0] * common)
            for i in range(1, 19, 2):
                c = VELOCITIES[i]
                along = None
                for a in range(3):
                    if c[a] != 0:
                        term = v[a] if c[a] == 1 else -v[a]
                        along = term if along is None else along + term
                even = WEIGHTS[i] * (common + 4.5 * along * along)
                odd = (3.0 * WEIGHTS[i]) * along
                here = jnp.where(wall, f[i + 1], f[i])
                there = jnp.where(wall, f[i], f[i + 1])
                post[i, plane, :, z] = keep * here + take * (even + odd)
                post[i + 1, plane, :, z] = keep * there + take * (even - odd)

    def pack(step):
        for s in (1, -1):
            tile = None
            for k, (i, plane) in enumerate(Z_SLOTS[s]):
                if s == 1:
                    col = pltpu.roll(post[i, plane, :, 128:256], (1 + k) % 128, 1)
                    at = k
                else:
                    col = pltpu.roll(post[i, plane, :, 0:128], (127 - k) % 128, 1)
                    at = 127 - k
                tile = col if tile is None else jnp.where(lane_id == at, col, tile)
            zs[step, side(s)] = tile
            row = 7 if s == 1 else 0
            for k, (i, plane) in enumerate(Y_SLOTS[s]):
                ys[step, side(s), k : k + 1] = post[i, plane, row : row + 1]

    def y_moved(planes, sign, edge_row):
        out = []
        for h in (0, 1):
            rolled = pltpu.roll(planes[h], sign % 8, 0)
            edge = 0 if sign == 1 else 7
            out.append(jnp.where(row_id == edge, edge_row[h], rolled))
        return out

    def z_moved(planes, sign, edge_tile):
        rolled = [pltpu.roll(p, sign % 128, 1) for p in planes]
        if sign == 1:
            at = lane_id == 0
            return [jnp.where(at, edge_tile, rolled[0]), jnp.where(at, rolled[0], rolled[1])]
        at = lane_id == 127
        return [jnp.where(at, rolled[1], rolled[0]), jnp.where(at, edge_tile, rolled[1])]

    def z_column(tile, sign, k):
        shift = (128 - k) % 128 if sign == 1 else k % 128
        return tile if shift == 0 else pltpu.roll(tile, shift, 1)

    def inside(step, i, plane):
        cx, cy, cz = VELOCITIES[i]
        q = plane - cx
        value = halves(post, i, q)
        if cy != 0:
            k = slot_of(Y_SLOTS, cy, i, q)
            row = [yr[step, side(cy), k : k + 1, h * 128 : h * 128 + 128] for h in (0, 1)]
            value = y_moved(value, cy, row)
        if cz != 0:
            tile = zr[step, side(cz)]
            if cy != 0:
                edge = 0 if cy == 1 else 7
                tile = jnp.where(row_id == edge, yzr[step, side(cy), side(cz), 0:1], pltpu.roll(tile, cy % 8, 0))
            value = z_moved(value, cz, z_column(tile, cz, slot_of(Z_SLOTS, cz, i, q)))
        return value

    def x_plane(cx):
        return 0 if cx == 1 else 1

    def put(i, plane, value):
        for h in (0, 1):
            field[i, plane, :, h * 128 : h * 128 + 128] = value[h]

    for plane, group in zip((1, 0), loads):
        for copy in group:
            copy.wait()
        collide(plane)
    for s in (1, -1):
        for k, i in enumerate(X_POPS[s]):
            xs1[side(s), k] = post[i, 1 - x_plane(s)]
    pack(0)
    pl.semaphore_wait(barrier, neighbours)
    order = [d for d in EDGES if d[0] != 0] + FACES[:2] + [d for d in EDGES if d[0] == 0] + FACES[2:]
    for d in order:
        send(0, d)

    for d in FACES[2:] + [d for d in EDGES if d[0] == 0]:
        received(0, d)
    for i in range(19):
        for plane in (0, 1):
            if 0 <= plane - VELOCITIES[i][0] <= 1:
                put(i, plane, inside(0, i, plane))
    for d in [d for d in EDGES if d[0] != 0] + FACES[:2]:
        received(0, d)
    for s in (1, -1):
        for n, i in enumerate(X_POPS[s]):
            _, cy, cz = VELOCITIES[i]
            value = halves(xr1, side(s), n)
            if cy != 0:
                row = [xyr[0, side(s), side(cy), 0:1, h * 128 : h * 128 + 128] for h in (0, 1)]
                value = y_moved(value, cy, row)
            if cz != 0:
                k = slot_of(Z_SLOTS, cz, i, 1 - x_plane(s))
                value = z_moved(value, cz, z_column(xzr[0, side(s), side(cz)], cz, k))
            put(i, x_plane(s), value)

    for plane in (1, 0):
        collide(plane)
    zero = jnp.zeros((8, 128), jnp.float32)
    zero_row = [jnp.zeros((1, 128), jnp.float32)] * 2
    for s in (1, -1):
        source = 1 - x_plane(s)
        total, moment_y, moment_z = None, None, None
        for i in X_POPS[s]:
            _, cy, cz = VELOCITIES[i]
            value = halves(post, i, source)
            if cy != 0:
                value = y_moved(value, cy, zero_row)
                moment_y = value if moment_y is None else [a - b for a, b in zip(moment_y, value)]
                flip_y = cy if moment_y is value else flip_y
            if cz != 0:
                value = z_moved(value, cz, zero)
                moment_z = value if moment_z is None else [a - b for a, b in zip(moment_z, value)]
                flip_z = cz if moment_z is value else flip_z
            total = value if total is None else [a + b for a, b in zip(total, value)]
        if flip_y == -1:
            moment_y = [-a for a in moment_y]
        if flip_z == -1:
            moment_z = [-a for a in moment_z]
        for n, value in enumerate((total, moment_y, moment_z)):
            for h in (0, 1):
                xs2[side(s), n, :, h * 128 : h * 128 + 128] = value[h]
    pack(1)
    for d in order:
        send(1, d)

    for d in FACES[2:] + [d for d in EDGES if d[0] == 0]:
        received(1, d)
    sums = []
    for plane in (0, 1):
        acc = [[zero, zero] for _ in range(4)]
        for i in range(19):
            c = VELOCITIES[i]
            if not 0 <= plane - c[0] <= 1:
                continue
            value = inside(1, i, plane)
            for h in (0, 1):
                acc[0][h] = acc[0][h] + value[h]
                for a in range(3):
                    if c[a] == 1:
                        acc[1 + a][h] = acc[1 + a][h] + value[h]
                    if c[a] == -1:
                        acc[1 + a][h] = acc[1 + a][h] - value[h]
        sums.append(acc)
    for d in [d for d in EDGES if d[0] != 0] + FACES[:2]:
        received(1, d)
    for s in (1, -1):
        plane = x_plane(s)
        acc = sums[plane]
        for h in (0, 1):
            z = slice(h * 128, h * 128 + 128)
            total, moment_y, moment_z = (xr2[side(s), n, :, z] for n in range(3))
            for cy in (1, -1):
                edge = 0 if cy == 1 else 7
                value = jnp.where(row_id == edge, xyr[1, side(s), side(cy), 0:1, z], zero)
                total = total + value
                moment_y = moment_y + value if cy == 1 else moment_y - value
            for cz in (1, -1):
                if h != (0 if cz == 1 else 1):
                    continue
                i = VELOCITIES.index((s, 0, cz))
                column = z_column(xzr[1, side(s), side(cz)], cz, slot_of(Z_SLOTS, cz, i, 1 - plane))
                value = jnp.where(lane_id == (0 if cz == 1 else 127), column, zero)
                total = total + value
                moment_z = moment_z + value if cz == 1 else moment_z - value
            rho_ref[plane, :, z] = acc[0][h] + total
            mom_ref[0, plane, :, z] = acc[1][h] + total if s == 1 else acc[1][h] - total
            mom_ref[1, plane, :, z] = acc[2][h] + moment_y
            mom_ref[2, plane, :, z] = acc[3][h] + moment_z

    for step in (0, 1):
        for d in DIRECTIONS:
            @pl.when(has(d))
            def _():
                copy_of(step, d).wait_send()


def solution(mesh):
    sizes = tuple(mesh.shape[a] for a in AXES)

    def shards(dist, site_kinds, relax, inflow):
        f32 = jnp.float32
        block = site_kinds.shape
        return pl.pallas_call(
            functools.partial(kernel, sizes),
            out_shape=(
                jax.ShapeDtypeStruct(block, f32),
                jax.ShapeDtypeStruct((3,) + block, f32),
            ),
            in_specs=[pl.BlockSpec(memory_space=pl.ANY)] * 4,
            out_specs=(pl.BlockSpec(memory_space=pltpu.VMEM), pl.BlockSpec(memory_space=pltpu.VMEM)),
            scratch_shapes=[
                pltpu.VMEM((19,) + block, f32),
                pltpu.VMEM(block, jnp.int32),
                pltpu.VMEM(block, f32),
                pltpu.VMEM((3,) + block, f32),
                pltpu.VMEM((19,) + block, f32),
                pltpu.VMEM((2, 5, 8, 256), f32),
                pltpu.VMEM((2, 3, 8, 256), f32),
                pltpu.VMEM((2, 5, 8, 256), f32),
                pltpu.VMEM((2, 3, 8, 256), f32),
                pltpu.VMEM((2, 2, 16, 256), f32),
                pltpu.VMEM((2, 2, 8, 256), f32),
                pltpu.VMEM((2, 2, 2, 8, 256), f32),
                pltpu.VMEM((2, 2, 8, 128), f32),
                pltpu.VMEM((2, 2, 8, 128), f32),
                pltpu.VMEM((2, 2, 2, 8, 128), f32),
                pltpu.VMEM((2, 2, 2, 8, 128), f32),
                pltpu.SemaphoreType.DMA((2, 4)),
                pltpu.SemaphoreType.DMA((2, 18)),
                pltpu.SemaphoreType.DMA((2, 18)),
            ],
            compiler_params=pltpu.CompilerParams(collective_id=0, has_side_effects=True),
        )(dist, site_kinds, relax, inflow)

    return jax.shard_map(
        shards,
        mesh=mesh,
        in_specs=(
            P(None, "gx", "gy", "gz"),
            P("gx", "gy", "gz"),
            P("gx", "gy", "gz"),
            P(None, "gx", "gy", "gz"),
        ),
        out_specs=(P("gx", "gy", "gz"), P(None, "gx", "gy", "gz")),
        check_vma=False,
    )
```

```python
import functools

import jax
import jax.numpy as jnp
from jax import lax
from jax.experimental import pallas as pl
from jax.experimental.pallas import tpu as pltpu
from jax.sharding import PartitionSpec as P

VELOCITIES = [
    (0, 0, 0),
    (1, 0, 0),
    (-1, 0, 0),
    (0, 1, 0),
    (0, -1, 0),
    (0, 0, 1),
    (0, 0, -1),
    (1, 1, 0),
    (-1, -1, 0),
    (1, -1, 0),
    (-1, 1, 0),
    (1, 0, 1),
    (-1, 0, -1),
    (1, 0, -1),
    (-1, 0, 1),
    (0, 1, 1),
    (0, -1, -1),
    (0, 1, -1),
    (0, -1, 1),
]
WEIGHTS = [1.0 / 3.0] + [1.0 / 18.0] * 6 + [1.0 / 36.0] * 12
AXES = ("gx", "gy", "gz")
MESH = pl.DeviceIdType.MESH

FACES = [v for v in VELOCITIES if sum(map(abs, v)) == 1]
EDGES = [v for v in VELOCITIES if sum(map(abs, v)) == 2]
DIRECTIONS = FACES + EDGES
X_POPS = {s: [i for i, v in enumerate(VELOCITIES) if v[0] == s] for s in (1, -1)}


def side(sign):
    return 0 if sign == 1 else 1


def crossing(axis, sign):
    inside, corner = [], []
    for i, v in enumerate(VELOCITIES):
        if v[axis] != sign:
            continue
        for plane in (0, 1):
            (inside if 0 <= plane + v[0] <= 1 else corner).append((i, plane))
    return inside + sorted(corner, key=lambda pair: -VELOCITIES[pair[0]][0])


Y_SLOTS = {s: crossing(1, s) for s in (1, -1)}
Z_SLOTS = {s: crossing(2, s) for s in (1, -1)}


def slot_of(slots, sign, i, plane):
    return slots[sign].index((i, plane))


def kernel(
    sizes, dist_hbm, kinds_hbm, relax_hbm, inflow_hbm, out_ref,
    field, kinds, relax, inflow, post, xs1, xs2, xr1, xr2, ys, yr, xyr, zs, zr, xzr, yzr,
    load_sem, send_sem, recv_sem, entered,
):
    me = tuple(lax.axis_index(a) for a in AXES)
    exists = {}
    for axis in range(3):
        exists[axis, 1] = me[axis] < sizes[axis] - 1
        exists[axis, -1] = me[axis] > 0

    def has(direction):
        parts = [exists[a, s] for a, s in enumerate(direction) if s != 0]
        return parts[0] if len(parts) == 1 else jnp.logical_and(parts[0], parts[1])

    def target(direction):
        return tuple(m + s for m, s in zip(me, direction))

    def opposite(direction):
        return tuple(-s for s in direction)

    loads = []
    for plane in (1, 0):
        group = [
            pltpu.make_async_copy(dist_hbm.at[:, plane], field.at[:, plane], load_sem.at[plane, 0]),
            pltpu.make_async_copy(kinds_hbm.at[plane], kinds.at[plane], load_sem.at[plane, 1]),
            pltpu.make_async_copy(relax_hbm.at[plane], relax.at[plane], load_sem.at[plane, 2]),
            pltpu.make_async_copy(inflow_hbm.at[:, plane], inflow.at[:, plane], load_sem.at[plane, 3]),
        ]
        for copy in group:
            copy.start()
        loads.append(group)

    def is_origin(place):
        return jnp.logical_and(place[0] == 0, jnp.logical_and(place[1] == 0, place[2] == 0))

    here_origin = is_origin(me)

    def upward(d):
        return next(s for s in (d[0], d[2], d[1]) if s != 0) == 1

    def later(d):
        if upward(d):
            return jnp.logical_and(has(d), jnp.logical_not(here_origin))
        if max(d) == 1:
            return None
        return is_origin(target(d))

    def earlier(d):
        if upward(d):
            return jnp.logical_and(has(d), here_origin)
        if max(d) == 1:
            return has(d)
        return jnp.logical_and(has(d), jnp.logical_not(is_origin(target(d))))

    barrier = pltpu.get_barrier_semaphore()
    for d in DIRECTIONS:
        if later(d) is not None:
            @pl.when(later(d))
            def _():
                pl.semaphore_signal(barrier, inc=1, device_id=target(d), device_id_type=MESH)
    before = 0
    for d in DIRECTIONS:
        before = before + earlier(d).astype(jnp.int32)

    def message(step, d):
        dx, dy, dz = d
        if dy == 0 and dz == 0:
            return ((xs1, xr1), (xs2, xr2))[step][0].at[side(dx)], ((xs1, xr1), (xs2, xr2))[step][1].at[side(dx)]
        if dz == 0 and dx == 0:
            return ys.at[step, side(dy), 0:8], yr.at[step, side(dy)]
        if dx == 0 and dy == 0:
            return zs.at[step, side(dz)], zr.at[step, side(dz)]
        if dz == 0:
            row = 8 + side(dx)
            return ys.at[step, side(dy), row : row + 1], xyr.at[step, side(dx), side(dy), 0:1]
        if dy == 0:
            return zs.at[step, side(dz)], xzr.at[step, side(dx), side(dz)]
        row = 7 if dy == 1 else 0
        return zs.at[step, side(dz), row : row + 1], yzr.at[step, side(dy), side(dz), 0:1]

    def copy_of(step, d):
        src, dst = message(step, d)
        k = DIRECTIONS.index(d)
        return pltpu.make_async_remote_copy(
            src_ref=src, dst_ref=dst, send_sem=send_sem.at[step, k], recv_sem=recv_sem.at[step, k],
            device_id=target(d), device_id_type=MESH,
        )

    def send(step, d):
        @pl.when(has(d))
        def _():
            copy_of(step, d).start()

    def send_later(d):
        @pl.when(later(d))
        def _():
            pl.semaphore_wait(entered.at[DIRECTIONS.index(d)], 1)
            copy_of(0, d).start()

    def received(step, d):
        @pl.when(has(opposite(d)))
        def _():
            copy_of(step, d).wait_recv()

    for d in DIRECTIONS:
        @pl.when(jnp.logical_not(has(opposite(d))))
        def _():
            for step in (0, 1):
                dst = message(step, d)[1]
                dst[...] = jnp.zeros(dst.shape, jnp.float32)

    row_id = lax.broadcasted_iota(jnp.int32, (8, 128), 0)
    lane_id = lax.broadcasted_iota(jnp.int32, (8, 128), 1)

    def halves(ref, *index):
        return [ref[index + (slice(None), slice(h * 128, h * 128 + 128))] for h in (0, 1)]

    def collide(plane):
        for h in (0, 1):
            z = slice(h * 128, h * 128 + 128)
            f = [field[i, plane, :, z] for i in range(19)]
            rho = f[0]
            for i in range(1, 19):
                rho = rho + f[i]
            u = []
            for axis in range(3):
                plus = [f[i] for i in range(19) if VELOCITIES[i][axis] == 1]
                minus = [f[i] for i in range(19) if VELOCITIES[i][axis] == -1]
                u.append(functools.reduce(jnp.add, plus) - functools.reduce(jnp.add, minus))
            kind = kinds[plane, :, z]
            wall, fluid, inlet, outlet = kind == 0, kind == 1, kind == 2, kind == 3
            one = jnp.ones((8, 128), jnp.float32)
            r = jnp.where(jnp.logical_or(wall, jnp.logical_or(fluid, inlet)), rho, one)
            v = [jnp.where(inlet, inflow[a, plane, :, z], u[a]) for a in range(3)]
            take = jnp.where(wall, jnp.zeros_like(one), jnp.where(fluid, relax[plane, :, z], one))
            keep = one - take
            usq = v[0] * v[0] + v[1] * v[1] + v[2] * v[2]
            common = r - 1.5 * usq
            post[0, plane, :, z] = keep * f[0] + take * (WEIGHTS[0] * common)
            for i in range(1, 19, 2):
                c = VELOCITIES[i]
                along = None
                for a in range(3):
                    if c[a] != 0:
                        term = v[a] if c[a] == 1 else -v[a]
                        along = term if along is None else along + term
                even = WEIGHTS[i] * (common + 4.5 * along * along)
                odd = (3.0 * WEIGHTS[i]) * along
                here = jnp.where(wall, f[i + 1], f[i])
                there = jnp.where(wall, f[i], f[i + 1])
                post[i, plane, :, z] = keep * here + take * (even + odd)
                post[i + 1, plane, :, z] = keep * there + take * (even - odd)

    def pack(step):
        for s in (1, -1):
            tile = None
            for k, (i, plane) in enumerate(Z_SLOTS[s]):
                if s == 1:
                    col = pltpu.roll(post[i, plane, :, 128:256], (1 + k) % 128, 1)
                    at = k
                else:
                    col = pltpu.roll(post[i, plane, :, 0:128], (127 - k) % 128, 1)
                    at = 127 - k
                tile = col if tile is None else jnp.where(lane_id == at, col, tile)
            zs[step, side(s)] = tile
            row = 7 if s == 1 else 0
            for k, (i, plane) in enumerate(Y_SLOTS[s]):
                ys[step, side(s), k : k + 1] = post[i, plane, row : row + 1]

    def y_moved(planes, sign, edge_row):
        out = []
        for h in (0, 1):
            rolled = pltpu.roll(planes[h], sign % 8, 0)
            edge = 0 if sign == 1 else 7
            out.append(jnp.where(row_id == edge, edge_row[h], rolled))
        return out

    def z_moved(planes, sign, edge_tile):
        rolled = [pltpu.roll(p, sign % 128, 1) for p in planes]
        if sign == 1:
            at = lane_id == 0
            return [jnp.where(at, edge_tile, rolled[0]), jnp.where(at, rolled[0], rolled[1])]
        at = lane_id == 127
        return [jnp.where(at, rolled[1], rolled[0]), jnp.where(at, edge_tile, rolled[1])]

    def z_column(tile, sign, k):
        shift = (128 - k) % 128 if sign == 1 else k % 128
        return tile if shift == 0 else pltpu.roll(tile, shift, 1)

    def inside(step, i, plane):
        cx, cy, cz = VELOCITIES[i]
        q = plane - cx
        value = halves(post, i, q)
        if cy != 0:
            k = slot_of(Y_SLOTS, cy, i, q)
            row = [yr[step, side(cy), k : k + 1, h * 128 : h * 128 + 128] for h in (0, 1)]
            value = y_moved(value, cy, row)
        if cz != 0:
            tile = zr[step, side(cz)]
            if cy != 0:
                edge = 0 if cy == 1 else 7
                tile = jnp.where(row_id == edge, yzr[step, side(cy), side(cz), 0:1], pltpu.roll(tile, cy % 8, 0))
            value = z_moved(value, cz, z_column(tile, cz, slot_of(Z_SLOTS, cz, i, q)))
        return value

    def x_plane(cx):
        return 0 if cx == 1 else 1

    def put(i, plane, value):
        for h in (0, 1):
            field[i, plane, :, h * 128 : h * 128 + 128] = value[h]

    @pl.when(before > 0)
    def _():
        pl.semaphore_wait(barrier, before)

    for d in DIRECTIONS:
        @pl.when(earlier(d))
        def _():
            at = entered.at[DIRECTIONS.index(opposite(d))]
            pl.semaphore_signal(at, inc=1, device_id=target(d), device_id_type=MESH)

    for plane, group in zip((1, 0), loads):
        for copy in group:
            copy.wait()
        collide(plane)
    for s in (1, -1):
        for k, i in enumerate(X_POPS[s]):
            xs1[side(s), k] = post[i, 1 - x_plane(s)]
    pack(0)
    order = [d for d in EDGES if d[0] != 0] + FACES[:2] + [d for d in EDGES if d[0] == 0] + FACES[2:]
    for d in order:
        @pl.when(earlier(d))
        def _():
            copy_of(0, d).start()
    for d in order:
        if upward(d):
            send_later(d)
    for d in order:
        if max(d) < 1:
            send_later(d)

    for d in FACES[2:] + [d for d in EDGES if d[0] == 0]:
        received(0, d)
    for i in range(19):
        for plane in (0, 1):
            if 0 <= plane - VELOCITIES[i][0] <= 1:
                put(i, plane, inside(0, i, plane))
    for d in [d for d in EDGES if d[0] != 0] + FACES[:2]:
        received(0, d)
    for s in (1, -1):
        for n, i in enumerate(X_POPS[s]):
            _, cy, cz = VELOCITIES[i]
            value = halves(xr1, side(s), n)
            if cy != 0:
                row = [xyr[0, side(s), side(cy), 0:1, h * 128 : h * 128 + 128] for h in (0, 1)]
                value = y_moved(value, cy, row)
            if cz != 0:
                k = slot_of(Z_SLOTS, cz, i, 1 - x_plane(s))
                value = z_moved(value, cz, z_column(xzr[0, side(s), side(cz)], cz, k))
            put(i, x_plane(s), value)

    for plane in (1, 0):
        collide(plane)
    zero = jnp.zeros((8, 128), jnp.float32)
    zero_row = [jnp.zeros((1, 128), jnp.float32)] * 2
    for s in (1, -1):
        source = 1 - x_plane(s)
        total, moment_y, moment_z = None, None, None
        for i in X_POPS[s]:
            _, cy, cz = VELOCITIES[i]
            value = halves(post, i, source)
            if cy != 0:
                value = y_moved(value, cy, zero_row)
                moment_y = value if moment_y is None else [a - b for a, b in zip(moment_y, value)]
                flip_y = cy if moment_y is value else flip_y
            if cz != 0:
                value = z_moved(value, cz, zero)
                moment_z = value if moment_z is None else [a - b for a, b in zip(moment_z, value)]
                flip_z = cz if moment_z is value else flip_z
            total = value if total is None else [a + b for a, b in zip(total, value)]
        if flip_y == -1:
            moment_y = [-a for a in moment_y]
        if flip_z == -1:
            moment_z = [-a for a in moment_z]
        for n, value in enumerate((total, moment_y, moment_z)):
            for h in (0, 1):
                xs2[side(s), n, :, h * 128 : h * 128 + 128] = value[h]
    pack(1)
    for d in order:
        send(1, d)

    for d in FACES[2:] + [d for d in EDGES if d[0] == 0]:
        received(1, d)
    sums = []
    for plane in (0, 1):
        acc = [[zero, zero] for _ in range(4)]
        for i in range(19):
            c = VELOCITIES[i]
            if not 0 <= plane - c[0] <= 1:
                continue
            value = inside(1, i, plane)
            for h in (0, 1):
                acc[0][h] = acc[0][h] + value[h]
                for a in range(3):
                    if c[a] == 1:
                        acc[1 + a][h] = acc[1 + a][h] + value[h]
                    if c[a] == -1:
                        acc[1 + a][h] = acc[1 + a][h] - value[h]
        sums.append(acc)
    for d in [d for d in EDGES if d[0] != 0] + FACES[:2]:
        received(1, d)
    for s in (1, -1):
        plane = x_plane(s)
        acc = sums[plane]
        for h in (0, 1):
            z = slice(h * 128, h * 128 + 128)
            total, moment_y, moment_z = (xr2[side(s), n, :, z] for n in range(3))
            for cy in (1, -1):
                edge = 0 if cy == 1 else 7
                value = jnp.where(row_id == edge, xyr[1, side(s), side(cy), 0:1, z], zero)
                total = total + value
                moment_y = moment_y + value if cy == 1 else moment_y - value
            for cz in (1, -1):
                if h != (0 if cz == 1 else 1):
                    continue
                i = VELOCITIES.index((s, 0, cz))
                column = z_column(xzr[1, side(s), side(cz)], cz, slot_of(Z_SLOTS, cz, i, 1 - plane))
                value = jnp.where(lane_id == (0 if cz == 1 else 127), column, zero)
                total = total + value
                moment_z = moment_z + value if cz == 1 else moment_z - value
            out_ref[0, plane, :, z] = acc[0][h] + total
            out_ref[1, plane, :, z] = acc[1][h] + total if s == 1 else acc[1][h] - total
            out_ref[2, plane, :, z] = acc[2][h] + moment_y
            out_ref[3, plane, :, z] = acc[3][h] + moment_z

    for step in (0, 1):
        for d in DIRECTIONS:
            @pl.when(has(d))
            def _():
                copy_of(step, d).wait_send()


def finish(sums_ref, rho_hbm, mom_hbm, sems):
    copies = [
        pltpu.make_async_copy(sums_ref.at[0], rho_hbm, sems.at[0]),
        pltpu.make_async_copy(sums_ref.at[1:4], mom_hbm, sems.at[1]),
    ]
    for copy in copies:
        copy.start()
    for copy in copies:
        copy.wait()


def solution(mesh):
    sizes = tuple(mesh.shape[a] for a in AXES)

    def shards(dist, site_kinds, relax, inflow):
        f32 = jnp.float32
        block = site_kinds.shape
        sums = pl.pallas_call(
            functools.partial(kernel, sizes),
            out_shape=pltpu.VMEM((4,) + block, f32),
            in_specs=[pl.BlockSpec(memory_space=pl.ANY)] * 4,
            out_specs=pl.BlockSpec(memory_space=pltpu.VMEM),
            scratch_shapes=[
                pltpu.VMEM((19,) + block, f32),
                pltpu.VMEM(block, jnp.int32),
                pltpu.VMEM(block, f32),
                pltpu.VMEM((3,) + block, f32),
                pltpu.VMEM((19,) + block, f32),
                pltpu.VMEM((2, 5, 8, 256), f32),
                pltpu.VMEM((2, 3, 8, 256), f32),
                pltpu.VMEM((2, 5, 8, 256), f32),
                pltpu.VMEM((2, 3, 8, 256), f32),
                pltpu.VMEM((2, 2, 16, 256), f32),
                pltpu.VMEM((2, 2, 8, 256), f32),
                pltpu.VMEM((2, 2, 2, 8, 256), f32),
                pltpu.VMEM((2, 2, 8, 128), f32),
                pltpu.VMEM((2, 2, 8, 128), f32),
                pltpu.VMEM((2, 2, 2, 8, 128), f32),
                pltpu.VMEM((2, 2, 2, 8, 128), f32),
                pltpu.SemaphoreType.DMA((2, 4)),
                pltpu.SemaphoreType.DMA((2, 18)),
                pltpu.SemaphoreType.DMA((2, 18)),
                pltpu.SemaphoreType.REGULAR((18,)),
            ],
            compiler_params=pltpu.CompilerParams(collective_id=0, has_side_effects=True),
        )(dist, site_kinds, relax, inflow)
        return pl.pallas_call(
            finish,
            out_shape=(
                jax.ShapeDtypeStruct(block, f32),
                jax.ShapeDtypeStruct((3,) + block, f32),
            ),
            in_specs=[pl.BlockSpec(memory_space=pltpu.VMEM)],
            out_specs=(pl.BlockSpec(memory_space=pl.ANY), pl.BlockSpec(memory_space=pl.ANY)),
            scratch_shapes=[pltpu.SemaphoreType.DMA((2,))],
        )(pltpu.with_memory_space_constraint(sums, pltpu.VMEM))

    return jax.shard_map(
        shards,
        mesh=mesh,
        in_specs=(
            P(None, "gx", "gy", "gz"),
            P("gx", "gy", "gz"),
            P("gx", "gy", "gz"),
            P(None, "gx", "gy", "gz"),
        ),
        out_specs=(P("gx", "gy", "gz"), P(None, "gx", "gy", "gz")),
        check_vma=False,
    )
```

```python
import functools

import jax
import jax.numpy as jnp
from jax import lax
from jax.experimental import pallas as pl
from jax.experimental.pallas import tpu as pltpu
from jax.sharding import PartitionSpec as P

VELOCITIES = [
    (0, 0, 0),
    (1, 0, 0),
    (-1, 0, 0),
    (0, 1, 0),
    (0, -1, 0),
    (0, 0, 1),
    (0, 0, -1),
    (1, 1, 0),
    (-1, -1, 0),
    (1, -1, 0),
    (-1, 1, 0),
    (1, 0, 1),
    (-1, 0, -1),
    (1, 0, -1),
    (-1, 0, 1),
    (0, 1, 1),
    (0, -1, -1),
    (0, 1, -1),
    (0, -1, 1),
]
WEIGHTS = [1.0 / 3.0] + [1.0 / 18.0] * 6 + [1.0 / 36.0] * 12
AXES = ("gx", "gy", "gz")
MESH = pl.DeviceIdType.MESH

KIND, RELAX, INFLOW = 19, 20, 21
VEL = VELOCITIES + [(0, 0, 0)] * 5
FIELDS = range(24)
ORDER = sorted(FIELDS, key=lambda j: (-VEL[j][0], j))
POS = [ORDER.index(j) for j in FIELDS]
STEPS = (-1, 0, 1)
DIRECTIONS = [(x, y, z) for x in STEPS for y in STEPS for z in STEPS if (x, y, z) != (0, 0, 0)]
NEAR = (-1, 0, 1, 2)


def groups(axis, sign):
    found = [(j, 1) for j in FIELDS if VEL[j][axis] in (0, sign)]
    found += [(j, 2) for j in FIELDS if VEL[j][axis] == sign]
    return sorted(found, key=lambda pair: VEL[pair[0]][0])


ROWS = {s: groups(1, s) for s in (1, -1)}
COLS = {s: groups(2, s) for s in (1, -1)}
LOCAL = {s: sorted([j for j in FIELDS if VEL[j][2] == -s], key=lambda j: VEL[j][0]) for s in (1, -1)}
LOCAL_LANE = {1: 96, -1: 64}


def side(sign):
    return 0 if sign == 1 else 1


def opposite(direction):
    return tuple(-s for s in direction)


def upward(d):
    return next(s for s in (d[0], d[2], d[1]) if s != 0) == 1


def messages():
    found = []
    for d in DIRECTIONS:
        dx, dy, dz = d
        if dy == 0 and dz == 0:
            found += [("xp", d), ("xb", d), ("xa", d)]
        if dz == 0 and dy != 0:
            found.append(("y", d))
        if dz != 0:
            found.append(("z", d))
        else:
            found.append(("l", d))
    return found


MESSAGES = messages()


def kernel(
    sizes, dist_hbm, kinds_hbm, relax_hbm, inflow_hbm, out_ref,
    field, kinds, block, ys, yr, zs, zr, ls, lr, first, second, row_tile, row_post,
    load_sem, send_sem, recv_sem, entered,
):
    me = tuple(lax.axis_index(a) for a in AXES)
    exists = {}
    for axis in range(3):
        exists[axis, 1] = me[axis] < sizes[axis] - 1
        exists[axis, -1] = me[axis] > 0

    def has(direction):
        parts = [exists[a, s] for a, s in enumerate(direction) if s != 0]
        return functools.reduce(jnp.logical_and, parts)

    def target(direction):
        return tuple(m + s for m, s in zip(me, direction))

    loads = []
    for p in (1, 0):
        group = [
            pltpu.make_async_copy(kinds_hbm.at[p], kinds.at[p], load_sem.at[p, 0]),
            pltpu.make_async_copy(relax_hbm.at[p], block.at[POS[RELAX], 2 + p], load_sem.at[p, 1]),
            pltpu.make_async_copy(
                inflow_hbm.at[:, p], block.at[POS[INFLOW] : POS[INFLOW] + 3, 2 + p], load_sem.at[p, 2]
            ),
            pltpu.make_async_copy(dist_hbm.at[:, p], field.at[:, p], load_sem.at[p, 3]),
        ]
        for copy in group:
            copy.start()
        loads.append(group)

    def is_origin(place):
        return jnp.logical_and(place[0] == 0, jnp.logical_and(place[1] == 0, place[2] == 0))

    here_origin = is_origin(me)

    def later(d):
        if upward(d):
            return jnp.logical_and(has(d), jnp.logical_not(here_origin))
        if max(d) == 1:
            return None
        return is_origin(target(d))

    def earlier(d):
        if upward(d):
            return jnp.logical_and(has(d), here_origin)
        if max(d) == 1:
            return has(d)
        return jnp.logical_and(has(d), jnp.logical_not(is_origin(target(d))))

    barrier = pltpu.get_barrier_semaphore()
    for d in DIRECTIONS:
        if later(d) is not None:
            @pl.when(later(d))
            def _():
                pl.semaphore_signal(barrier, inc=1, device_id=target(d), device_id_type=MESH)
    before = 0
    for d in DIRECTIONS:
        before = before + earlier(d).astype(jnp.int32)

    def ends(m):
        kind, (dx, dy, dz) = m
        if kind == "xa":
            at, mine, theirs = (slice(0, 5), slice(2, 4), slice(0, 2)) if dx == 1 else (slice(19, 24), slice(2, 4), slice(4, 6))
            return block.at[at, mine], block.at[at, theirs]
        if kind in ("xb", "xp"):
            at = slice(5, 14) if kind == "xb" else slice(14, 19)
            mine, theirs = (3, 1) if dx == 1 else (2, 4)
            return block.at[at, mine : mine + 1], block.at[at, theirs : theirs + 1]
        if kind == "y":
            rows = {0: slice(0, 48), 1: slice(8, 48), -1: slice(0, 40)}[dx]
            return ys.at[side(dy), rows], yr.at[side(dy), dx + 1, rows]
        if kind == "z":
            return zs.at[side(dz)], zr.at[side(dz), dx + 1, dy + 1]
        return ls.at[0], lr.at[dx + 1, dy + 1]

    def copy_of(m):
        src, dst = ends(m)
        k = MESSAGES.index(m)
        return pltpu.make_async_remote_copy(
            src_ref=src, dst_ref=dst, send_sem=send_sem.at[k], recv_sem=recv_sem.at[k],
            device_id=target(m[1]), device_id_type=MESH,
        )

    for m in MESSAGES:
        @pl.when(jnp.logical_not(has(opposite(m[1]))))
        def _():
            dst = ends(m)[1]
            dst[...] = jnp.zeros(dst.shape, jnp.float32)

    row_id = lax.broadcasted_iota(jnp.int32, (8, 128), 0)
    lane_id = lax.broadcasted_iota(jnp.int32, (8, 128), 1)
    one = jnp.ones((8, 128), jnp.float32)
    zero = jnp.zeros((8, 128), jnp.float32)

    def turn(tile, shift):
        shift %= 128
        return tile if shift == 0 else pltpu.roll(tile, shift, 1)

    def slide(tile, shift):
        return pltpu.roll(tile, shift % 8, 0)

    def lanes(h):
        return slice(h * 128, h * 128 + 128)

    def collide(f, kind, relax, inflow, wanted, inside=None):
        rho = functools.reduce(jnp.add, f)
        u = []
        for axis in range(3):
            plus = [f[i] for i in range(19) if VELOCITIES[i][axis] == 1]
            minus = [f[i] for i in range(19) if VELOCITIES[i][axis] == -1]
            u.append(functools.reduce(jnp.add, plus) - functools.reduce(jnp.add, minus))
        wall, fluid = kind < 0.5, jnp.logical_and(kind > 0.5, kind < 1.5)
        inlet, outlet = jnp.logical_and(kind > 1.5, kind < 2.5), kind > 2.5
        r = jnp.where(outlet, one, rho)
        v = [jnp.where(inlet, inflow[a], u[a]) for a in range(3)]
        take = jnp.where(wall, zero, jnp.where(fluid, relax, one))
        keep = one - take
        if inside is not None:
            take, keep = take * inside, keep * inside
        usq = v[0] * v[0] + v[1] * v[1] + v[2] * v[2]
        common = r - 1.5 * usq
        post = {}
        if 0 in wanted:
            post[0] = keep * f[0] + take * (WEIGHTS[0] * common)
        for i in range(1, 19, 2):
            if i not in wanted and i + 1 not in wanted:
                continue
            along = None
            for a in range(3):
                if VELOCITIES[i][a] != 0:
                    term = v[a] if VELOCITIES[i][a] == 1 else -v[a]
                    along = term if along is None else along + term
            even = WEIGHTS[i] * (common + 4.5 * along * along)
            odd = (3.0 * WEIGHTS[i]) * along
            if i in wanted:
                post[i] = keep * jnp.where(wall, f[i + 1], f[i]) + take * (even + odd)
            if i + 1 in wanted:
                post[i + 1] = keep * jnp.where(wall, f[i], f[i + 1]) + take * (even - odd)
        return post

    def send_when(m, condition):
        @pl.when(condition)
        def _():
            copy_of(m).start()

    @pl.when(before > 0)
    def _():
        pl.semaphore_wait(barrier, before)

    for d in DIRECTIONS:
        @pl.when(earlier(d))
        def _():
            at = entered.at[DIRECTIONS.index(opposite(d))]
            pl.semaphore_signal(at, inc=1, device_id=target(d), device_id_type=MESH)

    for p, group in zip((1, 0), loads):
        for copy in group[:3]:
            copy.wait()
        block[POS[KIND], 2 + p] = kinds[p].astype(jnp.float32)
        for m in MESSAGES:
            if m[0] == "xp" and m[1][0] == (1 if p == 1 else -1):
                send_when(m, earlier(m[1]))
        group[3].wait()
        for h in (0, 1):
            z = lanes(h)
            post = collide(
                [field[i, p, :, z] for i in range(19)],
                block[POS[KIND], 2 + p, :, z],
                block[POS[RELAX], 2 + p, :, z],
                [block[POS[INFLOW + a], 2 + p, :, z] for a in range(3)],
                range(19),
            )
            for i in range(19):
                block[POS[i], 2 + p, :, z] = post[i]

    def column(j, p, at):
        return block[POS[j], 2 + p, :, lanes(at // 128)], at % 128

    for s in (1, -1):
        tile = zero
        for g, (j, depth) in enumerate(COLS[s]):
            for p in (0, 1):
                value, at = column(j, p, 256 - depth if s == 1 else depth - 1)
                to = 4 * g + p + VEL[j][0] + 1
                tile = jnp.where(lane_id == to, turn(value, to - at), tile)
        zs[side(s)] = tile
    tile = zero
    for s in (1, -1):
        for g, j in enumerate(LOCAL[s]):
            for p in (0, 1):
                value, at = column(j, p, 0 if s == 1 else 255)
                to = LOCAL_LANE[s] + 4 * g + p + VEL[j][0] + 1
                tile = jnp.where(lane_id == to, turn(value, to - at), tile)
    ls[0] = tile
    small = [m for m in MESSAGES if m[0] in ("z", "l")]
    small = sorted(small, key=lambda m: -sum(map(abs, m[1])))
    planes = [m for m in MESSAGES if m[0] in ("xb", "xa")]
    rows = sorted([m for m in MESSAGES if m[0] == "y"], key=lambda m: -abs(m[1][0]))
    for m in small + planes:
        send_when(m, earlier(m[1]))
    for s in (1, -1):
        for g, (j, depth) in enumerate(ROWS[s]):
            for p in (0, 1):
                row = 8 - depth if s == 1 else depth - 1
                ys[side(s), 2 * g + p : 2 * g + p + 1] = block[POS[j], 2 + p, row : row + 1]
    for m in rows:
        send_when(m, earlier(m[1]))

    def send_later(d):
        @pl.when(later(d))
        def _():
            pl.semaphore_wait(entered.at[DIRECTIONS.index(d)], 1)
            for m in small + planes + rows + [m for m in MESSAGES if m[0] == "xp"]:
                if m[1] == d:
                    copy_of(m).start()

    for d in DIRECTIONS:
        if upward(d):
            send_later(d)
    for d in DIRECTIONS:
        if max(d) < 1:
            send_later(d)

    for m in MESSAGES:
        @pl.when(has(opposite(m[1])))
        def _():
            copy_of(m).wait_recv()

    group_id = lane_id // 4
    lane_cx = jnp.where(group_id < 5, -1, jnp.where(group_id < 19, 0, 1))
    lane_cx = jnp.where(group_id >= 24, jnp.where(group_id < 25, -1, jnp.where(group_id < 28, 0, 1)), lane_cx)
    source = lane_id % 4 - 1 - lane_cx
    straight, shifted = {}, {}
    for s in (1, -1):
        merged = {}
        for dy in STEPS:
            parts = []
            for dx in STEPS:
                local = ls[0] if dx == 0 and dy == 0 else lr[dx + 1, dy + 1]
                if s == -1:
                    local = turn(local, 32)
                part = jnp.where(lane_id >= 96, local, zr[side(s), dx + 1, dy + 1])
                parts.append(turn(part, -2 * dx))
            merged[dy] = jnp.where(source < 0, parts[2], jnp.where(source > 1, parts[0], parts[1]))
        below, own, above = merged[1], merged[0], merged[-1]
        top, bottom = row_id == 0, row_id == 7
        straight[s, 0] = own
        straight[s, 1] = jnp.where(top, slide(below, 1), slide(own, 1))
        straight[s, -1] = jnp.where(bottom, slide(above, -1), slide(own, -1))
        shifted[s, 0] = jnp.where(top, slide(below, 1), slide(above, -1))
        shifted[s, 1] = jnp.where(top, slide(below, 2), own)
        shifted[s, -1] = jnp.where(bottom, slide(above, -2), own)

    def y_moved(value, sign, edge_row):
        edge = 0 if sign == 1 else 7
        return [jnp.where(row_id == edge, edge_row[h], slide(value[h], sign)) for h in (0, 1)]

    def z_moved(value, sign, edge_tile):
        rolled = [turn(v, sign) for v in value]
        if sign == 1:
            at = lane_id == 0
            return [jnp.where(at, edge_tile, rolled[0]), jnp.where(at, rolled[0], rolled[1])]
        at = lane_id == 127
        return [jnp.where(at, rolled[1], rolled[0]), jnp.where(at, edge_tile, rolled[1])]

    def edge_lane(sign):
        return 0 if sign == 1 else 127

    def incoming_row(s, j, depth, plane):
        p = plane - VEL[j][0]
        dx = 1 if p < 0 else -1 if p > 1 else 0
        k = 2 * ROWS[s].index((j, depth)) + p + 2 * dx
        return [yr[side(s), dx + 1, k : k + 1, lanes(h)] for h in (0, 1)]

    def presence(axis, sign):
        return exists[axis, sign].astype(jnp.float32)

    for plane in NEAR:
        for i in range(19):
            cx, cy, cz = VELOCITIES[i]
            value = [block[POS[i], plane - cx + 2, :, lanes(h)] for h in (0, 1)]
            if cy != 0:
                value = y_moved(value, cy, incoming_row(cy, i, 1, plane))
            if cz != 0:
                at = 4 * COLS[cz].index((i, 1)) + plane + 1
                value = z_moved(value, cz, turn(straight[cz, cy], edge_lane(cz) - at))
            for h in (0, 1):
                first[i, plane + 1, :, lanes(h)] = value[h]
        inside, wanted = None, range(19)
        if plane == -1:
            inside, wanted = one * presence(0, -1), [i for i in range(19) if VELOCITIES[i][0] == 1]
        if plane == 2:
            inside, wanted = one * presence(0, 1), [i for i in range(19) if VELOCITIES[i][0] == -1]
        for h in (0, 1):
            z = lanes(h)
            post = collide(
                [first[i, plane + 1, :, z] for i in range(19)],
                block[POS[KIND], plane + 2, :, z],
                block[POS[RELAX], plane + 2, :, z],
                [block[POS[INFLOW + a], plane + 2, :, z] for a in range(3)],
                wanted, inside,
            )
            for i in wanted:
                second[i, plane + 1, :, z] = post[i]

    lowest, highest = row_id % 4 == 0, row_id % 4 == 3
    beside = jnp.where(lowest, presence(0, -1), jnp.where(highest, presence(0, 1), one))
    outside = beside * jnp.where(row_id < 4, presence(1, -1), presence(1, 1))
    edges = {}
    for s in (1, -1):
        for cy in STEPS:
            tile = shifted[s, cy]
            tile = jnp.where(row_id < 4, tile[0:1], turn(jnp.broadcast_to(tile[7:8], (8, 128)), 4))
            aligned = tile
            for r in range(1, 8):
                aligned = jnp.where(row_id == r, turn(tile, -r), aligned)
            edges[s, cy] = aligned
    for j in FIELDS:
        cx, cy, cz = VEL[j]
        for s in (1, -1):
            for plane in NEAR:
                k = 4 * side(s) + plane + 1
                if cy == -s:
                    row = 0 if s == 1 else 7
                    row_tile[j, k : k + 1] = block[POS[j], plane - cx + 2, row : row + 1]
                else:
                    value = incoming_row(s, j, 1 if cy == 0 else 2, plane)
                    for h in (0, 1):
                        row_tile[j, k : k + 1, lanes(h)] = value[h]
    for i in range(19):
        cx, cy, cz = VELOCITIES[i]
        if cz != 0:
            value = [row_tile[i, :, lanes(h)] for h in (0, 1)]
            at = 4 * COLS[cz].index((i, 1))
            value = z_moved(value, cz, turn(edges[cz, cy], edge_lane(cz) - at))
            for h in (0, 1):
                row_tile[i, :, lanes(h)] = value[h]
    moving_y = [i for i in range(19) if VELOCITIES[i][1] != 0]
    for h in (0, 1):
        f = [row_tile[j, :, lanes(h)] for j in FIELDS]
        post = collide(f[:19], f[KIND], f[RELAX], f[INFLOW : INFLOW + 3], moving_y, outside)
        for i in moving_y:
            row_post[i, :, lanes(h)] = post[i]

    def column_tile(j):
        _, cy, cz = VEL[j]
        tile = None
        for s in (1, -1):
            if cz == -s:
                at = 96 + 4 * LOCAL[s].index(j)
            else:
                at = 4 * COLS[s].index((j, 1 if cz == 0 else 2))
            for outer, parts in ((0, straight), (8, shifted)):
                start = outer + 4 * side(s)
                part = turn(parts[s, cy], start - at)
                here = jnp.logical_and(lane_id >= start, lane_id < start + 4)
                tile = part if tile is None else jnp.where(here, part, tile)
        return tile

    lowest, highest = lane_id % 4 == 0, lane_id % 4 == 3
    beside = jnp.where(lowest, presence(0, -1), jnp.where(highest, presence(0, 1), one))
    outside = beside * jnp.where(lane_id % 8 < 4, presence(2, -1), presence(2, 1))
    beyond = jnp.where(row_id == 0, presence(1, -1), presence(1, 1))
    outside = outside * jnp.where(lane_id < 8, one, beyond)
    f = [column_tile(j) for j in FIELDS]
    moving_z = [i for i in range(19) if VELOCITIES[i][2] != 0]
    column_post = collide(f[:19], f[KIND], f[RELAX], f[INFLOW : INFLOW + 3], moving_z, outside)

    for p in (0, 1):
        acc = [[None, None] for _ in range(4)]
        for i in range(19):
            c = cx, cy, cz = VELOCITIES[i]
            plane = p - cx
            value = [second[i, plane + 1, :, lanes(h)] for h in (0, 1)]
            if cy != 0:
                k = 4 * side(cy) + plane + 1
                value = y_moved(value, cy, [row_post[i, k : k + 1, lanes(h)] for h in (0, 1)])
            if cz != 0:
                at = 4 * side(cz) + plane + 1
                edge = turn(column_post[i], edge_lane(cz) - at)
                if cy != 0:
                    corner = turn(column_post[i], edge_lane(cz) - at - 8)
                    edge = jnp.where(row_id == (0 if cy == 1 else 7), corner, slide(edge, cy))
                value = z_moved(value, cz, edge)
            for h in (0, 1):
                acc[0][h] = value[h] if acc[0][h] is None else acc[0][h] + value[h]
                for a in range(3):
                    if c[a] != 0:
                        old = zero if acc[1 + a][h] is None else acc[1 + a][h]
                        acc[1 + a][h] = old + value[h] if c[a] == 1 else old - value[h]
        for h in (0, 1):
            for k in range(4):
                out_ref[k, p, :, lanes(h)] = acc[k][h]

    for m in MESSAGES:
        @pl.when(has(m[1]))
        def _():
            copy_of(m).wait_send()


def finish(sums_ref, rho_hbm, mom_hbm, sems):
    copies = [
        pltpu.make_async_copy(sums_ref.at[0], rho_hbm, sems.at[0]),
        pltpu.make_async_copy(sums_ref.at[1:4], mom_hbm, sems.at[1]),
    ]
    for copy in copies:
        copy.start()
    for copy in copies:
        copy.wait()


def solution(mesh):
    sizes = tuple(mesh.shape[a] for a in AXES)
    count = len(MESSAGES)

    def shards(dist, site_kinds, relax, inflow):
        f32 = jnp.float32
        shape = site_kinds.shape
        sums = pl.pallas_call(
            functools.partial(kernel, sizes),
            out_shape=pltpu.VMEM((4,) + shape, f32),
            in_specs=[pl.BlockSpec(memory_space=pl.ANY)] * 4,
            out_specs=pl.BlockSpec(memory_space=pltpu.VMEM),
            scratch_shapes=[
                pltpu.VMEM((19,) + shape, f32),
                pltpu.VMEM(shape, jnp.int32),
                pltpu.VMEM((24, 6, 8, 256), f32),
                pltpu.VMEM((2, 48, 256), f32),
                pltpu.VMEM((2, 3, 48, 256), f32),
                pltpu.VMEM((2, 8, 128), f32),
                pltpu.VMEM((2, 3, 3, 8, 128), f32),
                pltpu.VMEM((1, 8, 128), f32),
                pltpu.VMEM((3, 3, 8, 128), f32),
                pltpu.VMEM((19, 4, 8, 256), f32),
                pltpu.VMEM((19, 4, 8, 256), f32),
                pltpu.VMEM((24, 8, 256), f32),
                pltpu.VMEM((19, 8, 256), f32),
                pltpu.SemaphoreType.DMA((2, 4)),
                pltpu.SemaphoreType.DMA((count,)),
                pltpu.SemaphoreType.DMA((count,)),
                pltpu.SemaphoreType.REGULAR((len(DIRECTIONS),)),
            ],
            compiler_params=pltpu.CompilerParams(collective_id=0, has_side_effects=True),
        )(dist, site_kinds, relax, inflow)
        return pl.pallas_call(
            finish,
            out_shape=(
                jax.ShapeDtypeStruct(shape, f32),
                jax.ShapeDtypeStruct((3,) + shape, f32),
            ),
            in_specs=[pl.BlockSpec(memory_space=pltpu.VMEM)],
            out_specs=(pl.BlockSpec(memory_space=pl.ANY), pl.BlockSpec(memory_space=pl.ANY)),
            scratch_shapes=[pltpu.SemaphoreType.DMA((2,))],
        )(pltpu.with_memory_space_constraint(sums, pltpu.VMEM))

    return jax.shard_map(
        shards,
        mesh=mesh,
        in_specs=(
            P(None, "gx", "gy", "gz"),
            P("gx", "gy", "gz"),
            P("gx", "gy", "gz"),
            P(None, "gx", "gy", "gz"),
        ),
        out_specs=(P("gx", "gy", "gz"), P(None, "gx", "gy", "gz")),
        check_vma=False,
    )
```

```python
import functools
import itertools

import jax
import jax.numpy as jnp
from jax import lax
from jax.experimental import pallas as pl
from jax.experimental.pallas import tpu as pltpu
from jax.sharding import PartitionSpec as P

VELOCITIES = [
    (0, 0, 0),
    (1, 0, 0),
    (-1, 0, 0),
    (0, 1, 0),
    (0, -1, 0),
    (0, 0, 1),
    (0, 0, -1),
    (1, 1, 0),
    (-1, -1, 0),
    (1, -1, 0),
    (-1, 1, 0),
    (1, 0, 1),
    (-1, 0, -1),
    (1, 0, -1),
    (-1, 0, 1),
    (0, 1, 1),
    (0, -1, -1),
    (0, 1, -1),
    (0, -1, 1),
]
WEIGHTS = [1.0 / 3.0] + [1.0 / 18.0] * 6 + [1.0 / 36.0] * 12
AXES = ("gx", "gy", "gz")
MESH = pl.DeviceIdType.MESH

KIND, RELAX, INFLOW = 19, 20, 21
VEL = VELOCITIES + [(0, 0, 0)] * 5
FIELDS = range(24)
ORDER = sorted(FIELDS, key=lambda j: (-VEL[j][0], j))
POS = [ORDER.index(j) for j in FIELDS]
STEPS = (-1, 0, 1)
DIRECTIONS = [(x, y, z) for x in STEPS for y in STEPS for z in STEPS if (x, y, z) != (0, 0, 0)]
NEAR = (-1, 0, 1, 2)


def groups(axis, sign):
    found = [(j, 1) for j in FIELDS if VEL[j][axis] in (0, sign)]
    found += [(j, 2) for j in FIELDS if VEL[j][axis] == sign]
    return sorted(found, key=lambda pair: VEL[pair[0]][0])


ROWS = {s: groups(1, s) for s in (1, -1)}
COLS = {s: groups(2, s) for s in (1, -1)}
LOCAL = {s: sorted([j for j in FIELDS if VEL[j][2] == -s], key=lambda j: VEL[j][0]) for s in (1, -1)}
LOCAL_LANE = {1: 96, -1: 64}


def side(sign):
    return 0 if sign == 1 else 1


def opposite(direction):
    return tuple(-s for s in direction)


def upward(d):
    return next(s for s in (d[0], d[2], d[1]) if s != 0) == 1


def row_place(g, p):
    if g < 5:
        return 2 * g + p
    if g < 19:
        return 10 + 14 * p + g - 5
    return 38 + 2 * (g - 19) + p


def messages():
    found = []
    for d in DIRECTIONS:
        dx, dy, dz = d
        if dy == 0 and dz == 0:
            found += [("xp", d), ("xb", d), ("xa", d)]
        if dz == 0 and dy != 0:
            found.append(("y", d))
        if dz != 0:
            found.append(("z", d))
        else:
            found.append(("l", d))
    return found


MESSAGES = messages()


def tiles(m):
    if m[0] == "y":
        return 12 if m[1][0] == 0 else 6
    return {"xp": 10, "xb": 18, "xa": 20, "z": 1, "l": 1}[m[0]]


def kernel(
    sizes, dist_hbm, kinds_hbm, relax_hbm, inflow_hbm, out_ref,
    field, kinds, block, ys, yr, zs, zr, ls, lr, first, second, row_tile, row_post,
    size_ref, load_sem, send_sem, recv_sem, entered,
):
    me = tuple(lax.axis_index(a) for a in AXES)
    exists = {}
    for axis in range(3):
        exists[axis, 1] = me[axis] < sizes[axis] - 1
        exists[axis, -1] = me[axis] > 0

    def has(direction):
        parts = [exists[a, s] for a, s in enumerate(direction) if s != 0]
        return functools.reduce(jnp.logical_and, parts)

    def target(direction):
        return tuple(m + s for m, s in zip(me, direction))

    for p in (1, 0):
        group = [
            pltpu.make_async_copy(kinds_hbm.at[p], kinds.at[p], load_sem.at[p]),
            pltpu.make_async_copy(relax_hbm.at[p], block.at[POS[RELAX], 2 + p], load_sem.at[p]),
            pltpu.make_async_copy(
                inflow_hbm.at[:, p], block.at[POS[INFLOW] : POS[INFLOW] + 3, 2 + p], load_sem.at[p]
            ),
            pltpu.make_async_copy(dist_hbm.at[:, p], field.at[:, p], load_sem.at[p]),
        ]
        for copy in group:
            copy.start()

    def is_origin(place):
        return jnp.logical_and(place[0] == 0, jnp.logical_and(place[1] == 0, place[2] == 0))

    here_origin = is_origin(me)

    def later(d):
        if upward(d):
            return jnp.logical_and(has(d), jnp.logical_not(here_origin))
        if max(d) == 1:
            return None
        return is_origin(target(d))

    def earlier(d):
        if upward(d):
            return jnp.logical_and(has(d), here_origin)
        if max(d) == 1:
            return has(d)
        return jnp.logical_and(has(d), jnp.logical_not(is_origin(target(d))))

    barrier = pltpu.get_barrier_semaphore()
    for d in DIRECTIONS:
        if later(d) is not None:
            @pl.when(later(d))
            def _():
                pl.semaphore_signal(barrier, inc=1, device_id=target(d), device_id_type=MESH)
    before = 0
    for d in DIRECTIONS:
        before = before + earlier(d).astype(jnp.int32)

    def ends(m):
        kind, (dx, dy, dz) = m
        if kind == "xa":
            at, mine, theirs = (slice(0, 5), slice(2, 4), slice(0, 2)) if dx == 1 else (slice(19, 24), slice(2, 4), slice(4, 6))
            return block.at[at, mine], block.at[at, theirs]
        if kind in ("xb", "xp"):
            at = slice(5, 14) if kind == "xb" else slice(14, 19)
            mine, theirs = (3, 1) if dx == 1 else (2, 4)
            return block.at[at, mine : mine + 1], block.at[at, theirs : theirs + 1]
        if kind == "y":
            rows = {0: slice(0, 48), 1: slice(24, 48), -1: slice(0, 24)}[dx]
            return ys.at[side(dy), rows], yr.at[side(dy), dx + 1, rows]
        if kind == "z":
            return zs.at[side(dz)], zr.at[side(dz), dx + 1, dy + 1]
        return ls.at[0], lr.at[dx + 1, dy + 1]

    def copy_of(m):
        src, dst = ends(m)
        return pltpu.make_async_remote_copy(
            src_ref=src, dst_ref=dst, send_sem=send_sem.at[0], recv_sem=recv_sem.at[side(m[1][0])],
            device_id=target(m[1]), device_id_type=MESH,
        )

    def await_tiles(count, sem):
        part = size_ref.at[0:count]
        pltpu.make_async_copy(part, part, sem).wait()

    def await_present(found, toward, sem):
        count = 0
        for m in found:
            count = count + tiles(m) * has(toward(m[1])).astype(jnp.int32)
        sums = set()
        for touched in itertools.product(((), (1,), (-1,), (1, -1)), repeat=3):
            known = [m for m in found if not any(v in touched[a] for a, v in enumerate(toward(m[1])))]
            sums.add(sum(map(tiles, known)))
        for total in sorted(sums - {0}):
            @pl.when(count == total)
            def _():
                await_tiles(total, sem)

    for m in MESSAGES:
        @pl.when(jnp.logical_not(has(opposite(m[1]))))
        def _():
            dst = ends(m)[1]
            dst[...] = jnp.zeros(dst.shape, jnp.float32)

    row_id = lax.broadcasted_iota(jnp.int32, (8, 128), 0)
    lane_id = lax.broadcasted_iota(jnp.int32, (8, 128), 1)
    one = jnp.ones((8, 128), jnp.float32)
    zero = jnp.zeros((8, 128), jnp.float32)

    def turn(tile, shift):
        shift %= 128
        return tile if shift == 0 else pltpu.roll(tile, shift, 1)

    def slide(tile, shift):
        return pltpu.roll(tile, shift % 8, 0)

    def lanes(h):
        return slice(h * 128, h * 128 + 128)

    def collide(f, kind, relax, inflow, wanted, inside=None):
        rho = functools.reduce(jnp.add, f)
        u = []
        for axis in range(3):
            plus = [f[i] for i in range(19) if VELOCITIES[i][axis] == 1]
            minus = [f[i] for i in range(19) if VELOCITIES[i][axis] == -1]
            u.append(functools.reduce(jnp.add, plus) - functools.reduce(jnp.add, minus))
        wall, fluid = kind < 0.5, jnp.logical_and(kind > 0.5, kind < 1.5)
        inlet, outlet = jnp.logical_and(kind > 1.5, kind < 2.5), kind > 2.5
        r = jnp.where(outlet, one, rho)
        v = [jnp.where(inlet, inflow[a], u[a]) for a in range(3)]
        take = jnp.where(wall, zero, jnp.where(fluid, relax, one))
        keep = one - take
        if inside is not None:
            take, keep = take * inside, keep * inside
        usq = v[0] * v[0] + v[1] * v[1] + v[2] * v[2]
        common = r - 1.5 * usq
        post = {}
        if 0 in wanted:
            post[0] = keep * f[0] + take * (WEIGHTS[0] * common)
        for i in range(1, 19, 2):
            if i not in wanted and i + 1 not in wanted:
                continue
            along = None
            for a in range(3):
                if VELOCITIES[i][a] != 0:
                    term = v[a] if VELOCITIES[i][a] == 1 else -v[a]
                    along = term if along is None else along + term
            even = WEIGHTS[i] * (common + 4.5 * along * along)
            odd = (3.0 * WEIGHTS[i]) * along
            if i in wanted:
                post[i] = keep * jnp.where(wall, f[i + 1], f[i]) + take * (even + odd)
            if i + 1 in wanted:
                post[i + 1] = keep * jnp.where(wall, f[i], f[i + 1]) + take * (even - odd)
        return post

    small = [m for m in MESSAGES if m[0] in ("z", "l")]
    small = sorted(small, key=lambda m: -sum(map(abs, m[1])))
    rows = sorted([m for m in MESSAGES if m[0] == "y"], key=lambda m: -abs(m[1][0]))
    everything = small + [m for m in MESSAGES if m[0] in ("xp", "xb", "xa")] + rows

    def start(found):
        for m in found:
            copy_of(m).start()

    def origin_starts(found):
        there = [m for m in found if min(m[1]) >= 0 and all(sizes[a] > 1 for a in range(3) if m[1][a] == 1)]
        if there:
            @pl.when(here_origin)
            def _():
                start(there)

    def all_to(d):
        start([m for m in everything if m[1] == d])

    @pl.when(before > 0)
    def _():
        pl.semaphore_wait(barrier, before)

    def answer(d, which):
        pl.semaphore_signal(entered.at[which], inc=1, device_id=target(d), device_id_type=MESH)

    @pl.when(here_origin)
    def _():
        for d in DIRECTIONS:
            if min(d) >= 0 and all(sizes[a] > 1 for a in range(3) if d[a] == 1):
                answer(d, 1)

    @pl.when(jnp.logical_not(here_origin))
    def _():
        for d in DIRECTIONS:
            if not upward(d):
                @pl.when(earlier(d))
                def _():
                    answer(d, 0)

    for p in (1, 0):
        await_tiles(48, load_sem.at[p])
        block[POS[KIND], 2 + p] = kinds[p].astype(jnp.float32)
        if p == 1:
            origin_starts([("xp", (1, 0, 0))])
        for h in (0, 1):
            z = lanes(h)
            post = collide(
                [field[i, p, :, z] for i in range(19)],
                block[POS[KIND], 2 + p, :, z],
                block[POS[RELAX], 2 + p, :, z],
                [block[POS[INFLOW + a], 2 + p, :, z] for a in range(3)],
                range(19),
            )
            for i in range(19):
                block[POS[i], 2 + p, :, z] = post[i]
        if p == 1:
            origin_starts([("xb", (1, 0, 0))])

    def column(j, p, at):
        return block[POS[j], 2 + p, :, lanes(at // 128)], at % 128

    for s in (1, -1):
        tile = zero
        for g, (j, depth) in enumerate(COLS[s]):
            for p in (0, 1):
                value, at = column(j, p, 256 - depth if s == 1 else depth - 1)
                to = 4 * g + p + VEL[j][0] + 1
                tile = jnp.where(lane_id == to, turn(value, to - at), tile)
        zs[side(s)] = tile
    tile = zero
    for s in (1, -1):
        for g, j in enumerate(LOCAL[s]):
            for p in (0, 1):
                value, at = column(j, p, 0 if s == 1 else 255)
                to = LOCAL_LANE[s] + 4 * g + p + VEL[j][0] + 1
                tile = jnp.where(lane_id == to, turn(value, to - at), tile)
    ls[0] = tile
    origin_starts(small + [("xa", (1, 0, 0))])
    for s in (1, -1):
        for g, (j, depth) in enumerate(ROWS[s]):
            for p in (0, 1):
                row = 8 - depth if s == 1 else depth - 1
                k = row_place(g, p)
                ys[side(s), k : k + 1] = block[POS[j], 2 + p, row : row + 1]
    origin_starts(rows)

    after = 0
    for d in DIRECTIONS:
        if upward(d):
            after = after + later(d).astype(jnp.int32)

    @pl.when(jnp.logical_not(here_origin))
    def _():
        for d in DIRECTIONS:
            if not upward(d):
                @pl.when(earlier(d))
                def _():
                    all_to(d)

        @pl.when(after > 0)
        def _():
            pl.semaphore_wait(entered.at[0], after)

        for d in DIRECTIONS:
            if upward(d):
                @pl.when(later(d))
                def _():
                    all_to(d)
        for d in DIRECTIONS:
            if max(d) < 1:
                @pl.when(later(d))
                def _():
                    pl.semaphore_wait(entered.at[1], 1)
                    all_to(d)

    await_present([m for m in MESSAGES if m[1][0] != 1], opposite, recv_sem.at[1])

    group_id = lane_id // 4
    lane_cx = jnp.where(group_id < 5, -1, jnp.where(group_id < 19, 0, 1))
    lane_cx = jnp.where(group_id >= 24, jnp.where(group_id < 25, -1, jnp.where(group_id < 28, 0, 1)), lane_cx)
    source = lane_id % 4 - 1 - lane_cx

    def merge(steps_x):
        straight, shifted = {}, {}
        for s in (1, -1):
            merged = {}
            for dy in STEPS:
                parts = {}
                for dx in steps_x:
                    local = ls[0] if dx == 0 and dy == 0 else lr[dx + 1, dy + 1]
                    if s == -1:
                        local = turn(local, 32)
                    part = jnp.where(lane_id >= 96, local, zr[side(s), dx + 1, dy + 1])
                    parts[dx] = turn(part, -2 * dx)
                whole = jnp.where(source > 1, parts[-1], parts[0])
                merged[dy] = jnp.where(source < 0, parts[1], whole) if 1 in parts else whole
            below, own, above = merged[1], merged[0], merged[-1]
            top, bottom = row_id == 0, row_id == 7
            straight[s, 0] = own
            straight[s, 1] = jnp.where(top, slide(below, 1), slide(own, 1))
            straight[s, -1] = jnp.where(bottom, slide(above, -1), slide(own, -1))
            shifted[s, 0] = jnp.where(top, slide(below, 1), slide(above, -1))
            shifted[s, 1] = jnp.where(top, slide(below, 2), own)
            shifted[s, -1] = jnp.where(bottom, slide(above, -2), own)
        return straight, shifted

    def y_moved(value, sign, edge_row):
        edge = 0 if sign == 1 else 7
        return [jnp.where(row_id == edge, edge_row[h], slide(value[h], sign)) for h in (0, 1)]

    def z_moved(value, sign, edge_tile):
        rolled = [turn(v, sign) for v in value]
        if sign == 1:
            at = lane_id == 0
            return [jnp.where(at, edge_tile, rolled[0]), jnp.where(at, rolled[0], rolled[1])]
        at = lane_id == 127
        return [jnp.where(at, rolled[1], rolled[0]), jnp.where(at, edge_tile, rolled[1])]

    def edge_lane(sign):
        return 0 if sign == 1 else 127

    def incoming_row(s, j, depth, plane):
        p = plane - VEL[j][0]
        dx = 1 if p < 0 else -1 if p > 1 else 0
        k = row_place(ROWS[s].index((j, depth)), p + 2 * dx)
        return [yr[side(s), dx + 1, k : k + 1, lanes(h)] for h in (0, 1)]

    def presence(axis, sign):
        return exists[axis, sign].astype(jnp.float32)

    def collide_plane(plane, straight):
        for i in range(19):
            cx, cy, cz = VELOCITIES[i]
            value = [block[POS[i], plane - cx + 2, :, lanes(h)] for h in (0, 1)]
            if cy != 0:
                value = y_moved(value, cy, incoming_row(cy, i, 1, plane))
            if cz != 0:
                at = 4 * COLS[cz].index((i, 1)) + plane + 1
                value = z_moved(value, cz, turn(straight[cz, cy], edge_lane(cz) - at))
            for h in (0, 1):
                first[i, plane + 1, :, lanes(h)] = value[h]
        inside, wanted = None, range(19)
        if plane == -1:
            inside, wanted = one * presence(0, -1), [i for i in range(19) if VELOCITIES[i][0] == 1]
        if plane == 2:
            inside, wanted = one * presence(0, 1), [i for i in range(19) if VELOCITIES[i][0] == -1]
        for h in (0, 1):
            z = lanes(h)
            post = collide(
                [first[i, plane + 1, :, z] for i in range(19)],
                block[POS[KIND], plane + 2, :, z],
                block[POS[RELAX], plane + 2, :, z],
                [block[POS[INFLOW + a], plane + 2, :, z] for a in range(3)],
                wanted, inside,
            )
            for i in wanted:
                second[i, plane + 1, :, z] = post[i]

    partial, _ = merge((-1, 0))
    for plane in (1, 2):
        collide_plane(plane, partial)
    await_present([m for m in MESSAGES if m[1][0] == 1], opposite, recv_sem.at[0])
    straight, shifted = merge(STEPS)
    for plane in (-1, 0):
        collide_plane(plane, straight)

    lowest, highest = row_id % 4 == 0, row_id % 4 == 3
    beside = jnp.where(lowest, presence(0, -1), jnp.where(highest, presence(0, 1), one))
    outside = beside * jnp.where(row_id < 4, presence(1, -1), presence(1, 1))
    edges = {}
    for s in (1, -1):
        for cy in STEPS:
            tile = shifted[s, cy]
            tile = jnp.where(row_id < 4, tile[0:1], turn(jnp.broadcast_to(tile[7:8], (8, 128)), 4))
            aligned = tile
            for r in range(1, 8):
                aligned = jnp.where(row_id == r, turn(tile, -r), aligned)
            edges[s, cy] = aligned
    for j in FIELDS:
        cx, cy, cz = VEL[j]
        for s in (1, -1):
            for plane in NEAR:
                k = 4 * side(s) + plane + 1
                if cy == -s:
                    row = 0 if s == 1 else 7
                    row_tile[j, k : k + 1] = block[POS[j], plane - cx + 2, row : row + 1]
                else:
                    value = incoming_row(s, j, 1 if cy == 0 else 2, plane)
                    for h in (0, 1):
                        row_tile[j, k : k + 1, lanes(h)] = value[h]
    for i in range(19):
        cx, cy, cz = VELOCITIES[i]
        if cz != 0:
            value = [row_tile[i, :, lanes(h)] for h in (0, 1)]
            at = 4 * COLS[cz].index((i, 1))
            value = z_moved(value, cz, turn(edges[cz, cy], edge_lane(cz) - at))
            for h in (0, 1):
                row_tile[i, :, lanes(h)] = value[h]
    moving_y = [i for i in range(19) if VELOCITIES[i][1] != 0]
    for h in (0, 1):
        f = [row_tile[j, :, lanes(h)] for j in FIELDS]
        post = collide(f[:19], f[KIND], f[RELAX], f[INFLOW : INFLOW + 3], moving_y, outside)
        for i in moving_y:
            row_post[i, :, lanes(h)] = post[i]

    def column_tile(j):
        _, cy, cz = VEL[j]
        tile = None
        for s in (1, -1):
            if cz == -s:
                at = 96 + 4 * LOCAL[s].index(j)
            else:
                at = 4 * COLS[s].index((j, 1 if cz == 0 else 2))
            for outer, parts in ((0, straight), (8, shifted)):
                start = outer + 4 * side(s)
                part = turn(parts[s, cy], start - at)
                here = jnp.logical_and(lane_id >= start, lane_id < start + 4)
                tile = part if tile is None else jnp.where(here, part, tile)
        return tile

    lowest, highest = lane_id % 4 == 0, lane_id % 4 == 3
    beside = jnp.where(lowest, presence(0, -1), jnp.where(highest, presence(0, 1), one))
    outside = beside * jnp.where(lane_id % 8 < 4, presence(2, -1), presence(2, 1))
    beyond = jnp.where(row_id == 0, presence(1, -1), presence(1, 1))
    outside = outside * jnp.where(lane_id < 8, one, beyond)
    f = [column_tile(j) for j in FIELDS]
    moving_z = [i for i in range(19) if VELOCITIES[i][2] != 0]
    column_post = collide(f[:19], f[KIND], f[RELAX], f[INFLOW : INFLOW + 3], moving_z, outside)

    for p in (0, 1):
        acc = [[None, None] for _ in range(4)]
        for i in range(19):
            c = cx, cy, cz = VELOCITIES[i]
            plane = p - cx
            value = [second[i, plane + 1, :, lanes(h)] for h in (0, 1)]
            if cy != 0:
                k = 4 * side(cy) + plane + 1
                value = y_moved(value, cy, [row_post[i, k : k + 1, lanes(h)] for h in (0, 1)])
            if cz != 0:
                at = 4 * side(cz) + plane + 1
                edge = turn(column_post[i], edge_lane(cz) - at)
                if cy != 0:
                    corner = turn(column_post[i], edge_lane(cz) - at - 8)
                    edge = jnp.where(row_id == (0 if cy == 1 else 7), corner, slide(edge, cy))
                value = z_moved(value, cz, edge)
            for h in (0, 1):
                acc[0][h] = value[h] if acc[0][h] is None else acc[0][h] + value[h]
                for a in range(3):
                    if c[a] != 0:
                        old = zero if acc[1 + a][h] is None else acc[1 + a][h]
                        acc[1 + a][h] = old + value[h] if c[a] == 1 else old - value[h]
        for h in (0, 1):
            for k in range(4):
                out_ref[k, p, :, lanes(h)] = acc[k][h]

    await_present(MESSAGES, lambda d: d, send_sem.at[0])


def finish(sums_ref, rho_hbm, mom_hbm, sems):
    copies = [
        pltpu.make_async_copy(sums_ref.at[0], rho_hbm, sems.at[0]),
        pltpu.make_async_copy(sums_ref.at[1:4], mom_hbm, sems.at[1]),
    ]
    for copy in copies:
        copy.start()
    for copy in copies:
        copy.wait()


def solution(mesh):
    sizes = tuple(mesh.shape[a] for a in AXES)

    def shards(dist, site_kinds, relax, inflow):
        f32 = jnp.float32
        shape = site_kinds.shape
        sums = pl.pallas_call(
            functools.partial(kernel, sizes),
            out_shape=pltpu.VMEM((4,) + shape, f32),
            in_specs=[pl.BlockSpec(memory_space=pl.ANY)] * 4,
            out_specs=pl.BlockSpec(memory_space=pltpu.VMEM),
            scratch_shapes=[
                pltpu.VMEM((19,) + shape, f32),
                pltpu.VMEM(shape, jnp.int32),
                pltpu.VMEM((24, 6, 8, 256), f32),
                pltpu.VMEM((2, 48, 256), f32),
                pltpu.VMEM((2, 3, 48, 256), f32),
                pltpu.VMEM((2, 8, 128), f32),
                pltpu.VMEM((2, 3, 3, 8, 128), f32),
                pltpu.VMEM((1, 8, 128), f32),
                pltpu.VMEM((3, 3, 8, 128), f32),
                pltpu.VMEM((19, 4, 8, 256), f32),
                pltpu.VMEM((19, 4, 8, 256), f32),
                pltpu.VMEM((24, 8, 256), f32),
                pltpu.VMEM((19, 8, 256), f32),
                pltpu.VMEM((sum(map(tiles, MESSAGES)), 8, 128), f32),
                pltpu.SemaphoreType.DMA((2,)),
                pltpu.SemaphoreType.DMA((1,)),
                pltpu.SemaphoreType.DMA((2,)),
                pltpu.SemaphoreType.REGULAR((2,)),
            ],
            compiler_params=pltpu.CompilerParams(collective_id=0, has_side_effects=True),
        )(dist, site_kinds, relax, inflow)
        return pl.pallas_call(
            finish,
            out_shape=(
                jax.ShapeDtypeStruct(shape, f32),
                jax.ShapeDtypeStruct((3,) + shape, f32),
            ),
            in_specs=[pl.BlockSpec(memory_space=pltpu.VMEM)],
            out_specs=(pl.BlockSpec(memory_space=pl.ANY), pl.BlockSpec(memory_space=pl.ANY)),
            scratch_shapes=[pltpu.SemaphoreType.DMA((2,))],
        )(pltpu.with_memory_space_constraint(sums, pltpu.VMEM))

    return jax.shard_map(
        shards,
        mesh=mesh,
        in_specs=(
            P(None, "gx", "gy", "gz"),
            P("gx", "gy", "gz"),
            P("gx", "gy", "gz"),
            P(None, "gx", "gy", "gz"),
        ),
        out_specs=(P("gx", "gy", "gz"), P(None, "gx", "gy", "gz")),
        check_vma=False,
    )
```

```python
import functools
import itertools

import jax
import jax.numpy as jnp
from jax import lax
from jax.experimental import pallas as pl
from jax.experimental.pallas import tpu as pltpu
from jax.sharding import PartitionSpec as P

VELOCITIES = [
    (0, 0, 0),
    (1, 0, 0),
    (-1, 0, 0),
    (0, 1, 0),
    (0, -1, 0),
    (0, 0, 1),
    (0, 0, -1),
    (1, 1, 0),
    (-1, -1, 0),
    (1, -1, 0),
    (-1, 1, 0),
    (1, 0, 1),
    (-1, 0, -1),
    (1, 0, -1),
    (-1, 0, 1),
    (0, 1, 1),
    (0, -1, -1),
    (0, 1, -1),
    (0, -1, 1),
]
WEIGHTS = [1.0 / 3.0] + [1.0 / 18.0] * 6 + [1.0 / 36.0] * 12
AXES = ("gx", "gy", "gz")
MESH = pl.DeviceIdType.MESH

KIND, RELAX, INFLOW = 19, 20, 21
VEL = VELOCITIES + [(0, 0, 0)] * 5
FIELDS = range(24)
ORDER = sorted(FIELDS, key=lambda j: (-VEL[j][0], j))
POS = [ORDER.index(j) for j in FIELDS]
STEPS = (-1, 0, 1)
DIRECTIONS = [(x, y, z) for x in STEPS for y in STEPS for z in STEPS if (x, y, z) != (0, 0, 0)]
NEAR = (-1, 0, 1, 2)


def groups(axis, sign):
    found = [(j, 1) for j in FIELDS if VEL[j][axis] in (0, sign)]
    found += [(j, 2) for j in FIELDS if VEL[j][axis] == sign]
    return sorted(found, key=lambda pair: VEL[pair[0]][0])


ROWS = {s: groups(1, s) for s in (1, -1)}
COLS = {s: groups(2, s) for s in (1, -1)}
LOCAL = {s: sorted([j for j in FIELDS if VEL[j][2] == -s], key=lambda j: VEL[j][0]) for s in (1, -1)}
LOCAL_LANE = {1: 96, -1: 64}
LEVEL = [i for i in range(19) if VELOCITIES[i][0] == 0]
FACE_ROWS = {s: [i for i in LEVEL if VELOCITIES[i][1] == -s] for s in (1, -1)}


def side(sign):
    return 0 if sign == 1 else 1


def opposite(direction):
    return tuple(-s for s in direction)


def upward(d):
    return next(s for s in (d[0], d[2], d[1]) if s != 0) == 1


def row_place(g, p):
    if g < 5:
        return 2 * g + p
    if g < 19:
        return 10 + 14 * p + g - 5
    return 38 + 2 * (g - 19) + p


def messages():
    found = []
    for d in DIRECTIONS:
        dx, dy, dz = d
        if dy == 0 and dz == 0:
            found += [("xp", d), ("xs", d), ("xa", d)]
        if dz == 0 and dy != 0:
            found.append(("y", d))
        if dz != 0:
            found.append(("z", d))
        else:
            found.append(("l", d))
    return found


MESSAGES = messages()


def tiles(m):
    if m[0] == "y":
        return 12 if m[1][0] == 0 else 6
    return {"xp": 10, "xs": 8, "xa": 20, "z": 1, "l": 1}[m[0]]


def kernel(
    sizes, dist_hbm, kinds_hbm, relax_hbm, inflow_hbm, out_ref,
    field, kinds, block, xs, xr, ys, yr, zs, zr, ls, lr, first, second, row_tile, row_post,
    size_ref, load_sem, send_sem, recv_sem, entered,
):
    me = tuple(lax.axis_index(a) for a in AXES)
    exists = {}
    for axis in range(3):
        exists[axis, 1] = me[axis] < sizes[axis] - 1
        exists[axis, -1] = me[axis] > 0

    def has(direction):
        parts = [exists[a, s] for a, s in enumerate(direction) if s != 0]
        return functools.reduce(jnp.logical_and, parts)

    def target(direction):
        return tuple(m + s for m, s in zip(me, direction))

    for p in (1, 0):
        group = [
            pltpu.make_async_copy(kinds_hbm.at[p], kinds.at[p], load_sem.at[p]),
            pltpu.make_async_copy(relax_hbm.at[p], block.at[POS[RELAX], 2 + p], load_sem.at[p]),
            pltpu.make_async_copy(
                inflow_hbm.at[:, p], block.at[POS[INFLOW] : POS[INFLOW] + 3, 2 + p], load_sem.at[p]
            ),
            pltpu.make_async_copy(dist_hbm.at[:, p], field.at[:, p], load_sem.at[p]),
        ]
        for copy in group:
            copy.start()

    def is_origin(place):
        return jnp.logical_and(place[0] == 0, jnp.logical_and(place[1] == 0, place[2] == 0))

    here_origin = is_origin(me)

    def later(d):
        if upward(d):
            return jnp.logical_and(has(d), jnp.logical_not(here_origin))
        if max(d) == 1:
            return None
        return is_origin(target(d))

    def earlier(d):
        if upward(d):
            return jnp.logical_and(has(d), here_origin)
        if max(d) == 1:
            return has(d)
        return jnp.logical_and(has(d), jnp.logical_not(is_origin(target(d))))

    barrier = pltpu.get_barrier_semaphore()
    for d in DIRECTIONS:
        if later(d) is not None:
            @pl.when(later(d))
            def _():
                pl.semaphore_signal(barrier, inc=1, device_id=target(d), device_id_type=MESH)
    before = 0
    for d in DIRECTIONS:
        before = before + earlier(d).astype(jnp.int32)

    def ends(m):
        kind, (dx, dy, dz) = m
        if kind == "xa":
            at, mine, theirs = (slice(0, 5), slice(2, 4), slice(0, 2)) if dx == 1 else (slice(19, 24), slice(2, 4), slice(4, 6))
            return block.at[at, mine], block.at[at, theirs]
        if kind == "xp":
            mine, theirs = (3, 1) if dx == 1 else (2, 4)
            return block.at[14:19, mine : mine + 1], block.at[14:19, theirs : theirs + 1]
        if kind == "xs":
            return xs.at[side(dx)], xr.at[side(dx)]
        if kind == "y":
            rows = {0: slice(0, 48), 1: slice(24, 48), -1: slice(0, 24)}[dx]
            return ys.at[side(dy), rows], yr.at[side(dy), dx + 1, rows]
        if kind == "z":
            return zs.at[side(dz)], zr.at[side(dz), dx + 1, dy + 1]
        return ls.at[0], lr.at[dx + 1, dy + 1]

    def copy_of(m):
        src, dst = ends(m)
        return pltpu.make_async_remote_copy(
            src_ref=src, dst_ref=dst, send_sem=send_sem.at[0], recv_sem=recv_sem.at[side(m[1][0])],
            device_id=target(m[1]), device_id_type=MESH,
        )

    def await_tiles(count, sem):
        part = size_ref.at[0:count]
        pltpu.make_async_copy(part, part, sem).wait()

    def await_present(found, toward, sem):
        count = 0
        for m in found:
            count = count + tiles(m) * has(toward(m[1])).astype(jnp.int32)
        sums = set()
        for touched in itertools.product(((), (1,), (-1,), (1, -1)), repeat=3):
            known = [m for m in found if not any(v in touched[a] for a, v in enumerate(toward(m[1])))]
            sums.add(sum(map(tiles, known)))
        for total in sorted(sums - {0}):
            @pl.when(count == total)
            def _():
                await_tiles(total, sem)

    for m in MESSAGES:
        @pl.when(jnp.logical_not(has(opposite(m[1]))))
        def _():
            dst = ends(m)[1]
            dst[...] = jnp.zeros(dst.shape, jnp.float32)

    row_id = lax.broadcasted_iota(jnp.int32, (8, 128), 0)
    lane_id = lax.broadcasted_iota(jnp.int32, (8, 128), 1)
    one = jnp.ones((8, 128), jnp.float32)
    zero = jnp.zeros((8, 128), jnp.float32)

    def turn(tile, shift):
        shift %= 128
        return tile if shift == 0 else pltpu.roll(tile, shift, 1)

    def slide(tile, shift):
        return pltpu.roll(tile, shift % 8, 0)

    def lanes(h):
        return slice(h * 128, h * 128 + 128)

    def y_moved(value, sign, edge_row):
        edge = 0 if sign == 1 else 7
        return [jnp.where(row_id == edge, edge_row[h], slide(value[h], sign)) for h in (0, 1)]

    def z_moved(value, sign, edge_tile):
        rolled = [turn(v, sign) for v in value]
        if sign == 1:
            at = lane_id == 0
            return [jnp.where(at, edge_tile, rolled[0]), jnp.where(at, rolled[0], rolled[1])]
        at = lane_id == 127
        return [jnp.where(at, rolled[1], rolled[0]), jnp.where(at, edge_tile, rolled[1])]

    def edge_lane(sign):
        return 0 if sign == 1 else 127

    def collide(f, kind, relax, inflow, wanted, inside=None, level=None):
        present = [i for i in range(19) if f[i] is not None]
        rho = functools.reduce(jnp.add, [f[i] for i in present])
        u = []
        for axis in range(3):
            plus = [f[i] for i in present if VELOCITIES[i][axis] == 1]
            minus = [f[i] for i in present if VELOCITIES[i][axis] == -1]
            u.append(functools.reduce(jnp.add, plus) - functools.reduce(jnp.add, minus))
        if level is not None:
            rho, u = rho + level[0], [u[0], u[1] + level[1], u[2] + level[2]]
        wall, fluid = kind < 0.5, jnp.logical_and(kind > 0.5, kind < 1.5)
        inlet, outlet = jnp.logical_and(kind > 1.5, kind < 2.5), kind > 2.5
        r = jnp.where(outlet, one, rho)
        v = [jnp.where(inlet, inflow[a], u[a]) for a in range(3)]
        take = jnp.where(wall, zero, jnp.where(fluid, relax, one))
        keep = one - take
        if inside is not None:
            take, keep = take * inside, keep * inside
        usq = v[0] * v[0] + v[1] * v[1] + v[2] * v[2]
        common = r - 1.5 * usq
        post = {}
        if 0 in wanted:
            post[0] = keep * f[0] + take * (WEIGHTS[0] * common)
        for i in range(1, 19, 2):
            if i not in wanted and i + 1 not in wanted:
                continue
            along = None
            for a in range(3):
                if VELOCITIES[i][a] != 0:
                    term = v[a] if VELOCITIES[i][a] == 1 else -v[a]
                    along = term if along is None else along + term
            even = WEIGHTS[i] * (common + 4.5 * along * along)
            odd = (3.0 * WEIGHTS[i]) * along
            if i in wanted:
                post[i] = keep * jnp.where(wall, f[i + 1], f[i]) + take * (even + odd)
            if i + 1 in wanted:
                post[i + 1] = keep * jnp.where(wall, f[i], f[i + 1]) + take * (even - odd)
        return post

    small = [m for m in MESSAGES if m[0] in ("z", "l")]
    small = sorted(small, key=lambda m: -sum(map(abs, m[1])))
    rows = sorted([m for m in MESSAGES if m[0] == "y"], key=lambda m: -abs(m[1][0]))
    everything = small + [m for m in MESSAGES if m[0] in ("xp", "xs", "xa")] + rows

    def start(found):
        for m in found:
            copy_of(m).start()

    def origin_starts(found):
        there = [m for m in found if min(m[1]) >= 0 and all(sizes[a] > 1 for a in range(3) if m[1][a] == 1)]
        if there:
            @pl.when(here_origin)
            def _():
                start(there)

    def all_to(d):
        start([m for m in everything if m[1] == d])

    def add_level(sums, i, value):
        for n, factor in enumerate((1, VELOCITIES[i][1], VELOCITIES[i][2])):
            for h in (0, 1):
                if factor != 0:
                    sums[n][h] = sums[n][h] + value[h] if factor == 1 else sums[n][h] - value[h]

    def sum_level(dx):
        p = 1 if dx == 1 else 0
        sums = [[zero, zero] for _ in range(3)]
        for i in LEVEL:
            _, cy, cz = VELOCITIES[i]
            value = [block[POS[i], 2 + p, :, lanes(h)] for h in (0, 1)]
            if cy != 0:
                value = y_moved(value, cy, [zero, zero])
            if cz != 0:
                value = z_moved(value, cz, zero)
            add_level(sums, i, value)
        for h in (0, 1):
            for n in range(3):
                xs[side(dx), n, :, lanes(h)] = sums[n][h]
            xs[side(dx), 3, :, lanes(h)] = zero
        for s in (1, -1):
            for n, j in enumerate(FACE_ROWS[s]):
                k, row = 3 * side(s) + n, 0 if s == 1 else 7
                xs[side(dx), 3, k : k + 1] = block[POS[j], 2 + p, row : row + 1]

    @pl.when(before > 0)
    def _():
        pl.semaphore_wait(barrier, before)

    def answer(d, which):
        pl.semaphore_signal(entered.at[which], inc=1, device_id=target(d), device_id_type=MESH)

    @pl.when(here_origin)
    def _():
        for d in DIRECTIONS:
            if min(d) >= 0 and all(sizes[a] > 1 for a in range(3) if d[a] == 1):
                answer(d, 1)

    @pl.when(jnp.logical_not(here_origin))
    def _():
        for d in DIRECTIONS:
            if not upward(d):
                @pl.when(earlier(d))
                def _():
                    answer(d, 0)

    for p in (1, 0):
        await_tiles(48, load_sem.at[p])
        block[POS[KIND], 2 + p] = kinds[p].astype(jnp.float32)
        if p == 1:
            origin_starts([("xp", (1, 0, 0))])
        for h in (0, 1):
            z = lanes(h)
            post = collide(
                [field[i, p, :, z] for i in range(19)],
                block[POS[KIND], 2 + p, :, z],
                block[POS[RELAX], 2 + p, :, z],
                [block[POS[INFLOW + a], 2 + p, :, z] for a in range(3)],
                range(19),
            )
            for i in range(19):
                block[POS[i], 2 + p, :, z] = post[i]
        if p == 1:
            sum_level(1)
            origin_starts([("xs", (1, 0, 0))])

    for s in (1, -1):
        for g, (j, depth) in enumerate(ROWS[s]):
            for p in (0, 1):
                row = 8 - depth if s == 1 else depth - 1
                k = row_place(g, p)
                ys[side(s), k : k + 1] = block[POS[j], 2 + p, row : row + 1]
    origin_starts([("y", (0, 1, 0))])

    def column(j, p, at):
        return block[POS[j], 2 + p, :, lanes(at // 128)], at % 128

    for s in (1, -1):
        tile = zero
        for g, (j, depth) in enumerate(COLS[s]):
            for p in (0, 1):
                value, at = column(j, p, 256 - depth if s == 1 else depth - 1)
                to = 4 * g + p + VEL[j][0] + 1
                tile = jnp.where(lane_id == to, turn(value, to - at), tile)
        zs[side(s)] = tile
    tile = zero
    for s in (1, -1):
        for g, j in enumerate(LOCAL[s]):
            for p in (0, 1):
                value, at = column(j, p, 0 if s == 1 else 255)
                to = LOCAL_LANE[s] + 4 * g + p + VEL[j][0] + 1
                tile = jnp.where(lane_id == to, turn(value, to - at), tile)
    ls[0] = tile
    origin_starts(small + [("xa", (1, 0, 0))])
    origin_starts([m for m in rows if m[1] != (0, 1, 0)])
    sum_level(-1)

    after = 0
    for d in DIRECTIONS:
        if upward(d):
            after = after + later(d).astype(jnp.int32)

    @pl.when(jnp.logical_not(here_origin))
    def _():
        for d in DIRECTIONS:
            if not upward(d):
                @pl.when(earlier(d))
                def _():
                    all_to(d)

        @pl.when(after > 0)
        def _():
            pl.semaphore_wait(entered.at[0], after)

        for d in DIRECTIONS:
            if upward(d):
                @pl.when(later(d))
                def _():
                    all_to(d)
        for d in DIRECTIONS:
            if max(d) < 1:
                @pl.when(later(d))
                def _():
                    pl.semaphore_wait(entered.at[1], 1)
                    all_to(d)

    await_present([m for m in MESSAGES if m[1][0] != 1], opposite, recv_sem.at[1])

    group_id = lane_id // 4
    lane_cx = jnp.where(group_id < 5, -1, jnp.where(group_id < 19, 0, 1))
    lane_cx = jnp.where(group_id >= 24, jnp.where(group_id < 25, -1, jnp.where(group_id < 28, 0, 1)), lane_cx)
    source = lane_id % 4 - 1 - lane_cx

    def merge(steps_x):
        straight, shifted = {}, {}
        for s in (1, -1):
            merged = {}
            for dy in STEPS:
                parts = {}
                for dx in steps_x:
                    local = ls[0] if dx == 0 and dy == 0 else lr[dx + 1, dy + 1]
                    if s == -1:
                        local = turn(local, 32)
                    part = jnp.where(lane_id >= 96, local, zr[side(s), dx + 1, dy + 1])
                    parts[dx] = turn(part, -2 * dx)
                whole = jnp.where(source > 1, parts[-1], parts[0])
                merged[dy] = jnp.where(source < 0, parts[1], whole) if 1 in parts else whole
            below, own, above = merged[1], merged[0], merged[-1]
            top, bottom = row_id == 0, row_id == 7
            straight[s, 0] = own
            straight[s, 1] = jnp.where(top, slide(below, 1), slide(own, 1))
            straight[s, -1] = jnp.where(bottom, slide(above, -1), slide(own, -1))
            shifted[s, 0] = jnp.where(top, slide(below, 1), slide(above, -1))
            shifted[s, 1] = jnp.where(top, slide(below, 2), own)
            shifted[s, -1] = jnp.where(bottom, slide(above, -2), own)
        return straight, shifted

    def incoming_row(s, j, depth, plane):
        p = plane - VEL[j][0]
        dx = 1 if p < 0 else -1 if p > 1 else 0
        k = row_place(ROWS[s].index((j, depth)), p + 2 * dx)
        return [yr[side(s), dx + 1, k : k + 1, lanes(h)] for h in (0, 1)]

    def presence(axis, sign):
        return exists[axis, sign].astype(jnp.float32)

    def collide_plane(plane, straight):
        near = plane in (-1, 2)
        sums = None
        if near:
            ends_at = 0 if plane == -1 else 1
            sums = [[xr[ends_at, n, :, lanes(h)] for h in (0, 1)] for n in range(3)]
        for i in range(19):
            cx, cy, cz = VELOCITIES[i]
            if near and cx == 0:
                value = [zero, zero]
            else:
                value = [block[POS[i], plane - cx + 2, :, lanes(h)] for h in (0, 1)]
            if cy != 0:
                value = y_moved(value, cy, incoming_row(cy, i, 1, plane))
            if cz != 0:
                at = 4 * COLS[cz].index((i, 1)) + plane + 1
                value = z_moved(value, cz, turn(straight[cz, cy], edge_lane(cz) - at))
            if near and cx == 0:
                add_level(sums, i, value)
                continue
            for h in (0, 1):
                first[i, plane + 1, :, lanes(h)] = value[h]
        inside, wanted = None, range(19)
        if plane == -1:
            inside, wanted = one * presence(0, -1), [i for i in range(19) if VELOCITIES[i][0] == 1]
        if plane == 2:
            inside, wanted = one * presence(0, 1), [i for i in range(19) if VELOCITIES[i][0] == -1]
        for h in (0, 1):
            z = lanes(h)
            post = collide(
                [None if near and i in LEVEL else first[i, plane + 1, :, z] for i in range(19)],
                block[POS[KIND], plane + 2, :, z],
                block[POS[RELAX], plane + 2, :, z],
                [block[POS[INFLOW + a], plane + 2, :, z] for a in range(3)],
                wanted, inside, [sums[n][h] for n in range(3)] if near else None,
            )
            for i in wanted:
                second[i, plane + 1, :, z] = post[i]

    def fill_rows(from_below):
        for j in FIELDS:
            cx, cy, cz = VEL[j]
            for s in (1, -1):
                for plane in NEAR:
                    if (plane - cx < 0) != from_below:
                        continue
                    k = 4 * side(s) + plane + 1
                    if cy == -s and cx == 0 and plane in (-1, 2):
                        n = 3 * side(s) + FACE_ROWS[s].index(j)
                        row_tile[j, k : k + 1] = xr[0 if plane == -1 else 1, 3, n : n + 1]
                    elif cy == -s:
                        row = 0 if s == 1 else 7
                        row_tile[j, k : k + 1] = block[POS[j], plane - cx + 2, row : row + 1]
                    else:
                        value = incoming_row(s, j, 1 if cy == 0 else 2, plane)
                        for h in (0, 1):
                            row_tile[j, k : k + 1, lanes(h)] = value[h]

    partial, _ = merge((-1, 0))
    fill_rows(False)
    for plane in (1, 2):
        collide_plane(plane, partial)
    await_present([m for m in MESSAGES if m[1][0] == 1], opposite, recv_sem.at[0])
    fill_rows(True)
    straight, shifted = merge(STEPS)
    for plane in (-1, 0):
        collide_plane(plane, straight)

    lowest, highest = row_id % 4 == 0, row_id % 4 == 3
    beside = jnp.where(lowest, presence(0, -1), jnp.where(highest, presence(0, 1), one))
    outside = beside * jnp.where(row_id < 4, presence(1, -1), presence(1, 1))
    edges = {}
    for s in (1, -1):
        for cy in STEPS:
            tile = shifted[s, cy]
            tile = jnp.where(row_id < 4, tile[0:1], turn(jnp.broadcast_to(tile[7:8], (8, 128)), 4))
            aligned = tile
            for r in range(1, 8):
                aligned = jnp.where(row_id == r, turn(tile, -r), aligned)
            edges[s, cy] = aligned
    for i in range(19):
        cx, cy, cz = VELOCITIES[i]
        if cz != 0:
            value = [row_tile[i, :, lanes(h)] for h in (0, 1)]
            at = 4 * COLS[cz].index((i, 1))
            value = z_moved(value, cz, turn(edges[cz, cy], edge_lane(cz) - at))
            for h in (0, 1):
                row_tile[i, :, lanes(h)] = value[h]
    moving_y = [i for i in range(19) if VELOCITIES[i][1] != 0]
    for h in (0, 1):
        f = [row_tile[j, :, lanes(h)] for j in FIELDS]
        post = collide(f[:19], f[KIND], f[RELAX], f[INFLOW : INFLOW + 3], moving_y, outside)
        for i in moving_y:
            row_post[i, :, lanes(h)] = post[i]

    def column_tile(j):
        _, cy, cz = VEL[j]
        tile = None
        for s in (1, -1):
            if cz == -s:
                at = 96 + 4 * LOCAL[s].index(j)
            else:
                at = 4 * COLS[s].index((j, 1 if cz == 0 else 2))
            for outer, parts in ((0, straight), (8, shifted)):
                start = outer + 4 * side(s)
                part = turn(parts[s, cy], start - at)
                here = jnp.logical_and(lane_id >= start, lane_id < start + 4)
                tile = part if tile is None else jnp.where(here, part, tile)
        return tile

    lowest, highest = lane_id % 4 == 0, lane_id % 4 == 3
    beside = jnp.where(lowest, presence(0, -1), jnp.where(highest, presence(0, 1), one))
    outside = beside * jnp.where(lane_id % 8 < 4, presence(2, -1), presence(2, 1))
    beyond = jnp.where(row_id == 0, presence(1, -1), presence(1, 1))
    outside = outside * jnp.where(lane_id < 8, one, beyond)
    f = [column_tile(j) for j in FIELDS]
    moving_z = [i for i in range(19) if VELOCITIES[i][2] != 0]
    column_post = collide(f[:19], f[KIND], f[RELAX], f[INFLOW : INFLOW + 3], moving_z, outside)

    for p in (0, 1):
        acc = [[None, None] for _ in range(4)]
        for i in range(19):
            c = cx, cy, cz = VELOCITIES[i]
            plane = p - cx
            value = [second[i, plane + 1, :, lanes(h)] for h in (0, 1)]
            if cy != 0:
                k = 4 * side(cy) + plane + 1
                value = y_moved(value, cy, [row_post[i, k : k + 1, lanes(h)] for h in (0, 1)])
            if cz != 0:
                at = 4 * side(cz) + plane + 1
                edge = turn(column_post[i], edge_lane(cz) - at)
                if cy != 0:
                    corner = turn(column_post[i], edge_lane(cz) - at - 8)
                    edge = jnp.where(row_id == (0 if cy == 1 else 7), corner, slide(edge, cy))
                value = z_moved(value, cz, edge)
            for h in (0, 1):
                acc[0][h] = value[h] if acc[0][h] is None else acc[0][h] + value[h]
                for a in range(3):
                    if c[a] != 0:
                        old = zero if acc[1 + a][h] is None else acc[1 + a][h]
                        acc[1 + a][h] = old + value[h] if c[a] == 1 else old - value[h]
        for h in (0, 1):
            for k in range(4):
                out_ref[k, p, :, lanes(h)] = acc[k][h]

    await_present(MESSAGES, lambda d: d, send_sem.at[0])


def finish(sums_ref, rho_hbm, mom_hbm, sems):
    copies = [
        pltpu.make_async_copy(sums_ref.at[0], rho_hbm, sems.at[0]),
        pltpu.make_async_copy(sums_ref.at[1:4], mom_hbm, sems.at[1]),
    ]
    for copy in copies:
        copy.start()
    for copy in copies:
        copy.wait()


def solution(mesh):
    sizes = tuple(mesh.shape[a] for a in AXES)

    def shards(dist, site_kinds, relax, inflow):
        f32 = jnp.float32
        shape = site_kinds.shape
        sums = pl.pallas_call(
            functools.partial(kernel, sizes),
            out_shape=pltpu.VMEM((4,) + shape, f32),
            in_specs=[pl.BlockSpec(memory_space=pl.ANY)] * 4,
            out_specs=pl.BlockSpec(memory_space=pltpu.VMEM),
            scratch_shapes=[
                pltpu.VMEM((19,) + shape, f32),
                pltpu.VMEM(shape, jnp.int32),
                pltpu.VMEM((24, 6, 8, 256), f32),
                pltpu.VMEM((2, 4, 8, 256), f32),
                pltpu.VMEM((2, 4, 8, 256), f32),
                pltpu.VMEM((2, 48, 256), f32),
                pltpu.VMEM((2, 3, 48, 256), f32),
                pltpu.VMEM((2, 8, 128), f32),
                pltpu.VMEM((2, 3, 3, 8, 128), f32),
                pltpu.VMEM((1, 8, 128), f32),
                pltpu.VMEM((3, 3, 8, 128), f32),
                pltpu.VMEM((19, 4, 8, 256), f32),
                pltpu.VMEM((19, 4, 8, 256), f32),
                pltpu.VMEM((24, 8, 256), f32),
                pltpu.VMEM((19, 8, 256), f32),
                pltpu.VMEM((sum(map(tiles, MESSAGES)), 8, 128), f32),
                pltpu.SemaphoreType.DMA((2,)),
                pltpu.SemaphoreType.DMA((1,)),
                pltpu.SemaphoreType.DMA((2,)),
                pltpu.SemaphoreType.REGULAR((2,)),
            ],
            compiler_params=pltpu.CompilerParams(collective_id=0, has_side_effects=True),
        )(dist, site_kinds, relax, inflow)
        return pl.pallas_call(
            finish,
            out_shape=(
                jax.ShapeDtypeStruct(shape, f32),
                jax.ShapeDtypeStruct((3,) + shape, f32),
            ),
            in_specs=[pl.BlockSpec(memory_space=pltpu.VMEM)],
            out_specs=(pl.BlockSpec(memory_space=pl.ANY), pl.BlockSpec(memory_space=pl.ANY)),
            scratch_shapes=[pltpu.SemaphoreType.DMA((2,))],
        )(pltpu.with_memory_space_constraint(sums, pltpu.VMEM))

    return jax.shard_map(
        shards,
        mesh=mesh,
        in_specs=(
            P(None, "gx", "gy", "gz"),
            P("gx", "gy", "gz"),
            P("gx", "gy", "gz"),
            P(None, "gx", "gy", "gz"),
        ),
        out_specs=(P("gx", "gy", "gz"), P(None, "gx", "gy", "gz")),
        check_vma=False,
    )
```

```python
import functools
import itertools

import jax
import jax.numpy as jnp
from jax import lax
from jax.experimental import pallas as pl
from jax.experimental.pallas import tpu as pltpu
from jax.sharding import PartitionSpec as P

VELOCITIES = [
    (0, 0, 0),
    (1, 0, 0),
    (-1, 0, 0),
    (0, 1, 0),
    (0, -1, 0),
    (0, 0, 1),
    (0, 0, -1),
    (1, 1, 0),
    (-1, -1, 0),
    (1, -1, 0),
    (-1, 1, 0),
    (1, 0, 1),
    (-1, 0, -1),
    (1, 0, -1),
    (-1, 0, 1),
    (0, 1, 1),
    (0, -1, -1),
    (0, 1, -1),
    (0, -1, 1),
]
WEIGHTS = [1.0 / 3.0] + [1.0 / 18.0] * 6 + [1.0 / 36.0] * 12
AXES = ("gx", "gy", "gz")
MESH = pl.DeviceIdType.MESH

KIND, OWN, INFLOW = 19, 20, 21
VEL = VELOCITIES + [(0, 0, 0)] * 4
FIELDS = range(23)
ORDER = sorted(FIELDS, key=lambda j: (-VEL[j][0], j))
POS = [ORDER.index(j) for j in FIELDS]
STEPS = (-1, 0, 1)
DIRECTIONS = [(x, y, z) for x in STEPS for y in STEPS for z in STEPS if (x, y, z) != (0, 0, 0)]
NEAR = (-1, 0, 1, 2)


def groups(axis, sign):
    found = [(j, 1) for j in FIELDS if VEL[j][axis] in (0, sign)]
    found += [(j, 2) for j in FIELDS if VEL[j][axis] == sign]
    return sorted(found, key=lambda pair: VEL[pair[0]][0])


ROWS = {s: groups(1, s) for s in (1, -1)}
COLS = {s: groups(2, s) for s in (1, -1)}
LOCAL = {s: sorted([j for j in FIELDS if VEL[j][2] == -s], key=lambda j: VEL[j][0]) for s in (1, -1)}
LOCAL_LANE = {1: 96, -1: 64}
LEVEL = [i for i in range(19) if VELOCITIES[i][0] == 0]
FACE_ROWS = {s: [i for i in LEVEL if VELOCITIES[i][1] == -s] for s in (1, -1)}


def side(sign):
    return 0 if sign == 1 else 1


def opposite(direction):
    return tuple(-s for s in direction)


def upward(d):
    return next(s for s in (d[0], d[2], d[1]) if s != 0) == 1


def row_place(g, p):
    if g < 5:
        return 2 * g + p
    if g < 18:
        return 10 + 14 * p + g - 5
    return 38 + 2 * (g - 18) + p


def messages():
    found = []
    for d in DIRECTIONS:
        dx, dy, dz = d
        if dy == 0 and dz == 0:
            found += [("xp", d), ("xs", d), ("xa", d)]
        if dz == 0 and dy != 0:
            found.append(("y", d))
        if dz != 0:
            found.append(("z", d))
        else:
            found.append(("l", d))
    return found


MESSAGES = messages()


def tiles(m):
    if m[0] == "y":
        return 12 if m[1][0] == 0 else 6
    return {"xp": 8, "xs": 8, "xa": 20, "z": 1, "l": 1}[m[0]]


def kernel(
    sizes, dist_hbm, kinds_hbm, relax_hbm, inflow_hbm, out_ref,
    field, kinds, either, block, xs, xr, ys, yr, zs, zr, ls, lr, first, second, row_tile, row_post,
    size_ref, load_sem, send_sem, recv_sem, entered,
):
    me = tuple(lax.axis_index(a) for a in AXES)
    exists = {}
    for axis in range(3):
        exists[axis, 1] = me[axis] < sizes[axis] - 1
        exists[axis, -1] = me[axis] > 0

    def has(direction):
        parts = [exists[a, s] for a, s in enumerate(direction) if s != 0]
        return functools.reduce(jnp.logical_and, parts)

    def target(direction):
        return tuple(m + s for m, s in zip(me, direction))

    for p in (1, 0):
        group = [
            pltpu.make_async_copy(kinds_hbm.at[p], kinds.at[p], load_sem.at[p]),
            pltpu.make_async_copy(relax_hbm.at[p], either.at[0, p], load_sem.at[p]),
            pltpu.make_async_copy(inflow_hbm.at[0, p], either.at[1, p], load_sem.at[p]),
            pltpu.make_async_copy(
                inflow_hbm.at[1:3, p], block.at[POS[INFLOW] : POS[INFLOW] + 2, 2 + p], load_sem.at[p]
            ),
            pltpu.make_async_copy(dist_hbm.at[:, p], field.at[:, p], load_sem.at[p]),
        ]
        for copy in group:
            copy.start()

    def is_origin(place):
        return jnp.logical_and(place[0] == 0, jnp.logical_and(place[1] == 0, place[2] == 0))

    here_origin = is_origin(me)

    def later(d):
        if upward(d):
            return jnp.logical_and(has(d), jnp.logical_not(here_origin))
        if max(d) == 1:
            return None
        return is_origin(target(d))

    def earlier(d):
        if upward(d):
            return jnp.logical_and(has(d), here_origin)
        if max(d) == 1:
            return has(d)
        return jnp.logical_and(has(d), jnp.logical_not(is_origin(target(d))))

    barrier = pltpu.get_barrier_semaphore()
    for d in DIRECTIONS:
        if later(d) is not None:
            @pl.when(later(d))
            def _():
                pl.semaphore_signal(barrier, inc=1, device_id=target(d), device_id_type=MESH)
    before = 0
    for d in DIRECTIONS:
        before = before + earlier(d).astype(jnp.int32)

    def ends(m):
        kind, (dx, dy, dz) = m
        if kind == "xa":
            at, mine, theirs = (slice(0, 5), slice(2, 4), slice(0, 2)) if dx == 1 else (slice(18, 23), slice(2, 4), slice(4, 6))
            return block.at[at, mine], block.at[at, theirs]
        if kind == "xp":
            mine, theirs = (3, 1) if dx == 1 else (2, 4)
            return block.at[14:18, mine : mine + 1], block.at[14:18, theirs : theirs + 1]
        if kind == "xs":
            return xs.at[side(dx)], xr.at[side(dx)]
        if kind == "y":
            rows = {0: slice(0, 48), 1: slice(24, 48), -1: slice(0, 24)}[dx]
            return ys.at[side(dy), rows], yr.at[side(dy), dx + 1, rows]
        if kind == "z":
            return zs.at[side(dz)], zr.at[side(dz), dx + 1, dy + 1]
        return ls.at[0], lr.at[dx + 1, dy + 1]

    def copy_of(m):
        src, dst = ends(m)
        return pltpu.make_async_remote_copy(
            src_ref=src, dst_ref=dst, send_sem=send_sem.at[0], recv_sem=recv_sem.at[side(m[1][0])],
            device_id=target(m[1]), device_id_type=MESH,
        )

    def await_tiles(count, sem):
        part = size_ref.at[0:count]
        pltpu.make_async_copy(part, part, sem).wait()

    def await_present(found, toward, sem):
        count = 0
        for m in found:
            count = count + tiles(m) * has(toward(m[1])).astype(jnp.int32)
        sums = set()
        for touched in itertools.product(((), (1,), (-1,), (1, -1)), repeat=3):
            known = [m for m in found if not any(v in touched[a] for a, v in enumerate(toward(m[1])))]
            sums.add(sum(map(tiles, known)))
        for total in sorted(sums - {0}):
            @pl.when(count == total)
            def _():
                await_tiles(total, sem)

    for m in MESSAGES:
        @pl.when(jnp.logical_not(has(opposite(m[1]))))
        def _():
            dst = ends(m)[1]
            dst[...] = jnp.zeros(dst.shape, jnp.float32)

    row_id = lax.broadcasted_iota(jnp.int32, (8, 128), 0)
    lane_id = lax.broadcasted_iota(jnp.int32, (8, 128), 1)
    one = jnp.ones((8, 128), jnp.float32)
    zero = jnp.zeros((8, 128), jnp.float32)

    def turn(tile, shift):
        shift %= 128
        return tile if shift == 0 else pltpu.roll(tile, shift, 1)

    def slide(tile, shift):
        return pltpu.roll(tile, shift % 8, 0)

    def lanes(h):
        return slice(h * 128, h * 128 + 128)

    def y_moved(value, sign, edge_row):
        edge = 0 if sign == 1 else 7
        return [jnp.where(row_id == edge, edge_row[h], slide(value[h], sign)) for h in (0, 1)]

    def z_moved(value, sign, edge_tile):
        rolled = [turn(v, sign) for v in value]
        if sign == 1:
            at = lane_id == 0
            return [jnp.where(at, edge_tile, rolled[0]), jnp.where(at, rolled[0], rolled[1])]
        at = lane_id == 127
        return [jnp.where(at, rolled[1], rolled[0]), jnp.where(at, edge_tile, rolled[1])]

    def edge_lane(sign):
        return 0 if sign == 1 else 127

    def collide(f, kind, own, inflow, wanted, inside=None, level=None):
        present = [i for i in range(19) if f[i] is not None]
        rho = functools.reduce(jnp.add, [f[i] for i in present])
        u = []
        for axis in range(3):
            plus = [f[i] for i in present if VELOCITIES[i][axis] == 1]
            minus = [f[i] for i in present if VELOCITIES[i][axis] == -1]
            u.append(functools.reduce(jnp.add, plus) - functools.reduce(jnp.add, minus))
        if level is not None:
            rho, u = rho + level[0], [u[0], u[1] + level[1], u[2] + level[2]]
        wall, fluid = kind < 0.5, jnp.logical_and(kind > 0.5, kind < 1.5)
        inlet, outlet = jnp.logical_and(kind > 1.5, kind < 2.5), kind > 2.5
        r = jnp.where(outlet, one, rho)
        v = [jnp.where(inlet, given, u[a]) for a, given in enumerate((own, inflow[0], inflow[1]))]
        take = jnp.where(wall, zero, jnp.where(fluid, own, one))
        keep = one - take
        if inside is not None:
            take, keep = take * inside, keep * inside
        usq = v[0] * v[0] + v[1] * v[1] + v[2] * v[2]
        common = r - 1.5 * usq
        post = {}
        if 0 in wanted:
            post[0] = keep * f[0] + take * (WEIGHTS[0] * common)
        for i in range(1, 19, 2):
            if i not in wanted and i + 1 not in wanted:
                continue
            along = None
            for a in range(3):
                if VELOCITIES[i][a] != 0:
                    term = v[a] if VELOCITIES[i][a] == 1 else -v[a]
                    along = term if along is None else along + term
            even = WEIGHTS[i] * (common + 4.5 * along * along)
            odd = (3.0 * WEIGHTS[i]) * along
            if i in wanted:
                post[i] = keep * jnp.where(wall, f[i + 1], f[i]) + take * (even + odd)
            if i + 1 in wanted:
                post[i + 1] = keep * jnp.where(wall, f[i], f[i + 1]) + take * (even - odd)
        return post

    small = [m for m in MESSAGES if m[0] in ("z", "l")]
    small = sorted(small, key=lambda m: -sum(map(abs, m[1])))
    rows = sorted([m for m in MESSAGES if m[0] == "y"], key=lambda m: -abs(m[1][0]))
    everything = small + [m for m in MESSAGES if m[0] in ("xp", "xs", "xa")] + rows

    def start(found):
        for m in found:
            copy_of(m).start()

    def origin_starts(found):
        there = [m for m in found if min(m[1]) >= 0 and all(sizes[a] > 1 for a in range(3) if m[1][a] == 1)]
        if there:
            @pl.when(here_origin)
            def _():
                start(there)

    def all_to(d):
        start([m for m in everything if m[1] == d])

    def add_level(sums, i, value):
        for n, factor in enumerate((1, VELOCITIES[i][1], VELOCITIES[i][2])):
            for h in (0, 1):
                if factor != 0:
                    sums[n][h] = sums[n][h] + value[h] if factor == 1 else sums[n][h] - value[h]

    def sum_level(dx):
        p = 1 if dx == 1 else 0
        sums = [[zero, zero] for _ in range(3)]
        for i in LEVEL:
            _, cy, cz = VELOCITIES[i]
            value = [block[POS[i], 2 + p, :, lanes(h)] for h in (0, 1)]
            if cy != 0:
                value = y_moved(value, cy, [zero, zero])
            if cz != 0:
                value = z_moved(value, cz, zero)
            add_level(sums, i, value)
        for h in (0, 1):
            for n in range(3):
                xs[side(dx), n, :, lanes(h)] = sums[n][h]
            xs[side(dx), 3, :, lanes(h)] = zero
        for s in (1, -1):
            for n, j in enumerate(FACE_ROWS[s]):
                k, row = 3 * side(s) + n, 0 if s == 1 else 7
                xs[side(dx), 3, k : k + 1] = block[POS[j], 2 + p, row : row + 1]

    @pl.when(before > 0)
    def _():
        pl.semaphore_wait(barrier, before)

    def answer(d, which):
        pl.semaphore_signal(entered.at[which], inc=1, device_id=target(d), device_id_type=MESH)

    @pl.when(here_origin)
    def _():
        for d in DIRECTIONS:
            if min(d) >= 0 and all(sizes[a] > 1 for a in range(3) if d[a] == 1):
                answer(d, 1)

    @pl.when(jnp.logical_not(here_origin))
    def _():
        for d in DIRECTIONS:
            if not upward(d):
                @pl.when(earlier(d))
                def _():
                    answer(d, 0)

    for p in (1, 0):
        await_tiles(48, load_sem.at[p])
        block[POS[KIND], 2 + p] = kinds[p].astype(jnp.float32)
        block[POS[OWN], 2 + p] = jnp.where(kinds[p] == 2, either[1, p], either[0, p])
        if p == 1:
            origin_starts([("xp", (1, 0, 0))])
        for h in (0, 1):
            z = lanes(h)
            post = collide(
                [field[i, p, :, z] for i in range(19)],
                block[POS[KIND], 2 + p, :, z],
                block[POS[OWN], 2 + p, :, z],
                [block[POS[INFLOW + a], 2 + p, :, z] for a in range(2)],
                range(19),
            )
            for i in range(19):
                block[POS[i], 2 + p, :, z] = post[i]

    for s in (1, -1):
        for g, (j, depth) in enumerate(ROWS[s]):
            for p in (0, 1):
                row = 8 - depth if s == 1 else depth - 1
                k = row_place(g, p)
                ys[side(s), k : k + 1] = block[POS[j], 2 + p, row : row + 1]
    origin_starts([("y", (0, 1, 0))])

    def column(j, p, at):
        return block[POS[j], 2 + p, :, lanes(at // 128)], at % 128

    tile = zero
    for s in (1, -1):
        for g, j in enumerate(LOCAL[s]):
            for p in (0, 1):
                value, at = column(j, p, 0 if s == 1 else 255)
                to = LOCAL_LANE[s] + 4 * g + p + VEL[j][0] + 1
                tile = jnp.where(lane_id == to, turn(value, to - at), tile)
    ls[0] = tile
    origin_starts([m for m in small if m[0] == "l"])
    sum_level(1)
    origin_starts([("xs", (1, 0, 0))])
    for s in (1, -1):
        tile = zero
        for g, (j, depth) in enumerate(COLS[s]):
            for p in (0, 1):
                value, at = column(j, p, 256 - depth if s == 1 else depth - 1)
                to = 4 * g + p + VEL[j][0] + 1
                tile = jnp.where(lane_id == to, turn(value, to - at), tile)
        zs[side(s)] = tile
    origin_starts([m for m in small if m[0] == "z"] + [("xa", (1, 0, 0))])
    origin_starts([m for m in rows if m[1] != (0, 1, 0)])
    sum_level(-1)

    after = 0
    for d in DIRECTIONS:
        if upward(d):
            after = after + later(d).astype(jnp.int32)

    @pl.when(jnp.logical_not(here_origin))
    def _():
        for d in DIRECTIONS:
            if not upward(d):
                @pl.when(earlier(d))
                def _():
                    all_to(d)

        @pl.when(after > 0)
        def _():
            pl.semaphore_wait(entered.at[0], after)

        for d in DIRECTIONS:
            if upward(d):
                @pl.when(later(d))
                def _():
                    all_to(d)
        for d in DIRECTIONS:
            if max(d) < 1:
                @pl.when(later(d))
                def _():
                    pl.semaphore_wait(entered.at[1], 1)
                    all_to(d)

    await_present([m for m in MESSAGES if m[1][0] != 1], opposite, recv_sem.at[1])

    group_id = lane_id // 4
    lane_cx = jnp.where(group_id < 5, -1, jnp.where(group_id < 18, 0, 1))
    lane_cx = jnp.where(group_id >= 24, jnp.where(group_id < 25, -1, jnp.where(group_id < 28, 0, 1)), lane_cx)
    source = lane_id % 4 - 1 - lane_cx

    def merge(steps_x):
        straight, shifted = {}, {}
        for s in (1, -1):
            merged = {}
            for dy in STEPS:
                parts = {}
                for dx in steps_x:
                    local = ls[0] if dx == 0 and dy == 0 else lr[dx + 1, dy + 1]
                    if s == -1:
                        local = turn(local, 32)
                    part = jnp.where(lane_id >= 96, local, zr[side(s), dx + 1, dy + 1])
                    parts[dx] = turn(part, -2 * dx)
                whole = jnp.where(source > 1, parts[-1], parts[0])
                merged[dy] = jnp.where(source < 0, parts[1], whole) if 1 in parts else whole
            below, own, above = merged[1], merged[0], merged[-1]
            top, bottom = row_id == 0, row_id == 7
            straight[s, 0] = own
            straight[s, 1] = jnp.where(top, slide(below, 1), slide(own, 1))
            straight[s, -1] = jnp.where(bottom, slide(above, -1), slide(own, -1))
            shifted[s, 0] = jnp.where(top, slide(below, 1), slide(above, -1))
            shifted[s, 1] = jnp.where(top, slide(below, 2), own)
            shifted[s, -1] = jnp.where(bottom, slide(above, -2), own)
        return straight, shifted

    def incoming_row(s, j, depth, plane):
        p = plane - VEL[j][0]
        dx = 1 if p < 0 else -1 if p > 1 else 0
        k = row_place(ROWS[s].index((j, depth)), p + 2 * dx)
        return [yr[side(s), dx + 1, k : k + 1, lanes(h)] for h in (0, 1)]

    def presence(axis, sign):
        return exists[axis, sign].astype(jnp.float32)

    def collide_plane(plane, straight):
        near = plane in (-1, 2)
        sums = None
        if near:
            ends_at = 0 if plane == -1 else 1
            sums = [[xr[ends_at, n, :, lanes(h)] for h in (0, 1)] for n in range(3)]
        for i in range(19):
            cx, cy, cz = VELOCITIES[i]
            if near and cx == 0:
                value = [zero, zero]
            else:
                value = [block[POS[i], plane - cx + 2, :, lanes(h)] for h in (0, 1)]
            if cy != 0:
                value = y_moved(value, cy, incoming_row(cy, i, 1, plane))
            if cz != 0:
                at = 4 * COLS[cz].index((i, 1)) + plane + 1
                value = z_moved(value, cz, turn(straight[cz, cy], edge_lane(cz) - at))
            if near and cx == 0:
                add_level(sums, i, value)
                continue
            for h in (0, 1):
                first[i, plane + 1, :, lanes(h)] = value[h]
        inside, wanted = None, range(19)
        if plane == -1:
            inside, wanted = one * presence(0, -1), [i for i in range(19) if VELOCITIES[i][0] == 1]
        if plane == 2:
            inside, wanted = one * presence(0, 1), [i for i in range(19) if VELOCITIES[i][0] == -1]
        for h in (0, 1):
            z = lanes(h)
            post = collide(
                [None if near and i in LEVEL else first[i, plane + 1, :, z] for i in range(19)],
                block[POS[KIND], plane + 2, :, z],
                block[POS[OWN], plane + 2, :, z],
                [block[POS[INFLOW + a], plane + 2, :, z] for a in range(2)],
                wanted, inside, [sums[n][h] for n in range(3)] if near else None,
            )
            for i in wanted:
                second[i, plane + 1, :, z] = post[i]

    def fill_rows(from_below):
        for j in FIELDS:
            cx, cy, cz = VEL[j]
            for s in (1, -1):
                for plane in NEAR:
                    if (plane - cx < 0) != from_below:
                        continue
                    k = 4 * side(s) + plane + 1
                    if cy == -s and cx == 0 and plane in (-1, 2):
                        n = 3 * side(s) + FACE_ROWS[s].index(j)
                        row_tile[j, k : k + 1] = xr[0 if plane == -1 else 1, 3, n : n + 1]
                    elif cy == -s:
                        row = 0 if s == 1 else 7
                        row_tile[j, k : k + 1] = block[POS[j], plane - cx + 2, row : row + 1]
                    else:
                        value = incoming_row(s, j, 1 if cy == 0 else 2, plane)
                        for h in (0, 1):
                            row_tile[j, k : k + 1, lanes(h)] = value[h]

    partial, _ = merge((-1, 0))
    fill_rows(False)
    for plane in (1, 2):
        collide_plane(plane, partial)
    await_present([m for m in MESSAGES if m[1][0] == 1], opposite, recv_sem.at[0])
    fill_rows(True)
    straight, shifted = merge(STEPS)
    for plane in (-1, 0):
        collide_plane(plane, straight)

    lowest, highest = row_id % 4 == 0, row_id % 4 == 3
    beside = jnp.where(lowest, presence(0, -1), jnp.where(highest, presence(0, 1), one))
    outside = beside * jnp.where(row_id < 4, presence(1, -1), presence(1, 1))
    edges = {}
    for s in (1, -1):
        for cy in STEPS:
            tile = shifted[s, cy]
            tile = jnp.where(row_id < 4, tile[0:1], turn(jnp.broadcast_to(tile[7:8], (8, 128)), 4))
            aligned = tile
            for r in range(1, 8):
                aligned = jnp.where(row_id == r, turn(tile, -r), aligned)
            edges[s, cy] = aligned
    for i in range(19):
        cx, cy, cz = VELOCITIES[i]
        if cz != 0:
            value = [row_tile[i, :, lanes(h)] for h in (0, 1)]
            at = 4 * COLS[cz].index((i, 1))
            value = z_moved(value, cz, turn(edges[cz, cy], edge_lane(cz) - at))
            for h in (0, 1):
                row_tile[i, :, lanes(h)] = value[h]
    moving_y = [i for i in range(19) if VELOCITIES[i][1] != 0]
    for h in (0, 1):
        f = [row_tile[j, :, lanes(h)] for j in FIELDS]
        post = collide(f[:19], f[KIND], f[OWN], f[INFLOW : INFLOW + 2], moving_y, outside)
        for i in moving_y:
            row_post[i, :, lanes(h)] = post[i]

    def column_tile(j):
        _, cy, cz = VEL[j]
        tile = None
        for s in (1, -1):
            if cz == -s:
                at = 96 + 4 * LOCAL[s].index(j)
            else:
                at = 4 * COLS[s].index((j, 1 if cz == 0 else 2))
            for outer, parts in ((0, straight), (8, shifted)):
                start = outer + 4 * side(s)
                part = turn(parts[s, cy], start - at)
                here = jnp.logical_and(lane_id >= start, lane_id < start + 4)
                tile = part if tile is None else jnp.where(here, part, tile)
        return tile

    lowest, highest = lane_id % 4 == 0, lane_id % 4 == 3
    beside = jnp.where(lowest, presence(0, -1), jnp.where(highest, presence(0, 1), one))
    outside = beside * jnp.where(lane_id % 8 < 4, presence(2, -1), presence(2, 1))
    beyond = jnp.where(row_id == 0, presence(1, -1), presence(1, 1))
    outside = outside * jnp.where(lane_id < 8, one, beyond)
    f = [column_tile(j) for j in FIELDS]
    moving_z = [i for i in range(19) if VELOCITIES[i][2] != 0]
    column_post = collide(f[:19], f[KIND], f[OWN], f[INFLOW : INFLOW + 2], moving_z, outside)

    for p in (0, 1):
        acc = [[None, None] for _ in range(4)]
        for i in range(19):
            c = cx, cy, cz = VELOCITIES[i]
            plane = p - cx
            value = [second[i, plane + 1, :, lanes(h)] for h in (0, 1)]
            if cy != 0:
                k = 4 * side(cy) + plane + 1
                value = y_moved(value, cy, [row_post[i, k : k + 1, lanes(h)] for h in (0, 1)])
            if cz != 0:
                at = 4 * side(cz) + plane + 1
                edge = turn(column_post[i], edge_lane(cz) - at)
                if cy != 0:
                    corner = turn(column_post[i], edge_lane(cz) - at - 8)
                    edge = jnp.where(row_id == (0 if cy == 1 else 7), corner, slide(edge, cy))
                value = z_moved(value, cz, edge)
            for h in (0, 1):
                acc[0][h] = value[h] if acc[0][h] is None else acc[0][h] + value[h]
                for a in range(3):
                    if c[a] != 0:
                        old = zero if acc[1 + a][h] is None else acc[1 + a][h]
                        acc[1 + a][h] = old + value[h] if c[a] == 1 else old - value[h]
        for h in (0, 1):
            for k in range(4):
                out_ref[k, p, :, lanes(h)] = acc[k][h]

    await_present(MESSAGES, lambda d: d, send_sem.at[0])


def finish(sums_ref, rho_hbm, mom_hbm, sems):
    copies = [
        pltpu.make_async_copy(sums_ref.at[0], rho_hbm, sems.at[0]),
        pltpu.make_async_copy(sums_ref.at[1:4], mom_hbm, sems.at[1]),
    ]
    for copy in copies:
        copy.start()
    for copy in copies:
        copy.wait()


def solution(mesh):
    sizes = tuple(mesh.shape[a] for a in AXES)

    def shards(dist, site_kinds, relax, inflow):
        f32 = jnp.float32
        shape = site_kinds.shape
        sums = pl.pallas_call(
            functools.partial(kernel, sizes),
            out_shape=pltpu.VMEM((4,) + shape, f32),
            in_specs=[pl.BlockSpec(memory_space=pl.ANY)] * 4,
            out_specs=pl.BlockSpec(memory_space=pltpu.VMEM),
            scratch_shapes=[
                pltpu.VMEM((19,) + shape, f32),
                pltpu.VMEM(shape, jnp.int32),
                pltpu.VMEM((2,) + shape, f32),
                pltpu.VMEM((23, 6, 8, 256), f32),
                pltpu.VMEM((2, 4, 8, 256), f32),
                pltpu.VMEM((2, 4, 8, 256), f32),
                pltpu.VMEM((2, 48, 256), f32),
                pltpu.VMEM((2, 3, 48, 256), f32),
                pltpu.VMEM((2, 8, 128), f32),
                pltpu.VMEM((2, 3, 3, 8, 128), f32),
                pltpu.VMEM((1, 8, 128), f32),
                pltpu.VMEM((3, 3, 8, 128), f32),
                pltpu.VMEM((19, 4, 8, 256), f32),
                pltpu.VMEM((19, 4, 8, 256), f32),
                pltpu.VMEM((23, 8, 256), f32),
                pltpu.VMEM((19, 8, 256), f32),
                pltpu.VMEM((sum(map(tiles, MESSAGES)), 8, 128), f32),
                pltpu.SemaphoreType.DMA((2,)),
                pltpu.SemaphoreType.DMA((1,)),
                pltpu.SemaphoreType.DMA((2,)),
                pltpu.SemaphoreType.REGULAR((2,)),
            ],
            compiler_params=pltpu.CompilerParams(collective_id=0, has_side_effects=True),
        )(dist, site_kinds, relax, inflow)
        return pl.pallas_call(
            finish,
            out_shape=(
                jax.ShapeDtypeStruct(shape, f32),
                jax.ShapeDtypeStruct((3,) + shape, f32),
            ),
            in_specs=[pl.BlockSpec(memory_space=pltpu.VMEM)],
            out_specs=(pl.BlockSpec(memory_space=pl.ANY), pl.BlockSpec(memory_space=pl.ANY)),
            scratch_shapes=[pltpu.SemaphoreType.DMA((2,))],
        )(pltpu.with_memory_space_constraint(sums, pltpu.VMEM))

    return jax.shard_map(
        shards,
        mesh=mesh,
        in_specs=(
            P(None, "gx", "gy", "gz"),
            P("gx", "gy", "gz"),
            P("gx", "gy", "gz"),
            P(None, "gx", "gy", "gz"),
        ),
        out_specs=(P("gx", "gy", "gz"), P(None, "gx", "gy", "gz")),
        check_vma=False,
    )
```

```python
import functools
import itertools

import jax
import jax.numpy as jnp
from jax import lax
from jax.experimental import pallas as pl
from jax.experimental.pallas import tpu as pltpu
from jax.sharding import PartitionSpec as P

VELOCITIES = [
    (0, 0, 0),
    (1, 0, 0),
    (-1, 0, 0),
    (0, 1, 0),
    (0, -1, 0),
    (0, 0, 1),
    (0, 0, -1),
    (1, 1, 0),
    (-1, -1, 0),
    (1, -1, 0),
    (-1, 1, 0),
    (1, 0, 1),
    (-1, 0, -1),
    (1, 0, -1),
    (-1, 0, 1),
    (0, 1, 1),
    (0, -1, -1),
    (0, 1, -1),
    (0, -1, 1),
]
WEIGHTS = [1.0 / 3.0] + [1.0 / 18.0] * 6 + [1.0 / 36.0] * 12
AXES = ("gx", "gy", "gz")
MESH = pl.DeviceIdType.MESH

KIND, OWN, INFLOW = 19, 20, 21
VEL = VELOCITIES + [(0, 0, 0)] * 4
FIELDS = range(23)
ORDER = sorted(FIELDS, key=lambda j: (-VEL[j][0], j))
POS = [ORDER.index(j) for j in FIELDS]
STEPS = (-1, 0, 1)
DIRECTIONS = [(x, y, z) for x in STEPS for y in STEPS for z in STEPS if (x, y, z) != (0, 0, 0)]
NEAR = (-1, 0, 1, 2)


def groups(axis, sign):
    found = [(j, 1) for j in FIELDS if VEL[j][axis] in (0, sign)]
    found += [(j, 2) for j in FIELDS if VEL[j][axis] == sign]
    return sorted(found, key=lambda pair: VEL[pair[0]][0])


ROWS = {s: groups(1, s) for s in (1, -1)}
COLS = {s: groups(2, s) for s in (1, -1)}
LOCAL = {s: sorted([j for j in FIELDS if VEL[j][2] == -s], key=lambda j: VEL[j][0]) for s in (1, -1)}
LOCAL_LANE = {1: 96, -1: 64}
LEVEL = [i for i in range(19) if VELOCITIES[i][0] == 0]
FACE_ROWS = {s: [i for i in LEVEL if VELOCITIES[i][1] == -s] for s in (1, -1)}


def side(sign):
    return 0 if sign == 1 else 1


def opposite(direction):
    return tuple(-s for s in direction)


def upward(d):
    return next(s for s in (d[0], d[2], d[1]) if s != 0) == 1


def row_place(g, p):
    if g < 5:
        return 2 * g + p
    if g < 18:
        return 10 + 14 * p + g - 5
    return 38 + 2 * (g - 18) + p


def messages():
    found = []
    for d in DIRECTIONS:
        dx, dy, dz = d
        if dy == 0 and dz == 0:
            found += [("xp", d), ("xs", d), ("xa", d)]
        if dz == 0 and dy != 0:
            found.append(("y", d))
        if dz != 0:
            found.append(("z", d))
        else:
            found.append(("l", d))
    return found


MESSAGES = messages()


def tiles(m):
    if m[0] == "y":
        return 12 if m[1][0] == 0 else 6
    return {"xp": 8, "xs": 8, "xa": 20, "z": 1, "l": 1}[m[0]]


def kernel(
    sizes, dist_hbm, kinds_hbm, relax_hbm, inflow_hbm, out_ref,
    field, kinds, either, block, xs, xr, ys, yr, zs, zr, ls, lr, first, second, row_tile, row_post,
    size_ref, load_sem, send_sem, recv_sem, entered,
):
    me = tuple(lax.axis_index(a) for a in AXES)
    exists = {}
    for axis in range(3):
        exists[axis, 1] = me[axis] < sizes[axis] - 1
        exists[axis, -1] = me[axis] > 0

    def has(direction):
        parts = [exists[a, s] for a, s in enumerate(direction) if s != 0]
        return functools.reduce(jnp.logical_and, parts)

    def target(direction):
        return tuple(m + s for m, s in zip(me, direction))

    for p in (1, 0):
        group = [
            pltpu.make_async_copy(kinds_hbm.at[p], kinds.at[p], load_sem.at[p]),
            pltpu.make_async_copy(relax_hbm.at[p], either.at[0, p], load_sem.at[p]),
            pltpu.make_async_copy(inflow_hbm.at[0, p], either.at[1, p], load_sem.at[p]),
            pltpu.make_async_copy(
                inflow_hbm.at[1:3, p], block.at[POS[INFLOW] : POS[INFLOW] + 2, 2 + p], load_sem.at[p]
            ),
            pltpu.make_async_copy(dist_hbm.at[:, p], field.at[:, p], load_sem.at[2 + p]),
        ]
        for copy in group:
            copy.start()

    def is_origin(place):
        return jnp.logical_and(place[0] == 0, jnp.logical_and(place[1] == 0, place[2] == 0))

    here_origin = is_origin(me)

    def later(d):
        if upward(d):
            return jnp.logical_and(has(d), jnp.logical_not(here_origin))
        if max(d) == 1:
            return None
        return is_origin(target(d))

    def earlier(d):
        if upward(d):
            return jnp.logical_and(has(d), here_origin)
        if max(d) == 1:
            return has(d)
        return jnp.logical_and(has(d), jnp.logical_not(is_origin(target(d))))

    barrier = pltpu.get_barrier_semaphore()
    for d in DIRECTIONS:
        if later(d) is not None:
            @pl.when(later(d))
            def _():
                pl.semaphore_signal(barrier, inc=1, device_id=target(d), device_id_type=MESH)
    before = 0
    for d in DIRECTIONS:
        before = before + earlier(d).astype(jnp.int32)

    def ends(m):
        kind, (dx, dy, dz) = m
        if kind == "xa":
            at, mine, theirs = (slice(0, 5), slice(2, 4), slice(0, 2)) if dx == 1 else (slice(18, 23), slice(2, 4), slice(4, 6))
            return block.at[at, mine], block.at[at, theirs]
        if kind == "xp":
            mine, theirs = (3, 1) if dx == 1 else (2, 4)
            return block.at[14:18, mine : mine + 1], block.at[14:18, theirs : theirs + 1]
        if kind == "xs":
            return xs.at[side(dx)], xr.at[side(dx)]
        if kind == "y":
            rows = {0: slice(0, 48), 1: slice(24, 48), -1: slice(0, 24)}[dx]
            return ys.at[side(dy), rows], yr.at[side(dy), dx + 1, rows]
        if kind == "z":
            return zs.at[side(dz)], zr.at[side(dz), dx + 1, dy + 1]
        return ls.at[0], lr.at[dx + 1, dy + 1]

    def copy_of(m):
        src, dst = ends(m)
        return pltpu.make_async_remote_copy(
            src_ref=src, dst_ref=dst, send_sem=send_sem.at[0], recv_sem=recv_sem.at[side(m[1][0])],
            device_id=target(m[1]), device_id_type=MESH,
        )

    def await_tiles(count, sem):
        part = size_ref.at[0:count]
        pltpu.make_async_copy(part, part, sem).wait()

    def await_present(found, toward, sem):
        count = 0
        for m in found:
            count = count + tiles(m) * has(toward(m[1])).astype(jnp.int32)
        sums = set()
        for touched in itertools.product(((), (1,), (-1,), (1, -1)), repeat=3):
            known = [m for m in found if not any(v in touched[a] for a, v in enumerate(toward(m[1])))]
            sums.add(sum(map(tiles, known)))
        for total in sorted(sums - {0}):
            @pl.when(count == total)
            def _():
                await_tiles(total, sem)

    for m in MESSAGES:
        @pl.when(jnp.logical_not(has(opposite(m[1]))))
        def _():
            dst = ends(m)[1]
            dst[...] = jnp.zeros(dst.shape, jnp.float32)

    row_id = lax.broadcasted_iota(jnp.int32, (8, 128), 0)
    lane_id = lax.broadcasted_iota(jnp.int32, (8, 128), 1)
    one = jnp.ones((8, 128), jnp.float32)
    zero = jnp.zeros((8, 128), jnp.float32)

    def turn(tile, shift):
        shift %= 128
        return tile if shift == 0 else pltpu.roll(tile, shift, 1)

    def slide(tile, shift):
        return pltpu.roll(tile, shift % 8, 0)

    def lanes(h):
        return slice(h * 128, h * 128 + 128)

    def y_moved(value, sign, edge_row):
        edge = 0 if sign == 1 else 7
        return [jnp.where(row_id == edge, edge_row[h], slide(value[h], sign)) for h in (0, 1)]

    def z_moved(value, sign, edge_tile):
        rolled = [turn(v, sign) for v in value]
        if sign == 1:
            at = lane_id == 0
            return [jnp.where(at, edge_tile, rolled[0]), jnp.where(at, rolled[0], rolled[1])]
        at = lane_id == 127
        return [jnp.where(at, rolled[1], rolled[0]), jnp.where(at, edge_tile, rolled[1])]

    def edge_lane(sign):
        return 0 if sign == 1 else 127

    def collide(f, kind, own, inflow, wanted, inside=None, level=None):
        present = [i for i in range(19) if f[i] is not None]
        rho = functools.reduce(jnp.add, [f[i] for i in present])
        u = []
        for axis in range(3):
            plus = [f[i] for i in present if VELOCITIES[i][axis] == 1]
            minus = [f[i] for i in present if VELOCITIES[i][axis] == -1]
            u.append(functools.reduce(jnp.add, plus) - functools.reduce(jnp.add, minus))
        if level is not None:
            rho, u = rho + level[0], [u[0], u[1] + level[1], u[2] + level[2]]
        wall, fluid = kind < 0.5, jnp.logical_and(kind > 0.5, kind < 1.5)
        inlet, outlet = jnp.logical_and(kind > 1.5, kind < 2.5), kind > 2.5
        r = jnp.where(outlet, one, rho)
        v = [jnp.where(inlet, given, u[a]) for a, given in enumerate((own, inflow[0], inflow[1]))]
        take = jnp.where(wall, zero, jnp.where(fluid, own, one))
        keep = one - take
        if inside is not None:
            take, keep = take * inside, keep * inside
        usq = v[0] * v[0] + v[1] * v[1] + v[2] * v[2]
        common = r - 1.5 * usq
        post = {}
        if 0 in wanted:
            post[0] = keep * f[0] + take * (WEIGHTS[0] * common)
        for i in range(1, 19, 2):
            if i not in wanted and i + 1 not in wanted:
                continue
            along = None
            for a in range(3):
                if VELOCITIES[i][a] != 0:
                    term = v[a] if VELOCITIES[i][a] == 1 else -v[a]
                    along = term if along is None else along + term
            even = WEIGHTS[i] * (common + 4.5 * along * along)
            odd = (3.0 * WEIGHTS[i]) * along
            if i in wanted:
                post[i] = keep * jnp.where(wall, f[i + 1], f[i]) + take * (even + odd)
            if i + 1 in wanted:
                post[i + 1] = keep * jnp.where(wall, f[i], f[i + 1]) + take * (even - odd)
        return post

    small = [m for m in MESSAGES if m[0] in ("z", "l")]
    small = sorted(small, key=lambda m: -sum(map(abs, m[1])))
    rows = sorted([m for m in MESSAGES if m[0] == "y"], key=lambda m: -abs(m[1][0]))
    everything = small + [m for m in MESSAGES if m[0] in ("xp", "xs", "xa")] + rows

    def start(found):
        for m in found:
            copy_of(m).start()

    def origin_starts(found):
        there = [m for m in found if min(m[1]) >= 0 and all(sizes[a] > 1 for a in range(3) if m[1][a] == 1)]
        if there:
            @pl.when(here_origin)
            def _():
                start(there)

    def all_to(d):
        start([m for m in everything if m[1] == d])

    def add_level(sums, i, value):
        for n, factor in enumerate((1, VELOCITIES[i][1], VELOCITIES[i][2])):
            for h in (0, 1):
                if factor != 0:
                    sums[n][h] = sums[n][h] + value[h] if factor == 1 else sums[n][h] - value[h]

    def sum_level(dx):
        p = 1 if dx == 1 else 0
        sums = [[zero, zero] for _ in range(3)]
        for i in LEVEL:
            _, cy, cz = VELOCITIES[i]
            value = [block[POS[i], 2 + p, :, lanes(h)] for h in (0, 1)]
            if cy != 0:
                value = y_moved(value, cy, [zero, zero])
            if cz != 0:
                value = z_moved(value, cz, zero)
            add_level(sums, i, value)
        for h in (0, 1):
            for n in range(3):
                xs[side(dx), n, :, lanes(h)] = sums[n][h]
            xs[side(dx), 3, :, lanes(h)] = zero
        for s in (1, -1):
            for n, j in enumerate(FACE_ROWS[s]):
                k, row = 3 * side(s) + n, 0 if s == 1 else 7
                xs[side(dx), 3, k : k + 1] = block[POS[j], 2 + p, row : row + 1]

    @pl.when(before > 0)
    def _():
        pl.semaphore_wait(barrier, before)

    def answer(d, which):
        pl.semaphore_signal(entered.at[which], inc=1, device_id=target(d), device_id_type=MESH)

    @pl.when(here_origin)
    def _():
        for d in DIRECTIONS:
            if min(d) >= 0 and all(sizes[a] > 1 for a in range(3) if d[a] == 1):
                answer(d, 1)

    @pl.when(jnp.logical_not(here_origin))
    def _():
        for d in DIRECTIONS:
            if not upward(d):
                @pl.when(earlier(d))
                def _():
                    answer(d, 0)

    for p in (1, 0):
        await_tiles(10, load_sem.at[p])
        block[POS[KIND], 2 + p] = kinds[p].astype(jnp.float32)
        block[POS[OWN], 2 + p] = jnp.where(kinds[p] == 2, either[1, p], either[0, p])
        if p == 1:
            origin_starts([("xp", (1, 0, 0))])
        await_tiles(38, load_sem.at[2 + p])
        for h in (0, 1):
            z = lanes(h)
            post = collide(
                [field[i, p, :, z] for i in range(19)],
                block[POS[KIND], 2 + p, :, z],
                block[POS[OWN], 2 + p, :, z],
                [block[POS[INFLOW + a], 2 + p, :, z] for a in range(2)],
                range(19),
            )
            for i in range(19):
                block[POS[i], 2 + p, :, z] = post[i]
        if p == 1:
            sum_level(1)
            origin_starts([("xs", (1, 0, 0))])

    for s in (1, -1):
        for g, (j, depth) in enumerate(ROWS[s]):
            for p in (0, 1):
                row = 8 - depth if s == 1 else depth - 1
                k = row_place(g, p)
                ys[side(s), k : k + 1] = block[POS[j], 2 + p, row : row + 1]
    origin_starts([("y", (0, 1, 0))])

    def column(j, p, at):
        return block[POS[j], 2 + p, :, lanes(at // 128)], at % 128

    tile = zero
    for s in (1, -1):
        for g, j in enumerate(LOCAL[s]):
            for p in (0, 1):
                value, at = column(j, p, 0 if s == 1 else 255)
                to = LOCAL_LANE[s] + 4 * g + p + VEL[j][0] + 1
                tile = jnp.where(lane_id == to, turn(value, to - at), tile)
    ls[0] = tile
    origin_starts([m for m in small if m[0] == "l"])
    for s in (1, -1):
        tile = zero
        for g, (j, depth) in enumerate(COLS[s]):
            for p in (0, 1):
                value, at = column(j, p, 256 - depth if s == 1 else depth - 1)
                to = 4 * g + p + VEL[j][0] + 1
                tile = jnp.where(lane_id == to, turn(value, to - at), tile)
        zs[side(s)] = tile
    origin_starts([m for m in small if m[0] == "z"] + [("xa", (1, 0, 0))])
    origin_starts([m for m in rows if m[1] != (0, 1, 0)])
    sum_level(-1)

    after = 0
    for d in DIRECTIONS:
        if upward(d):
            after = after + later(d).astype(jnp.int32)

    @pl.when(jnp.logical_not(here_origin))
    def _():
        for d in DIRECTIONS:
            if not upward(d):
                @pl.when(earlier(d))
                def _():
                    all_to(d)

        @pl.when(after > 0)
        def _():
            pl.semaphore_wait(entered.at[0], after)

        for d in DIRECTIONS:
            if upward(d):
                @pl.when(later(d))
                def _():
                    all_to(d)
        for d in DIRECTIONS:
            if max(d) < 1:
                @pl.when(later(d))
                def _():
                    pl.semaphore_wait(entered.at[1], 1)
                    all_to(d)

    await_present([m for m in MESSAGES if m[1][0] != 1], opposite, recv_sem.at[1])

    group_id = lane_id // 4
    lane_cx = jnp.where(group_id < 5, -1, jnp.where(group_id < 18, 0, 1))
    lane_cx = jnp.where(group_id >= 24, jnp.where(group_id < 25, -1, jnp.where(group_id < 28, 0, 1)), lane_cx)
    source = lane_id % 4 - 1 - lane_cx

    def merge(steps_x):
        straight, shifted = {}, {}
        for s in (1, -1):
            merged = {}
            for dy in STEPS:
                parts = {}
                for dx in steps_x:
                    local = ls[0] if dx == 0 and dy == 0 else lr[dx + 1, dy + 1]
                    if s == -1:
                        local = turn(local, 32)
                    part = jnp.where(lane_id >= 96, local, zr[side(s), dx + 1, dy + 1])
                    parts[dx] = turn(part, -2 * dx)
                whole = jnp.where(source > 1, parts[-1], parts[0])
                merged[dy] = jnp.where(source < 0, parts[1], whole) if 1 in parts else whole
            below, own, above = merged[1], merged[0], merged[-1]
            top, bottom = row_id == 0, row_id == 7
            straight[s, 0] = own
            straight[s, 1] = jnp.where(top, slide(below, 1), slide(own, 1))
            straight[s, -1] = jnp.where(bottom, slide(above, -1), slide(own, -1))
            shifted[s, 0] = jnp.where(top, slide(below, 1), slide(above, -1))
            shifted[s, 1] = jnp.where(top, slide(below, 2), own)
            shifted[s, -1] = jnp.where(bottom, slide(above, -2), own)
        return straight, shifted

    def incoming_row(s, j, depth, plane):
        p = plane - VEL[j][0]
        dx = 1 if p < 0 else -1 if p > 1 else 0
        k = row_place(ROWS[s].index((j, depth)), p + 2 * dx)
        return [yr[side(s), dx + 1, k : k + 1, lanes(h)] for h in (0, 1)]

    def presence(axis, sign):
        return exists[axis, sign].astype(jnp.float32)

    def collide_plane(plane, straight):
        near = plane in (-1, 2)
        sums = None
        if near:
            ends_at = 0 if plane == -1 else 1
            sums = [[xr[ends_at, n, :, lanes(h)] for h in (0, 1)] for n in range(3)]
        for i in range(19):
            cx, cy, cz = VELOCITIES[i]
            if near and cx == 0:
                value = [zero, zero]
            else:
                value = [block[POS[i], plane - cx + 2, :, lanes(h)] for h in (0, 1)]
            if cy != 0:
                value = y_moved(value, cy, incoming_row(cy, i, 1, plane))
            if cz != 0:
                at = 4 * COLS[cz].index((i, 1)) + plane + 1
                value = z_moved(value, cz, turn(straight[cz, cy], edge_lane(cz) - at))
            if near and cx == 0:
                add_level(sums, i, value)
                continue
            for h in (0, 1):
                first[i, plane + 1, :, lanes(h)] = value[h]
        inside, wanted = None, range(19)
        if plane == -1:
            inside, wanted = one * presence(0, -1), [i for i in range(19) if VELOCITIES[i][0] == 1]
        if plane == 2:
            inside, wanted = one * presence(0, 1), [i for i in range(19) if VELOCITIES[i][0] == -1]
        for h in (0, 1):
            z = lanes(h)
            post = collide(
                [None if near and i in LEVEL else first[i, plane + 1, :, z] for i in range(19)],
                block[POS[KIND], plane + 2, :, z],
                block[POS[OWN], plane + 2, :, z],
                [block[POS[INFLOW + a], plane + 2, :, z] for a in range(2)],
                wanted, inside, [sums[n][h] for n in range(3)] if near else None,
            )
            for i in wanted:
                second[i, plane + 1, :, z] = post[i]

    def fill_rows(from_below):
        for j in FIELDS:
            cx, cy, cz = VEL[j]
            for s in (1, -1):
                for plane in NEAR:
                    if (plane - cx < 0) != from_below:
                        continue
                    k = 4 * side(s) + plane + 1
                    if cy == -s and cx == 0 and plane in (-1, 2):
                        n = 3 * side(s) + FACE_ROWS[s].index(j)
                        row_tile[j, k : k + 1] = xr[0 if plane == -1 else 1, 3, n : n + 1]
                    elif cy == -s:
                        row = 0 if s == 1 else 7
                        row_tile[j, k : k + 1] = block[POS[j], plane - cx + 2, row : row + 1]
                    else:
                        value = incoming_row(s, j, 1 if cy == 0 else 2, plane)
                        for h in (0, 1):
                            row_tile[j, k : k + 1, lanes(h)] = value[h]

    partial, _ = merge((-1, 0))
    fill_rows(False)
    for plane in (1, 2):
        collide_plane(plane, partial)
    await_present([m for m in MESSAGES if m[1][0] == 1], opposite, recv_sem.at[0])
    fill_rows(True)
    straight, shifted = merge(STEPS)
    for plane in (-1, 0):
        collide_plane(plane, straight)

    lowest, highest = row_id % 4 == 0, row_id % 4 == 3
    beside = jnp.where(lowest, presence(0, -1), jnp.where(highest, presence(0, 1), one))
    outside = beside * jnp.where(row_id < 4, presence(1, -1), presence(1, 1))
    edges = {}
    for s in (1, -1):
        for cy in STEPS:
            tile = shifted[s, cy]
            tile = jnp.where(row_id < 4, tile[0:1], turn(jnp.broadcast_to(tile[7:8], (8, 128)), 4))
            aligned = tile
            for r in range(1, 8):
                aligned = jnp.where(row_id == r, turn(tile, -r), aligned)
            edges[s, cy] = aligned
    for i in range(19):
        cx, cy, cz = VELOCITIES[i]
        if cz != 0:
            value = [row_tile[i, :, lanes(h)] for h in (0, 1)]
            at = 4 * COLS[cz].index((i, 1))
            value = z_moved(value, cz, turn(edges[cz, cy], edge_lane(cz) - at))
            for h in (0, 1):
                row_tile[i, :, lanes(h)] = value[h]
    moving_y = [i for i in range(19) if VELOCITIES[i][1] != 0]
    for h in (0, 1):
        f = [row_tile[j, :, lanes(h)] for j in FIELDS]
        post = collide(f[:19], f[KIND], f[OWN], f[INFLOW : INFLOW + 2], moving_y, outside)
        for i in moving_y:
            row_post[i, :, lanes(h)] = post[i]

    def column_tile(j):
        _, cy, cz = VEL[j]
        tile = None
        for s in (1, -1):
            if cz == -s:
                at = 96 + 4 * LOCAL[s].index(j)
            else:
                at = 4 * COLS[s].index((j, 1 if cz == 0 else 2))
            for outer, parts in ((0, straight), (8, shifted)):
                start = outer + 4 * side(s)
                part = turn(parts[s, cy], start - at)
                here = jnp.logical_and(lane_id >= start, lane_id < start + 4)
                tile = part if tile is None else jnp.where(here, part, tile)
        return tile

    lowest, highest = lane_id % 4 == 0, lane_id % 4 == 3
    beside = jnp.where(lowest, presence(0, -1), jnp.where(highest, presence(0, 1), one))
    outside = beside * jnp.where(lane_id % 8 < 4, presence(2, -1), presence(2, 1))
    beyond = jnp.where(row_id == 0, presence(1, -1), presence(1, 1))
    outside = outside * jnp.where(lane_id < 8, one, beyond)
    f = [column_tile(j) for j in FIELDS]
    moving_z = [i for i in range(19) if VELOCITIES[i][2] != 0]
    column_post = collide(f[:19], f[KIND], f[OWN], f[INFLOW : INFLOW + 2], moving_z, outside)

    for p in (0, 1):
        acc = [[None, None] for _ in range(4)]
        for i in range(19):
            c = cx, cy, cz = VELOCITIES[i]
            plane = p - cx
            value = [second[i, plane + 1, :, lanes(h)] for h in (0, 1)]
            if cy != 0:
                k = 4 * side(cy) + plane + 1
                value = y_moved(value, cy, [row_post[i, k : k + 1, lanes(h)] for h in (0, 1)])
            if cz != 0:
                at = 4 * side(cz) + plane + 1
                edge = turn(column_post[i], edge_lane(cz) - at)
                if cy != 0:
                    corner = turn(column_post[i], edge_lane(cz) - at - 8)
                    edge = jnp.where(row_id == (0 if cy == 1 else 7), corner, slide(edge, cy))
                value = z_moved(value, cz, edge)
            for h in (0, 1):
                acc[0][h] = value[h] if acc[0][h] is None else acc[0][h] + value[h]
                for a in range(3):
                    if c[a] != 0:
                        old = zero if acc[1 + a][h] is None else acc[1 + a][h]
                        acc[1 + a][h] = old + value[h] if c[a] == 1 else old - value[h]
        for h in (0, 1):
            for k in range(4):
                out_ref[k, p, :, lanes(h)] = acc[k][h]

    await_present(MESSAGES, lambda d: d, send_sem.at[0])


def finish(sums_ref, rho_hbm, mom_hbm, sems):
    copies = [
        pltpu.make_async_copy(sums_ref.at[0], rho_hbm, sems.at[0]),
        pltpu.make_async_copy(sums_ref.at[1:4], mom_hbm, sems.at[1]),
    ]
    for copy in copies:
        copy.start()
    for copy in copies:
        copy.wait()


def solution(mesh):
    sizes = tuple(mesh.shape[a] for a in AXES)

    def shards(dist, site_kinds, relax, inflow):
        f32 = jnp.float32
        shape = site_kinds.shape
        sums = pl.pallas_call(
            functools.partial(kernel, sizes),
            out_shape=pltpu.VMEM((4,) + shape, f32),
            in_specs=[pl.BlockSpec(memory_space=pl.ANY)] * 4,
            out_specs=pl.BlockSpec(memory_space=pltpu.VMEM),
            scratch_shapes=[
                pltpu.VMEM((19,) + shape, f32),
                pltpu.VMEM(shape, jnp.int32),
                pltpu.VMEM((2,) + shape, f32),
                pltpu.VMEM((23, 6, 8, 256), f32),
                pltpu.VMEM((2, 4, 8, 256), f32),
                pltpu.VMEM((2, 4, 8, 256), f32),
                pltpu.VMEM((2, 48, 256), f32),
                pltpu.VMEM((2, 3, 48, 256), f32),
                pltpu.VMEM((2, 8, 128), f32),
                pltpu.VMEM((2, 3, 3, 8, 128), f32),
                pltpu.VMEM((1, 8, 128), f32),
                pltpu.VMEM((3, 3, 8, 128), f32),
                pltpu.VMEM((19, 4, 8, 256), f32),
                pltpu.VMEM((19, 4, 8, 256), f32),
                pltpu.VMEM((23, 8, 256), f32),
                pltpu.VMEM((19, 8, 256), f32),
                pltpu.VMEM((sum(map(tiles, MESSAGES)), 8, 128), f32),
                pltpu.SemaphoreType.DMA((4,)),
                pltpu.SemaphoreType.DMA((1,)),
                pltpu.SemaphoreType.DMA((2,)),
                pltpu.SemaphoreType.REGULAR((2,)),
            ],
            compiler_params=pltpu.CompilerParams(collective_id=0, has_side_effects=True),
        )(dist, site_kinds, relax, inflow)
        return pl.pallas_call(
            finish,
            out_shape=(
                jax.ShapeDtypeStruct(shape, f32),
                jax.ShapeDtypeStruct((3,) + shape, f32),
            ),
            in_specs=[pl.BlockSpec(memory_space=pltpu.VMEM)],
            out_specs=(pl.BlockSpec(memory_space=pl.ANY), pl.BlockSpec(memory_space=pl.ANY)),
            scratch_shapes=[pltpu.SemaphoreType.DMA((2,))],
        )(pltpu.with_memory_space_constraint(sums, pltpu.VMEM))

    return jax.shard_map(
        shards,
        mesh=mesh,
        in_specs=(
            P(None, "gx", "gy", "gz"),
            P("gx", "gy", "gz"),
            P("gx", "gy", "gz"),
            P(None, "gx", "gy", "gz"),
        ),
        out_specs=(P("gx", "gy", "gz"), P(None, "gx", "gy", "gz")),
        check_vma=False,
    )
```

```python
import functools
import itertools

import jax
import jax.numpy as jnp
from jax import lax
from jax.experimental import pallas as pl
from jax.experimental.pallas import tpu as pltpu
from jax.sharding import PartitionSpec as P

VELOCITIES = [
    (0, 0, 0),
    (1, 0, 0),
    (-1, 0, 0),
    (0, 1, 0),
    (0, -1, 0),
    (0, 0, 1),
    (0, 0, -1),
    (1, 1, 0),
    (-1, -1, 0),
    (1, -1, 0),
    (-1, 1, 0),
    (1, 0, 1),
    (-1, 0, -1),
    (1, 0, -1),
    (-1, 0, 1),
    (0, 1, 1),
    (0, -1, -1),
    (0, 1, -1),
    (0, -1, 1),
]
WEIGHTS = [1.0 / 3.0] + [1.0 / 18.0] * 6 + [1.0 / 36.0] * 12
AXES = ("gx", "gy", "gz")
MESH = pl.DeviceIdType.MESH

KIND, OWN, INFLOW = 19, 20, 21
VEL = VELOCITIES + [(0, 0, 0)] * 4
FIELDS = range(23)
ORDER = sorted(FIELDS, key=lambda j: (-VEL[j][0], j))
POS = [ORDER.index(j) for j in FIELDS]
STEPS = (-1, 0, 1)
DIRECTIONS = [(x, y, z) for x in STEPS for y in STEPS for z in STEPS if (x, y, z) != (0, 0, 0)]
NEAR = (-1, 0, 1, 2)


def groups(axis, sign):
    found = [(j, 1) for j in FIELDS if VEL[j][axis] in (0, sign)]
    found += [(j, 2) for j in FIELDS if VEL[j][axis] == sign]
    return sorted(found, key=lambda pair: VEL[pair[0]][0])


ROWS = {s: groups(1, s) for s in (1, -1)}
COLS = {s: groups(2, s) for s in (1, -1)}
LOCAL = {s: sorted([j for j in FIELDS if VEL[j][2] == -s], key=lambda j: VEL[j][0]) for s in (1, -1)}
LOCAL_LANE = {1: 96, -1: 64}
LEVEL = [i for i in range(19) if VELOCITIES[i][0] == 0]
FACE_ROWS = {s: [i for i in LEVEL if VELOCITIES[i][1] == -s] for s in (1, -1)}


def side(sign):
    return 0 if sign == 1 else 1


def opposite(direction):
    return tuple(-s for s in direction)


def upward(d):
    return next(s for s in (d[0], d[2], d[1]) if s != 0) == 1


def row_place(g, p):
    if g < 5:
        return 2 * g + p
    if g < 18:
        return 10 + 14 * p + g - 5
    return 38 + 2 * (g - 18) + p


def messages():
    found = []
    for d in DIRECTIONS:
        dx, dy, dz = d
        if dy == 0 and dz == 0:
            found += [("xp", d), ("xs", d), ("xa", d), ("xc", d)]
        if dz == 0 and dy != 0:
            found.append(("y", d))
        if dz != 0:
            found.append(("z", d))
        else:
            found.append(("l", d))
    return found


MESSAGES = messages()


def tiles(m):
    if m[0] == "y":
        return 12 if m[1][0] == 0 else 6
    return {"xp": 8, "xs": 8, "xa": 10, "xc": 10, "z": 1, "l": 1}[m[0]]


def kernel(
    sizes, dist_hbm, kinds_hbm, relax_hbm, inflow_hbm, out_ref,
    field, kinds, either, block, xs, xr, ys, yr, zs, zr, ls, lr, first, second, row_tile, row_post,
    size_ref, load_sem, send_sem, recv_sem, entered,
):
    me = tuple(lax.axis_index(a) for a in AXES)
    exists = {}
    for axis in range(3):
        exists[axis, 1] = me[axis] < sizes[axis] - 1
        exists[axis, -1] = me[axis] > 0

    def has(direction):
        parts = [exists[a, s] for a, s in enumerate(direction) if s != 0]
        return functools.reduce(jnp.logical_and, parts)

    def target(direction):
        return tuple(m + s for m, s in zip(me, direction))

    for p in (1, 0):
        group = [
            pltpu.make_async_copy(kinds_hbm.at[p], kinds.at[p], load_sem.at[p]),
            pltpu.make_async_copy(relax_hbm.at[p], either.at[0, p], load_sem.at[p]),
            pltpu.make_async_copy(inflow_hbm.at[0, p], either.at[1, p], load_sem.at[p]),
            pltpu.make_async_copy(
                inflow_hbm.at[1:3, p], block.at[POS[INFLOW] : POS[INFLOW] + 2, 2 + p], load_sem.at[p]
            ),
            pltpu.make_async_copy(dist_hbm.at[:, p], field.at[:, p], load_sem.at[2 + p]),
        ]
        for copy in group:
            copy.start()

    def is_origin(place):
        return jnp.logical_and(place[0] == 0, jnp.logical_and(place[1] == 0, place[2] == 0))

    here_origin = is_origin(me)

    def later(d):
        if upward(d):
            return jnp.logical_and(has(d), jnp.logical_not(here_origin))
        if max(d) == 1:
            return None
        return is_origin(target(d))

    def earlier(d):
        if upward(d):
            return jnp.logical_and(has(d), here_origin)
        if max(d) == 1:
            return has(d)
        return jnp.logical_and(has(d), jnp.logical_not(is_origin(target(d))))

    barrier = pltpu.get_barrier_semaphore()
    for d in DIRECTIONS:
        if later(d) is not None:
            @pl.when(later(d))
            def _():
                pl.semaphore_signal(barrier, inc=1, device_id=target(d), device_id_type=MESH)
    before = 0
    for d in DIRECTIONS:
        before = before + earlier(d).astype(jnp.int32)

    def ends(m):
        kind, (dx, dy, dz) = m
        if kind in ("xa", "xc"):
            at = slice(0, 5) if dx == 1 else slice(18, 23)
            mine = 3 if (kind == "xa") == (dx == 1) else 2
            theirs = mine - 2 * dx
            return block.at[at, mine : mine + 1], block.at[at, theirs : theirs + 1]
        if kind == "xp":
            mine, theirs = (3, 1) if dx == 1 else (2, 4)
            return block.at[14:18, mine : mine + 1], block.at[14:18, theirs : theirs + 1]
        if kind == "xs":
            return xs.at[side(dx)], xr.at[side(dx)]
        if kind == "y":
            rows = {0: slice(0, 48), 1: slice(24, 48), -1: slice(0, 24)}[dx]
            return ys.at[side(dy), rows], yr.at[side(dy), dx + 1, rows]
        if kind == "z":
            return zs.at[side(dz)], zr.at[side(dz), dx + 1, dy + 1]
        return ls.at[0], lr.at[dx + 1, dy + 1]

    def copy_of(m):
        src, dst = ends(m)
        return pltpu.make_async_remote_copy(
            src_ref=src, dst_ref=dst, send_sem=send_sem.at[0], recv_sem=recv_sem.at[side(m[1][0])],
            device_id=target(m[1]), device_id_type=MESH,
        )

    def await_tiles(count, sem):
        part = size_ref.at[0:count]
        pltpu.make_async_copy(part, part, sem).wait()

    def await_present(found, toward, sem):
        count = 0
        for m in found:
            count = count + tiles(m) * has(toward(m[1])).astype(jnp.int32)
        sums = set()
        for touched in itertools.product(((), (1,), (-1,), (1, -1)), repeat=3):
            known = [m for m in found if not any(v in touched[a] for a, v in enumerate(toward(m[1])))]
            sums.add(sum(map(tiles, known)))
        for total in sorted(sums - {0}):
            @pl.when(count == total)
            def _():
                await_tiles(total, sem)

    for m in MESSAGES:
        @pl.when(jnp.logical_not(has(opposite(m[1]))))
        def _():
            dst = ends(m)[1]
            dst[...] = jnp.zeros(dst.shape, jnp.float32)

    row_id = lax.broadcasted_iota(jnp.int32, (8, 128), 0)
    lane_id = lax.broadcasted_iota(jnp.int32, (8, 128), 1)
    one = jnp.ones((8, 128), jnp.float32)
    zero = jnp.zeros((8, 128), jnp.float32)

    def turn(tile, shift):
        shift %= 128
        return tile if shift == 0 else pltpu.roll(tile, shift, 1)

    def slide(tile, shift):
        return pltpu.roll(tile, shift % 8, 0)

    def lanes(h):
        return slice(h * 128, h * 128 + 128)

    def y_moved(value, sign, edge_row):
        edge = 0 if sign == 1 else 7
        return [jnp.where(row_id == edge, edge_row[h], slide(value[h], sign)) for h in (0, 1)]

    def z_moved(value, sign, edge_tile):
        rolled = [turn(v, sign) for v in value]
        if sign == 1:
            at = lane_id == 0
            return [jnp.where(at, edge_tile, rolled[0]), jnp.where(at, rolled[0], rolled[1])]
        at = lane_id == 127
        return [jnp.where(at, rolled[1], rolled[0]), jnp.where(at, edge_tile, rolled[1])]

    def edge_lane(sign):
        return 0 if sign == 1 else 127

    def collide(f, kind, own, inflow, wanted, inside=None, level=None):
        present = [i for i in range(19) if f[i] is not None]
        rho = functools.reduce(jnp.add, [f[i] for i in present])
        u = []
        for axis in range(3):
            plus = [f[i] for i in present if VELOCITIES[i][axis] == 1]
            minus = [f[i] for i in present if VELOCITIES[i][axis] == -1]
            u.append(functools.reduce(jnp.add, plus) - functools.reduce(jnp.add, minus))
        if level is not None:
            rho, u = rho + level[0], [u[0], u[1] + level[1], u[2] + level[2]]
        wall, fluid = kind < 0.5, jnp.logical_and(kind > 0.5, kind < 1.5)
        inlet, outlet = jnp.logical_and(kind > 1.5, kind < 2.5), kind > 2.5
        r = jnp.where(outlet, one, rho)
        v = [jnp.where(inlet, given, u[a]) for a, given in enumerate((own, inflow[0], inflow[1]))]
        take = jnp.where(wall, zero, jnp.where(fluid, own, one))
        keep = one - take
        if inside is not None:
            take, keep = take * inside, keep * inside
        usq = v[0] * v[0] + v[1] * v[1] + v[2] * v[2]
        common = r - 1.5 * usq
        post = {}
        if 0 in wanted:
            post[0] = keep * f[0] + take * (WEIGHTS[0] * common)
        for i in range(1, 19, 2):
            if i not in wanted and i + 1 not in wanted:
                continue
            along = None
            for a in range(3):
                if VELOCITIES[i][a] != 0:
                    term = v[a] if VELOCITIES[i][a] == 1 else -v[a]
                    along = term if along is None else along + term
            even = WEIGHTS[i] * (common + 4.5 * along * along)
            odd = (3.0 * WEIGHTS[i]) * along
            if i in wanted:
                post[i] = keep * jnp.where(wall, f[i + 1], f[i]) + take * (even + odd)
            if i + 1 in wanted:
                post[i + 1] = keep * jnp.where(wall, f[i], f[i + 1]) + take * (even - odd)
        return post

    small = [m for m in MESSAGES if m[0] in ("z", "l")]
    small = sorted(small, key=lambda m: -sum(map(abs, m[1])))
    rows = sorted([m for m in MESSAGES if m[0] == "y"], key=lambda m: -abs(m[1][0]))
    everything = small + [m for m in MESSAGES if m[0] in ("xp", "xs", "xa", "xc")] + rows

    def start(found):
        for m in found:
            copy_of(m).start()

    def origin_starts(found):
        there = [m for m in found if min(m[1]) >= 0 and all(sizes[a] > 1 for a in range(3) if m[1][a] == 1)]
        if there:
            @pl.when(here_origin)
            def _():
                start(there)

    def all_to(d):
        start([m for m in everything if m[1] == d])

    def add_level(sums, i, value):
        for n, factor in enumerate((1, VELOCITIES[i][1], VELOCITIES[i][2])):
            for h in (0, 1):
                if factor != 0:
                    sums[n][h] = sums[n][h] + value[h] if factor == 1 else sums[n][h] - value[h]

    def sum_level(dx):
        p = 1 if dx == 1 else 0
        sums = [[zero, zero] for _ in range(3)]
        for i in LEVEL:
            _, cy, cz = VELOCITIES[i]
            value = [block[POS[i], 2 + p, :, lanes(h)] for h in (0, 1)]
            if cy != 0:
                value = y_moved(value, cy, [zero, zero])
            if cz != 0:
                value = z_moved(value, cz, zero)
            add_level(sums, i, value)
        for h in (0, 1):
            for n in range(3):
                xs[side(dx), n, :, lanes(h)] = sums[n][h]
            xs[side(dx), 3, :, lanes(h)] = zero
        for s in (1, -1):
            for n, j in enumerate(FACE_ROWS[s]):
                k, row = 3 * side(s) + n, 0 if s == 1 else 7
                xs[side(dx), 3, k : k + 1] = block[POS[j], 2 + p, row : row + 1]

    @pl.when(before > 0)
    def _():
        pl.semaphore_wait(barrier, before)

    def answer(d, which):
        pl.semaphore_signal(entered.at[which], inc=1, device_id=target(d), device_id_type=MESH)

    @pl.when(here_origin)
    def _():
        for d in DIRECTIONS:
            if min(d) >= 0 and all(sizes[a] > 1 for a in range(3) if d[a] == 1):
                answer(d, 1)

    @pl.when(jnp.logical_not(here_origin))
    def _():
        for d in DIRECTIONS:
            if not upward(d):
                @pl.when(earlier(d))
                def _():
                    answer(d, 0)

    for p in (1, 0):
        await_tiles(10, load_sem.at[p])
        block[POS[KIND], 2 + p] = kinds[p].astype(jnp.float32)
        block[POS[OWN], 2 + p] = jnp.where(kinds[p] == 2, either[1, p], either[0, p])
        if p == 1:
            origin_starts([("xp", (1, 0, 0))])
        await_tiles(38, load_sem.at[2 + p])
        for h in (0, 1):
            z = lanes(h)
            post = collide(
                [field[i, p, :, z] for i in range(19)],
                block[POS[KIND], 2 + p, :, z],
                block[POS[OWN], 2 + p, :, z],
                [block[POS[INFLOW + a], 2 + p, :, z] for a in range(2)],
                range(19),
            )
            for i in range(19):
                block[POS[i], 2 + p, :, z] = post[i]
        if p == 1:
            sum_level(1)
            origin_starts([("xs", (1, 0, 0)), ("xa", (1, 0, 0))])

    for s in (1, -1):
        for g, (j, depth) in enumerate(ROWS[s]):
            for p in (0, 1):
                row = 8 - depth if s == 1 else depth - 1
                k = row_place(g, p)
                ys[side(s), k : k + 1] = block[POS[j], 2 + p, row : row + 1]
    origin_starts([("y", (0, 1, 0))])

    def column(j, p, at):
        return block[POS[j], 2 + p, :, lanes(at // 128)], at % 128

    tile = zero
    for s in (1, -1):
        for g, j in enumerate(LOCAL[s]):
            for p in (0, 1):
                value, at = column(j, p, 0 if s == 1 else 255)
                to = LOCAL_LANE[s] + 4 * g + p + VEL[j][0] + 1
                tile = jnp.where(lane_id == to, turn(value, to - at), tile)
    ls[0] = tile
    origin_starts([m for m in small if m[0] == "l"])
    for s in (1, -1):
        tile = zero
        for g, (j, depth) in enumerate(COLS[s]):
            for p in (0, 1):
                value, at = column(j, p, 256 - depth if s == 1 else depth - 1)
                to = 4 * g + p + VEL[j][0] + 1
                tile = jnp.where(lane_id == to, turn(value, to - at), tile)
        zs[side(s)] = tile
    origin_starts([m for m in small if m[0] == "z"] + [("xc", (1, 0, 0))])
    origin_starts([m for m in rows if m[1] != (0, 1, 0)])
    sum_level(-1)

    after = 0
    for d in DIRECTIONS:
        if upward(d):
            after = after + later(d).astype(jnp.int32)

    @pl.when(jnp.logical_not(here_origin))
    def _():
        for d in DIRECTIONS:
            if not upward(d):
                @pl.when(earlier(d))
                def _():
                    all_to(d)

        @pl.when(after > 0)
        def _():
            pl.semaphore_wait(entered.at[0], after)

        for d in DIRECTIONS:
            if upward(d):
                @pl.when(later(d))
                def _():
                    all_to(d)
        for d in DIRECTIONS:
            if max(d) < 1:
                @pl.when(later(d))
                def _():
                    pl.semaphore_wait(entered.at[1], 1)
                    all_to(d)

    await_present([m for m in MESSAGES if m[1][0] != 1], opposite, recv_sem.at[1])

    group_id = lane_id // 4
    lane_cx = jnp.where(group_id < 5, -1, jnp.where(group_id < 18, 0, 1))
    lane_cx = jnp.where(group_id >= 24, jnp.where(group_id < 25, -1, jnp.where(group_id < 28, 0, 1)), lane_cx)
    source = lane_id % 4 - 1 - lane_cx

    def merge(steps_x):
        straight, shifted = {}, {}
        for s in (1, -1):
            merged = {}
            for dy in STEPS:
                parts = {}
                for dx in steps_x:
                    local = ls[0] if dx == 0 and dy == 0 else lr[dx + 1, dy + 1]
                    if s == -1:
                        local = turn(local, 32)
                    part = jnp.where(lane_id >= 96, local, zr[side(s), dx + 1, dy + 1])
                    parts[dx] = turn(part, -2 * dx)
                whole = jnp.where(source > 1, parts[-1], parts[0])
                merged[dy] = jnp.where(source < 0, parts[1], whole) if 1 in parts else whole
            below, own, above = merged[1], merged[0], merged[-1]
            top, bottom = row_id == 0, row_id == 7
            straight[s, 0] = own
            straight[s, 1] = jnp.where(top, slide(below, 1), slide(own, 1))
            straight[s, -1] = jnp.where(bottom, slide(above, -1), slide(own, -1))
            shifted[s, 0] = jnp.where(top, slide(below, 1), slide(above, -1))
            shifted[s, 1] = jnp.where(top, slide(below, 2), own)
            shifted[s, -1] = jnp.where(bottom, slide(above, -2), own)
        return straight, shifted

    def incoming_row(s, j, depth, plane):
        p = plane - VEL[j][0]
        dx = 1 if p < 0 else -1 if p > 1 else 0
        k = row_place(ROWS[s].index((j, depth)), p + 2 * dx)
        return [yr[side(s), dx + 1, k : k + 1, lanes(h)] for h in (0, 1)]

    def presence(axis, sign):
        return exists[axis, sign].astype(jnp.float32)

    def collide_plane(plane, straight):
        near = plane in (-1, 2)
        sums = None
        if near:
            ends_at = 0 if plane == -1 else 1
            sums = [[xr[ends_at, n, :, lanes(h)] for h in (0, 1)] for n in range(3)]
        for i in range(19):
            cx, cy, cz = VELOCITIES[i]
            if near and cx == 0:
                value = [zero, zero]
            else:
                value = [block[POS[i], plane - cx + 2, :, lanes(h)] for h in (0, 1)]
            if cy != 0:
                value = y_moved(value, cy, incoming_row(cy, i, 1, plane))
            if cz != 0:
                at = 4 * COLS[cz].index((i, 1)) + plane + 1
                value = z_moved(value, cz, turn(straight[cz, cy], edge_lane(cz) - at))
            if near and cx == 0:
                add_level(sums, i, value)
                continue
            for h in (0, 1):
                first[i, plane + 1, :, lanes(h)] = value[h]
        inside, wanted = None, range(19)
        if plane == -1:
            inside, wanted = one * presence(0, -1), [i for i in range(19) if VELOCITIES[i][0] == 1]
        if plane == 2:
            inside, wanted = one * presence(0, 1), [i for i in range(19) if VELOCITIES[i][0] == -1]
        for h in (0, 1):
            z = lanes(h)
            post = collide(
                [None if near and i in LEVEL else first[i, plane + 1, :, z] for i in range(19)],
                block[POS[KIND], plane + 2, :, z],
                block[POS[OWN], plane + 2, :, z],
                [block[POS[INFLOW + a], plane + 2, :, z] for a in range(2)],
                wanted, inside, [sums[n][h] for n in range(3)] if near else None,
            )
            for i in wanted:
                second[i, plane + 1, :, z] = post[i]

    def fill_rows(from_below):
        for j in FIELDS:
            cx, cy, cz = VEL[j]
            for s in (1, -1):
                for plane in NEAR:
                    if (plane - cx < 0) != from_below:
                        continue
                    k = 4 * side(s) + plane + 1
                    if cy == -s and cx == 0 and plane in (-1, 2):
                        n = 3 * side(s) + FACE_ROWS[s].index(j)
                        row_tile[j, k : k + 1] = xr[0 if plane == -1 else 1, 3, n : n + 1]
                    elif cy == -s:
                        row = 0 if s == 1 else 7
                        row_tile[j, k : k + 1] = block[POS[j], plane - cx + 2, row : row + 1]
                    else:
                        value = incoming_row(s, j, 1 if cy == 0 else 2, plane)
                        for h in (0, 1):
                            row_tile[j, k : k + 1, lanes(h)] = value[h]

    partial, _ = merge((-1, 0))
    fill_rows(False)
    for plane in (1, 2):
        collide_plane(plane, partial)
    await_present([m for m in MESSAGES if m[1][0] == 1], opposite, recv_sem.at[0])
    fill_rows(True)
    straight, shifted = merge(STEPS)
    for plane in (-1, 0):
        collide_plane(plane, straight)

    lowest, highest = row_id % 4 == 0, row_id % 4 == 3
    beside = jnp.where(lowest, presence(0, -1), jnp.where(highest, presence(0, 1), one))
    outside = beside * jnp.where(row_id < 4, presence(1, -1), presence(1, 1))
    edges = {}
    for s in (1, -1):
        for cy in STEPS:
            tile = shifted[s, cy]
            tile = jnp.where(row_id < 4, tile[0:1], turn(jnp.broadcast_to(tile[7:8], (8, 128)), 4))
            aligned = tile
            for r in range(1, 8):
                aligned = jnp.where(row_id == r, turn(tile, -r), aligned)
            edges[s, cy] = aligned
    for i in range(19):
        cx, cy, cz = VELOCITIES[i]
        if cz != 0:
            value = [row_tile[i, :, lanes(h)] for h in (0, 1)]
            at = 4 * COLS[cz].index((i, 1))
            value = z_moved(value, cz, turn(edges[cz, cy], edge_lane(cz) - at))
            for h in (0, 1):
                row_tile[i, :, lanes(h)] = value[h]
    moving_y = [i for i in range(19) if VELOCITIES[i][1] != 0]
    for h in (0, 1):
        f = [row_tile[j, :, lanes(h)] for j in FIELDS]
        post = collide(f[:19], f[KIND], f[OWN], f[INFLOW : INFLOW + 2], moving_y, outside)
        for i in moving_y:
            row_post[i, :, lanes(h)] = post[i]

    def column_tile(j):
        _, cy, cz = VEL[j]
        tile = None
        for s in (1, -1):
            if cz == -s:
                at = 96 + 4 * LOCAL[s].index(j)
            else:
                at = 4 * COLS[s].index((j, 1 if cz == 0 else 2))
            for outer, parts in ((0, straight), (8, shifted)):
                start = outer + 4 * side(s)
                part = turn(parts[s, cy], start - at)
                here = jnp.logical_and(lane_id >= start, lane_id < start + 4)
                tile = part if tile is None else jnp.where(here, part, tile)
        return tile

    lowest, highest = lane_id % 4 == 0, lane_id % 4 == 3
    beside = jnp.where(lowest, presence(0, -1), jnp.where(highest, presence(0, 1), one))
    outside = beside * jnp.where(lane_id % 8 < 4, presence(2, -1), presence(2, 1))
    beyond = jnp.where(row_id == 0, presence(1, -1), presence(1, 1))
    outside = outside * jnp.where(lane_id < 8, one, beyond)
    f = [column_tile(j) for j in FIELDS]
    moving_z = [i for i in range(19) if VELOCITIES[i][2] != 0]
    column_post = collide(f[:19], f[KIND], f[OWN], f[INFLOW : INFLOW + 2], moving_z, outside)

    for p in (0, 1):
        acc = [[None, None] for _ in range(4)]
        for i in range(19):
            c = cx, cy, cz = VELOCITIES[i]
            plane = p - cx
            value = [second[i, plane + 1, :, lanes(h)] for h in (0, 1)]
            if cy != 0:
                k = 4 * side(cy) + plane + 1
                value = y_moved(value, cy, [row_post[i, k : k + 1, lanes(h)] for h in (0, 1)])
            if cz != 0:
                at = 4 * side(cz) + plane + 1
                edge = turn(column_post[i], edge_lane(cz) - at)
                if cy != 0:
                    corner = turn(column_post[i], edge_lane(cz) - at - 8)
                    edge = jnp.where(row_id == (0 if cy == 1 else 7), corner, slide(edge, cy))
                value = z_moved(value, cz, edge)
            for h in (0, 1):
                acc[0][h] = value[h] if acc[0][h] is None else acc[0][h] + value[h]
                for a in range(3):
                    if c[a] != 0:
                        old = zero if acc[1 + a][h] is None else acc[1 + a][h]
                        acc[1 + a][h] = old + value[h] if c[a] == 1 else old - value[h]
        for h in (0, 1):
            for k in range(4):
                out_ref[k, p, :, lanes(h)] = acc[k][h]

    await_present(MESSAGES, lambda d: d, send_sem.at[0])


def finish(sums_ref, rho_hbm, mom_hbm, sems):
    copies = [
        pltpu.make_async_copy(sums_ref.at[0], rho_hbm, sems.at[0]),
        pltpu.make_async_copy(sums_ref.at[1:4], mom_hbm, sems.at[1]),
    ]
    for copy in copies:
        copy.start()
    for copy in copies:
        copy.wait()


def solution(mesh):
    sizes = tuple(mesh.shape[a] for a in AXES)

    def shards(dist, site_kinds, relax, inflow):
        f32 = jnp.float32
        shape = site_kinds.shape
        sums = pl.pallas_call(
            functools.partial(kernel, sizes),
            out_shape=pltpu.VMEM((4,) + shape, f32),
            in_specs=[pl.BlockSpec(memory_space=pl.ANY)] * 4,
            out_specs=pl.BlockSpec(memory_space=pltpu.VMEM),
            scratch_shapes=[
                pltpu.VMEM((19,) + shape, f32),
                pltpu.VMEM(shape, jnp.int32),
                pltpu.VMEM((2,) + shape, f32),
                pltpu.VMEM((23, 6, 8, 256), f32),
                pltpu.VMEM((2, 4, 8, 256), f32),
                pltpu.VMEM((2, 4, 8, 256), f32),
                pltpu.VMEM((2, 48, 256), f32),
                pltpu.VMEM((2, 3, 48, 256), f32),
                pltpu.VMEM((2, 8, 128), f32),
                pltpu.VMEM((2, 3, 3, 8, 128), f32),
                pltpu.VMEM((1, 8, 128), f32),
                pltpu.VMEM((3, 3, 8, 128), f32),
                pltpu.VMEM((19, 4, 8, 256), f32),
                pltpu.VMEM((19, 4, 8, 256), f32),
                pltpu.VMEM((23, 8, 256), f32),
                pltpu.VMEM((19, 8, 256), f32),
                pltpu.VMEM((sum(map(tiles, MESSAGES)), 8, 128), f32),
                pltpu.SemaphoreType.DMA((4,)),
                pltpu.SemaphoreType.DMA((1,)),
                pltpu.SemaphoreType.DMA((2,)),
                pltpu.SemaphoreType.REGULAR((2,)),
            ],
            compiler_params=pltpu.CompilerParams(collective_id=0, has_side_effects=True),
        )(dist, site_kinds, relax, inflow)
        return pl.pallas_call(
            finish,
            out_shape=(
                jax.ShapeDtypeStruct(shape, f32),
                jax.ShapeDtypeStruct((3,) + shape, f32),
            ),
            in_specs=[pl.BlockSpec(memory_space=pltpu.VMEM)],
            out_specs=(pl.BlockSpec(memory_space=pl.ANY), pl.BlockSpec(memory_space=pl.ANY)),
            scratch_shapes=[pltpu.SemaphoreType.DMA((2,))],
        )(pltpu.with_memory_space_constraint(sums, pltpu.VMEM))

    return jax.shard_map(
        shards,
        mesh=mesh,
        in_specs=(
            P(None, "gx", "gy", "gz"),
            P("gx", "gy", "gz"),
            P("gx", "gy", "gz"),
            P(None, "gx", "gy", "gz"),
        ),
        out_specs=(P("gx", "gy", "gz"), P(None, "gx", "gy", "gz")),
        check_vma=False,
    )
```
